16 devices in a mesh: stage: 2 (over z), expert: 8 (over y, x, core).
Axes of the slice: x: 2, y: 2, z: 2, core: 2. Of those that a mesh axis runs over, the one named last changes fastest.
Arguments:
- x_act: bfloat16 [2, 8192, 2048], P('stage', 'expert')
- route_idx: int32 [2, 8192, 8], P('stage', 'expert')
- route_wts: float32 [2, 8192, 8], P('stage', 'expert')
- w_one: bfloat16 [2, 32, 2048, 512], P('stage', 'expert')
- w_three: bfloat16 [2, 32, 2048, 512], P('stage', 'expert')
- w_two: bfloat16 [2, 32, 512, 2048], P('stage', 'expert')
- dy_act: bfloat16 [2, 8192, 2048], P('stage', 'expert')
Outputs:
- output 1: bfloat16 [2, 8192, 2048], P('stage', 'expert')
- output 2: bfloat16 [2, 8192, 2048], P('stage', 'expert')
- output 3: bfloat16 [2, 32, 2048, 512], P('stage', 'expert')
- output 4: bfloat16 [2, 32, 2048, 512], P('stage', 'expert')
- output 5: bfloat16 [2, 32, 512, 2048], P('stage', 'expert')
All inputs are finite; a program needn't handle non-finite values.
Results may differ from the reference program's by a relative error of at most 0.0126552.
Values are sent between devices in bfloat16 or wider.
A program may use at most 1 GiB of HBM per device.

```python
import jax
import jax.numpy as jnp
from jax import lax

STAGES = 2
EXPERT_DEVS = 8
TOK_DEV = 1024
MODEL_DIM = 2048
FFN_DIM = 512
EXPERTS = 32
TOP_K = 8
ROUTE_DEVS = 8

LOCAL_EXP = EXPERTS // EXPERT_DEVS
CAPACITY = 2 * TOK_DEV * TOP_K // EXPERTS - 1
TOKENS = EXPERT_DEVS * TOK_DEV
N_SLOT = TOK_DEV * TOP_K


def draw_routing(rng_key):
    n_blocks = EXPERTS // TOP_K
    mean_load = TOK_DEV * TOP_K // EXPERTS
    group_devs = min(ROUTE_DEVS, EXPERT_DEVS)
    group_exp = group_devs * LOCAL_EXP
    key_pair, key_shift, key_tok, key_grp, key_dev = jax.random.split(rng_key, 5)
    block_ids = jnp.broadcast_to(jnp.arange(n_blocks, dtype=jnp.int32), (STAGES, n_blocks))
    pair_perm = jax.random.permutation(key_pair, block_ids, axis=1, independent=True)
    shifts = jax.random.randint(key_shift, (STAGES, EXPERT_DEVS, n_blocks // 2), 0, mean_load)
    shifts = shifts.at[:, :, 0].set(mean_load - 1)
    pair_sign = jnp.array([1, -1], dtype=jnp.int32)
    delta_pos = (shifts[:, :, :, None] * pair_sign).reshape(STAGES, EXPERT_DEVS, n_blocks)
    inv_perm = jnp.broadcast_to(jnp.argsort(pair_perm, axis=1)[:, None, :], delta_pos.shape)
    blk_load = mean_load + jnp.take_along_axis(delta_pos, inv_perm, axis=2)
    blk_ends = jnp.cumsum(blk_load, axis=2)
    tok_pos = jnp.arange(TOK_DEV, dtype=jnp.int32)
    blk_of = jnp.sum((blk_ends[:, :, None, :] <= tok_pos[None, None, :, None]).astype(jnp.int32), axis=3)
    blk_of = jax.random.permutation(key_tok, blk_of, axis=2, independent=True)
    virt_ids = blk_of[:, :, :, None] * TOP_K + jnp.arange(TOP_K, dtype=jnp.int32)
    virt_flat = virt_ids.reshape(STAGES, TOKENS * TOP_K)
    inner_ids = jnp.broadcast_to(jnp.arange(group_exp, dtype=jnp.int32), (STAGES, EXPERTS // group_exp, group_exp))
    grp_perm = jax.random.permutation(key_grp, inner_ids, axis=2, independent=True).reshape(STAGES, EXPERTS)
    dev_ids = jnp.broadcast_to(jnp.arange(EXPERT_DEVS, dtype=jnp.int32), (STAGES, EXPERT_DEVS))
    dev_perm = jax.random.permutation(key_dev, dev_ids, axis=1, independent=True)
    in_group = jnp.take_along_axis(grp_perm, virt_flat, axis=1)
    pre_dev = (virt_flat // group_exp) * group_devs + in_group // LOCAL_EXP
    dest_dev = jnp.take_along_axis(dev_perm, pre_dev, axis=1)
    expert_id = dest_dev * LOCAL_EXP + in_group % LOCAL_EXP
    return expert_id.reshape(STAGES, TOKENS, TOP_K)


def setup_inputs(seed: int = 0) -> dict:
    rng_key = jax.random.key(seed)
    key_x, key_idx, key_wts, key_one, key_three, key_two, key_dy = jax.random.split(rng_key, 7)
    x_act = jax.random.normal(key_x, (STAGES, TOKENS, MODEL_DIM), jnp.float32)
    route_idx = draw_routing(key_idx)
    route_wts = jax.random.uniform(key_wts, (STAGES, TOKENS, TOP_K), jnp.float32, 0.5, 1.5)
    w_one = jax.random.normal(key_one, (STAGES, EXPERTS, MODEL_DIM, FFN_DIM), jnp.float32) * MODEL_DIM ** -0.5
    w_three = jax.random.normal(key_three, (STAGES, EXPERTS, MODEL_DIM, FFN_DIM), jnp.float32) * MODEL_DIM ** -0.5
    w_two = jax.random.normal(key_two, (STAGES, EXPERTS, FFN_DIM, MODEL_DIM), jnp.float32) * FFN_DIM ** -0.5
    dy_act = jax.random.normal(key_dy, (STAGES, TOKENS, MODEL_DIM), jnp.float32)
    return {
        'x_act': x_act.astype(jnp.bfloat16),
        'route_idx': route_idx,
        'route_wts': route_wts,
        'w_one': w_one.astype(jnp.bfloat16),
        'w_three': w_three.astype(jnp.bfloat16),
        'w_two': w_two.astype(jnp.bfloat16),
        'dy_act': dy_act.astype(jnp.bfloat16),
    }


def take_rows(row_table, row_ids):
    return jnp.take(row_table, row_ids, axis=0, mode='fill', fill_value=0)


def stage_tables(idx_blk):
    slot_ids = idx_blk.reshape(N_SLOT)
    hit_mat = (slot_ids[:, None] == jnp.arange(EXPERTS, dtype=jnp.int32)[None, :]).astype(jnp.int32)
    slot_rank = jnp.sum(jnp.cumsum(hit_mat, axis=0) * hit_mat, axis=1) - 1
    buf_pos = slot_ids * CAPACITY + slot_rank
    slot_at = jnp.full((EXPERTS * CAPACITY,), N_SLOT, jnp.int32).at[buf_pos].set(jnp.arange(N_SLOT, dtype=jnp.int32))
    return buf_pos, slot_at


def one_expert(operands):
    x_rows, d_rows, w_in_one, w_in_three, w_out = operands
    pre_one = jnp.dot(x_rows, w_in_one, preferred_element_type=jnp.float32)
    pre_three = jnp.dot(x_rows, w_in_three, preferred_element_type=jnp.float32)
    sig_one = jax.nn.sigmoid(pre_one)
    act_one = pre_one * sig_one
    hidden = (act_one * pre_three).astype(jnp.bfloat16)
    out_rows = jnp.dot(hidden, w_out, preferred_element_type=jnp.float32).astype(jnp.bfloat16)
    d_hidden = jnp.dot(d_rows, w_out.T, preferred_element_type=jnp.float32).astype(jnp.bfloat16).astype(jnp.float32)
    d_three = (d_hidden * act_one).astype(jnp.bfloat16)
    d_one = (d_hidden * pre_three * sig_one * (1.0 + pre_one * (1.0 - sig_one))).astype(jnp.bfloat16)
    dx_rows = (jnp.dot(d_one, w_in_one.T, preferred_element_type=jnp.float32) + jnp.dot(d_three, w_in_three.T, preferred_element_type=jnp.float32)).astype(jnp.bfloat16)
    g_one = jnp.dot(x_rows.T, d_one, preferred_element_type=jnp.float32).astype(jnp.bfloat16)
    g_three = jnp.dot(x_rows.T, d_three, preferred_element_type=jnp.float32).astype(jnp.bfloat16)
    g_two = jnp.dot(hidden.T, d_rows, preferred_element_type=jnp.float32).astype(jnp.bfloat16)
    return out_rows, dx_rows, g_one, g_three, g_two


def to_experts(rows):
    return jnp.transpose(rows.reshape(EXPERT_DEVS, EXPERTS, CAPACITY, MODEL_DIM), (1, 0, 2, 3)).reshape(EXPERTS, EXPERT_DEVS * CAPACITY, MODEL_DIM)


def from_experts(rows):
    return jnp.transpose(rows.reshape(EXPERTS, EXPERT_DEVS, CAPACITY, MODEL_DIM), (1, 0, 2, 3)).reshape(EXPERT_DEVS, EXPERTS * CAPACITY, MODEL_DIM)


def stage_layer(operands):
    x_in, idx_in, wts_in, w_one, w_three, w_two, dy_in = operands
    buf_pos, slot_at = lax.map(stage_tables, idx_in.reshape(EXPERT_DEVS, TOK_DEV, TOP_K))
    x_dev = x_in.reshape(EXPERT_DEVS, TOK_DEV, MODEL_DIM)
    wts_dev = wts_in.reshape(EXPERT_DEVS, TOK_DEV, TOP_K)
    dy_dev = dy_in.reshape(EXPERT_DEVS, TOK_DEV, 1, MODEL_DIM)
    d_slot = (wts_dev[:, :, :, None] * dy_dev.astype(jnp.float32)).astype(jnp.bfloat16).reshape(EXPERT_DEVS, N_SLOT, MODEL_DIM)
    x_exp = to_experts(jax.vmap(take_rows)(x_dev, slot_at // TOP_K))
    d_exp = to_experts(jax.vmap(take_rows)(d_slot, slot_at))
    out_exp, dx_exp, dw_one, dw_three, dw_two = lax.map(one_expert, (x_exp, d_exp, w_one, w_three, w_two))
    out_slot = jax.vmap(take_rows)(from_experts(out_exp), buf_pos).reshape(EXPERT_DEVS, TOK_DEV, TOP_K, MODEL_DIM)
    dx_slot = jax.vmap(take_rows)(from_experts(dx_exp), buf_pos).reshape(EXPERT_DEVS, TOK_DEV, TOP_K, MODEL_DIM)
    y_out = jnp.sum(wts_dev[:, :, :, None] * out_slot.astype(jnp.float32), axis=2).astype(jnp.bfloat16)
    dx_out = jnp.sum(dx_slot.astype(jnp.float32), axis=2).astype(jnp.bfloat16)
    return y_out.reshape(TOKENS, MODEL_DIM), dx_out.reshape(TOKENS, MODEL_DIM), dw_one, dw_three, dw_two


def reference(x_act, route_idx, route_wts, w_one, w_three, w_two, dy_act):
    x_in = jnp.roll(x_act, 1, axis=0)
    idx_in = jnp.roll(route_idx, 1, axis=0)
    wts_in = jnp.roll(route_wts, 1, axis=0)
    y_act, dx_dst, dw_one, dw_three, dw_two = lax.map(stage_layer, (x_in, idx_in, wts_in, w_one, w_three, w_two, dy_act))
    dx_act = jnp.roll(dx_dst, -1, axis=0)
    return (y_act, dx_act, dw_one, dw_three, dw_two)
```

```python
import functools

import jax
import jax.numpy as jnp
from jax import lax
from jax.experimental import pallas as pl
from jax.experimental.pallas import tpu as pltpu
from jax.sharding import PartitionSpec as P


F32 = jnp.float32
BF16 = jnp.bfloat16
FWD_CHUNKS = (256, 256, 512)
BWD_CHUNKS = (512, 384, 128)
TILE_F = 256
TILE_A = 128
VMEM_LIMIT = 64000 * 1024


def dot(lhs, rhs):
    return jnp.dot(lhs, rhs, preferred_element_type=F32)


def dot_t(lhs, rhs):
    return lax.dot_general(lhs, rhs, (((1,), (1,)), ((), ())), preferred_element_type=F32)


def dot_a(lhs, rhs):
    return lax.dot_general(lhs, rhs, (((0,), (0,)), ((), ())), preferred_element_type=F32)


def gate_column(gates, expert):
    lanes = lax.broadcasted_iota(jnp.int32, gates.shape, 1)
    return jnp.sum(jnp.where(lanes == expert, gates, 0.0), axis=1, keepdims=True)


def params(semantics):
    return pltpu.CompilerParams(dimension_semantics=semantics, vmem_limit_bytes=VMEM_LIMIT)


def fwd_body(ffn, n_local, first_ref, x_ref, g_ref, w13_ref, w2_ref, y_ref):
    gates = g_ref[0]
    for e in range(n_local):
        gate = gate_column(gates, first_ref[0] + e)
        pre = dot(x_ref[0], w13_ref[e])
        one, three = pre[:, :ffn], pre[:, ffn:]
        hidden = jnp.where(gate > 0.0, one * jax.nn.sigmoid(one) * three, 0.0).astype(BF16)
        out = gate * dot(hidden, w2_ref[e]).astype(BF16).astype(F32)
        if e == 0:
            y_ref[0] = out
        else:
            y_ref[0] += out


def expert_fwd(first, x, gates, w13, w2, start):
    n_src, rows, model = x.shape
    n_local, ffn = w2.shape[:2]
    tile = min(TILE_F, rows)
    steps = rows // tile
    n_exp = gates.shape[2]
    flops = 2 * n_src * rows * n_local * model * ffn * 3
    return pl.pallas_call(
        functools.partial(fwd_body, ffn, n_local),
        grid_spec=pltpu.PrefetchScalarGridSpec(
            num_scalar_prefetch=1,
            grid=(n_src, steps),
            in_specs=[
                pl.BlockSpec((1, tile, model), lambda s, t, _: (s, t, 0)),
                pl.BlockSpec((1, tile, n_exp), lambda s, t, _: (s, start // tile + t, 0)),
                pl.BlockSpec(w13.shape, lambda s, t, _: (0, 0, 0), pipeline_mode=pl.Buffered(1)),
                pl.BlockSpec(w2.shape, lambda s, t, _: (0, 0, 0), pipeline_mode=pl.Buffered(1)),
            ],
            out_specs=pl.BlockSpec((1, tile, model), lambda s, t, _: (s, t, 0)),
        ),
        out_shape=jax.ShapeDtypeStruct((n_src, rows, model), F32),
        compiler_params=params(('arbitrary', 'arbitrary')),
        cost_estimate=pl.CostEstimate(flops=flops, bytes_accessed=n_src * rows * model * 6, transcendentals=0),
        name='expert_fwd',
    )(first, x, gates, w13, w2)


def bwd_body(ffn, n_local, first_ref, x_ref, dy_ref, g_ref, w13_ref, w2_ref, *refs):
    dx_ref, da_ref, h_ref = refs[-3:]
    gates = g_ref[0]
    for e in range(n_local):
        gate = gate_column(gates, first_ref[0] + e)
        live = gate > 0.0
        pre = dot(x_ref[0], w13_ref[e])
        one, three = pre[:, :ffn], pre[:, ffn:]
        sig = jax.nn.sigmoid(one)
        act = one * sig
        h_ref[0, :, e * ffn:(e + 1) * ffn] = jnp.where(live, act * three, 0.0).astype(BF16)
        d_out = (gate * dy_ref[0].astype(F32)).astype(BF16)
        d_hid = dot_t(d_out, w2_ref[e]).astype(BF16).astype(F32)
        d_one = jnp.where(live, d_hid * three * sig * (1.0 + one * (1.0 - sig)), 0.0).astype(BF16)
        d_three = jnp.where(live, d_hid * act, 0.0).astype(BF16)
        d_pre = jnp.concatenate([d_one, d_three], axis=1)
        da_ref[0, :, 2 * e * ffn:2 * (e + 1) * ffn] = d_pre
        dx = dot_t(d_pre, w13_ref[e]).astype(BF16).astype(F32)
        if e == 0:
            dx_ref[0] = dx
        else:
            dx_ref[0] += dx


def expert_bwd(first, x, dy, gates, w13, w2, start, dy_start, rows, carried):
    n_src, n_tok, model = x.shape
    n_local, ffn = w2.shape[:2]
    tile = min(TILE_A, rows)
    steps, base = rows // tile, start // tile
    n_exp = gates.shape[2]
    flops = 2 * n_src * rows * n_local * model * ffn * 5
    at = lambda s, t, _: (s, base + t, 0)
    in_specs = [
        pl.BlockSpec((1, tile, model), at),
        pl.BlockSpec((1, tile, model), lambda s, t, _: (s, dy_start // tile + t, 0)),
        pl.BlockSpec((1, tile, n_exp), at),
        pl.BlockSpec(w13.shape, lambda s, t, _: (0, 0, 0), pipeline_mode=pl.Buffered(1)),
        pl.BlockSpec(w2.shape, lambda s, t, _: (0, 0, 0), pipeline_mode=pl.Buffered(1)),
    ]
    operands = [x, dy, gates, w13, w2]
    aliases = {}
    if carried is not None:
        in_specs += [pl.BlockSpec(memory_space=pl.ANY)] * 2
        operands += list(carried)
        aliases = {6: 1, 7: 2}
    return pl.pallas_call(
        functools.partial(bwd_body, ffn, n_local),
        grid_spec=pltpu.PrefetchScalarGridSpec(
            num_scalar_prefetch=1,
            grid=(n_src, steps),
            in_specs=in_specs,
            out_specs=[
                pl.BlockSpec((1, tile, model), lambda s, t, _: (s, t, 0)),
                pl.BlockSpec((1, tile, 2 * ffn * n_local), at),
                pl.BlockSpec((1, tile, ffn * n_local), at),
            ],
        ),
        out_shape=[
            jax.ShapeDtypeStruct((n_src, rows, model), F32),
            jax.ShapeDtypeStruct((n_src, n_tok, 2 * ffn * n_local), BF16),
            jax.ShapeDtypeStruct((n_src, n_tok, ffn * n_local), BF16),
        ],
        input_output_aliases=aliases,
        compiler_params=params(('arbitrary', 'arbitrary')),
        cost_estimate=pl.CostEstimate(flops=flops, bytes_accessed=n_src * rows * model * 14, transcendentals=0),
        name='expert_bwd',
    )(first, *operands)


def grad_body(ffn, first_ref, x_ref, lo_ref, hi_ref, g_ref, da_ref, h_ref, dw1_ref, dw3_ref, dw2_ref, acc13_ref, acc2_ref):
    e, k = pl.program_id(0), pl.program_id(1)
    half = lo_ref.shape[1]

    @pl.when(k == 0)
    def _():
        acc13_ref[...] = jnp.zeros_like(acc13_ref)
        acc2_ref[...] = jnp.zeros_like(acc2_ref)

    acc13_ref[...] += dot_a(x_ref[0], da_ref[0])
    gate = gate_column(g_ref[0], first_ref[0] + e)
    for part, dy_ref in enumerate((lo_ref, hi_ref)):
        rows = slice(part * half, (part + 1) * half)
        d_out = (gate[rows] * dy_ref[0].astype(F32)).astype(BF16)
        acc2_ref[...] += dot_a(h_ref[0, rows], d_out)

    @pl.when(k == pl.num_programs(1) - 1)
    def _():
        dw1_ref[0] = acc13_ref[:, :ffn].astype(BF16)
        dw3_ref[0] = acc13_ref[:, ffn:].astype(BF16)
        dw2_ref[0] = acc2_ref[...].astype(BF16)


def weight_grads(first, x, dy_lo, dy_hi, gates, d_pre, hidden, n_local):
    n_src, n_tok, model = x.shape
    ffn = hidden.shape[2] // n_local
    half = dy_lo.shape[1]
    n_exp = gates.shape[2]
    flops = 2 * n_src * n_tok * n_local * model * ffn * 3
    at = lambda e, k, _: (k, 0, 0)
    at_e = lambda e, k, _: (k, 0, e)
    out = lambda e, k, _: (e, 0, 0)
    return pl.pallas_call(
        functools.partial(grad_body, ffn),
        grid_spec=pltpu.PrefetchScalarGridSpec(
            num_scalar_prefetch=1,
            grid=(n_local, n_src),
            in_specs=[
                pl.BlockSpec((1, n_tok, model), at),
                pl.BlockSpec((1, half, model), at),
                pl.BlockSpec((1, half, model), at),
                pl.BlockSpec((1, n_tok, n_exp), at),
                pl.BlockSpec((1, n_tok, 2 * ffn), at_e),
                pl.BlockSpec((1, n_tok, ffn), at_e),
            ],
            out_specs=[
                pl.BlockSpec((1, model, ffn), out),
                pl.BlockSpec((1, model, ffn), out),
                pl.BlockSpec((1, ffn, model), out),
            ],
            scratch_shapes=[pltpu.VMEM((model, 2 * ffn), F32), pltpu.VMEM((ffn, model), F32)],
        ),
        out_shape=[
            jax.ShapeDtypeStruct((n_local, model, ffn), BF16),
            jax.ShapeDtypeStruct((n_local, model, ffn), BF16),
            jax.ShapeDtypeStruct((n_local, ffn, model), BF16),
        ],
        compiler_params=params(('arbitrary', 'arbitrary')),
        cost_estimate=pl.CostEstimate(flops=flops, bytes_accessed=n_src * n_tok * model * 4 * n_local, transcendentals=0),
        name='weight_grads',
    )(first, x, dy_lo, dy_hi, gates, d_pre, hidden)


def solution(mesh):
    n_stage = mesh.shape['stage']
    n_dev = mesh.shape['expert']
    to_next = [(stage_idx, (stage_idx + 1) % n_stage) for stage_idx in range(n_stage)]
    to_prev = [((stage_idx + 1) % n_stage, stage_idx) for stage_idx in range(n_stage)]
    tok_spec = P('stage', 'expert', None)
    w_spec = P('stage', 'expert', None, None)

    def moe_body(x_act, route_idx, route_wts, w_one, w_three, w_two, dy_act):
        x_src = x_act[0]
        n_tok, _ = x_src.shape
        n_local = w_one.shape[1]
        n_exp = n_local * n_dev
        first = (lax.axis_index('expert') * n_local).astype(jnp.int32).reshape(1)

        hits = route_idx[0][:, :, None] == jnp.arange(n_exp, dtype=jnp.int32)
        gate_src = jnp.sum(jnp.where(hits, route_wts[0][:, :, None], 0.0), axis=1)
        gate_dst = lax.ppermute(gate_src, 'stage', to_next)
        gates = lax.all_gather(gate_dst, 'expert', axis=0, tiled=False)

        w13 = jnp.concatenate([w_one[0], w_three[0]], axis=2)
        w2 = w_two[0]

        half = n_tok // 2
        dy_lo = lax.all_gather(dy_act[0, :half], 'expert', axis=0, tiled=False)

        y_parts = []
        start = 0
        y_part = None
        for rows in FWD_CHUNKS:
            x_dst = lax.ppermute(x_src[start:start + rows], 'stage', to_next)
            x_all = lax.all_gather(x_dst, 'expert', axis=0, tiled=False)
            if y_part is None:
                x_first = x_all
            else:
                x_all, _ = lax.optimization_barrier((x_all, y_part))
            y_part = expert_fwd(first, x_all, gates, w13, w2, start)
            y_parts.append(lax.psum_scatter(y_part, 'expert', scatter_dimension=0, tiled=False).astype(BF16))
            start += rows
        y_out = jnp.concatenate(y_parts, axis=0)

        dy_hi = lax.all_gather(dy_act[0, half:], 'expert', axis=0, tiled=False)
        x_again, _ = lax.optimization_barrier((x_src, x_first))
        x_dst = lax.ppermute(x_again, 'stage', to_next)
        x_all = lax.all_gather(x_dst, 'expert', axis=0, tiled=False)
        x_all, _ = lax.optimization_barrier((x_all, y_part))

        dx_parts = []
        carried = None
        start = 0
        for rows in BWD_CHUNKS:
            dx_part, d_pre, hidden = expert_bwd(first, x_all, dy_lo if start < half else dy_hi, gates, w13, w2, start, start % half, rows, carried)
            carried = (d_pre, hidden)
            dx_dst = lax.psum_scatter(dx_part, 'expert', scatter_dimension=0, tiled=False).astype(BF16)
            dx_parts.append(lax.ppermute(dx_dst, 'stage', to_prev))
            start += rows
        dx_out = jnp.concatenate(dx_parts, axis=0)

        g_one, g_three, g_two = weight_grads(first, x_all, dy_lo, dy_hi, gates, d_pre, hidden, n_local)
        return y_out[None], dx_out[None], g_one[None], g_three[None], g_two[None]

    return jax.shard_map(moe_body, mesh=mesh, in_specs=(tok_spec, tok_spec, tok_spec, w_spec, w_spec, w_spec, tok_spec), out_specs=(tok_spec, tok_spec, w_spec, w_spec, w_spec), check_vma=False)
```

```python
import functools

import jax
import jax.numpy as jnp
from jax import lax
from jax.experimental import pallas as pl
from jax.experimental.pallas import tpu as pltpu
from jax.sharding import PartitionSpec as P


F32 = jnp.float32
BF16 = jnp.bfloat16
FWD_CHUNKS = (256, 768)
BWD_CHUNKS = (512, 256, 256)
TILE_F = 256
TILE_A = 512
VMEM_LIMIT = 65400 * 1024
N_ACC = 3
CORES = 2
MESH = pl.DeviceIdType.MESH


def dot(lhs, rhs):
    return jnp.dot(lhs, rhs, preferred_element_type=F32)


def dot_t(lhs, rhs):
    return lax.dot_general(lhs, rhs, (((1,), (1,)), ((), ())), preferred_element_type=F32)


def dot_a(lhs, rhs):
    return lax.dot_general(lhs, rhs, (((0,), (0,)), ((), ())), preferred_element_type=F32)


def gate_column(gates, expert):
    lanes = lax.broadcasted_iota(jnp.int32, gates.shape, 1)
    return jnp.sum(jnp.where(lanes == expert, gates, 0.0), axis=1, keepdims=True)


def pair_source(step, half, steps):
    core = lax.rem(lax.axis_index('expert'), CORES)
    mine = step // half
    tile = lax.rem(step, half)
    lane = lax.rem(core + 1 + mine, CORES)
    return CORES * (tile // steps) + lane, lax.rem(tile, steps)


def pair_sum(compute, half, steps, tile, inbox_ref, out_ref, acc_ref, send_sem, recv_sem, in_sem, out_sem):
    step = pl.program_id(0)
    last = 2 * half - 1
    me = lax.axis_index('expert')
    other = me + 1 - 2 * lax.rem(me, CORES)

    def at(ref, job):
        return ref.at[job // steps, pl.ds(lax.rem(job, steps) * tile, tile)]

    def send(job):
        slot = lax.rem(job, N_ACC)
        return pltpu.make_async_remote_copy(
            src_ref=acc_ref.at[slot], dst_ref=at(inbox_ref, job), send_sem=send_sem.at[slot], recv_sem=recv_sem.at[job],
            device_id={'expert': other}, device_id_type=MESH)

    def fetch(job):
        slot = lax.rem(job + half, N_ACC)
        return pltpu.make_async_copy(at(inbox_ref, job), acc_ref.at[slot], in_sem.at[slot])

    def store(job):
        slot = lax.rem(job + half, N_ACC)
        return pltpu.make_async_copy(acc_ref.at[slot], at(out_ref, job), out_sem.at[slot])

    @pl.when(step == 0)
    def _():
        barrier = pltpu.get_barrier_semaphore()
        pl.semaphore_signal(barrier, inc=1, device_id={'expert': other}, device_id_type=MESH)
        pl.semaphore_wait(barrier, 1)

    back = step - (N_ACC - 1)

    @pl.when((back >= 0) & (back < half))
    def _():
        send(back).wait_send()

    @pl.when(back >= half)
    def _():
        store(back - half).wait()

    ahead = step + 1 - half

    @pl.when((ahead >= 0) & (ahead < half))
    def _():
        send(ahead).wait_recv()
        fetch(ahead).start()

    acc = acc_ref.at[lax.rem(step, N_ACC)]

    @pl.when(step < half)
    def _():
        acc[...] = jnp.zeros_like(acc)

    @pl.when(step >= half)
    def _():
        fetch(step - half).wait()

    compute(acc)

    @pl.when(step < half)
    def _():
        send(step).start()

    @pl.when(step >= half)
    def _():
        store(step - half).start()

    @pl.when(step == last)
    def _():
        for job in range(half - N_ACC + 1, half):
            store(job).wait()


def fwd_body(ffn, n_local, half, steps, x_ref, g_ref, w13_ref, w2_ref, y_ref, inbox_ref, *scratch):
    tile = x_ref.shape[1]

    def compute(acc):
        for e in range(n_local):
            gate = gate_column(g_ref[0], e)
            pre = dot(x_ref[0], w13_ref[e])
            one, three = pre[:, :ffn], pre[:, ffn:]
            hidden = jnp.where(gate > 0.0, one * jax.nn.sigmoid(one) * three, 0.0).astype(BF16)
            acc[...] += gate * dot(hidden, w2_ref[e]).astype(BF16).astype(F32)

    pair_sum(compute, half, steps, tile, inbox_ref, y_ref, *scratch)


def pair_scratch(tile, model, half):
    return [
        pltpu.VMEM((N_ACC, tile, model), F32),
        pltpu.SemaphoreType.DMA((N_ACC,)),
        pltpu.SemaphoreType.DMA((half,)),
        pltpu.SemaphoreType.DMA((N_ACC,)),
        pltpu.SemaphoreType.DMA((N_ACC,)),
    ]


def whole(array):
    return pl.BlockSpec(array.shape, lambda i: (0,) * array.ndim, pipeline_mode=pl.Buffered(1))


def expert_fwd(x, gates, w13, w2, start, collective_id):
    n_src, rows, model = x.shape
    n_local, ffn = w2.shape[:2]
    tile = min(TILE_F, rows)
    steps = rows // tile
    n_own = n_src // CORES
    half = n_own * steps
    flops = 2 * n_src * rows * n_local * model * ffn * 3

    def at(base):
        def index(i):
            src, t = pair_source(i, half, steps)
            return src, base // tile + t, 0

        return index

    part = jax.ShapeDtypeStruct((n_own, rows, model), F32)
    return pl.pallas_call(
        functools.partial(fwd_body, ffn, n_local, half, steps),
        grid=(2 * half,),
        in_specs=[
            pl.BlockSpec((1, tile, model), at(0)),
            pl.BlockSpec((1, tile, n_local), at(start)),
            whole(w13),
            whole(w2),
        ],
        out_specs=[pl.BlockSpec(memory_space=pl.ANY)] * 2,
        out_shape=[part, part],
        scratch_shapes=pair_scratch(tile, model, half),
        compiler_params=pltpu.CompilerParams(
            dimension_semantics=('arbitrary',), vmem_limit_bytes=VMEM_LIMIT, collective_id=collective_id, has_side_effects=True),
        cost_estimate=pl.CostEstimate(flops=flops, bytes_accessed=n_src * rows * model * 6, transcendentals=0),
        name='expert_fwd',
    )(x, gates, w13, w2)[0]


def bwd_body(ffn, n_local, half, steps, n_carried, x_ref, dy_ref, g_ref, w13_ref, w2_ref, *refs):
    dx_ref, inbox_ref, da_ref, h_ref = refs[n_carried:n_carried + 4]
    tile = x_ref.shape[1]

    def compute(acc):
        def expert(e, carry):
            gate = gate_column(g_ref[0], e)
            live = gate > 0.0
            pre = dot(x_ref[0], w13_ref[e])
            one, three = pre[:, :ffn], pre[:, ffn:]
            sig = jax.nn.sigmoid(one)
            act = one * sig
            h_ref[0, :, pl.ds(pl.multiple_of(e * ffn, ffn), ffn)] = jnp.where(live, act * three, 0.0).astype(BF16)
            d_out = (gate * dy_ref[0].astype(F32)).astype(BF16)
            d_hid = dot_t(d_out, w2_ref[e]).astype(BF16).astype(F32)
            d_one = jnp.where(live, d_hid * three * sig * (1.0 + one * (1.0 - sig)), 0.0).astype(BF16)
            d_three = jnp.where(live, d_hid * act, 0.0).astype(BF16)
            d_pre = jnp.concatenate([d_one, d_three], axis=1)
            da_ref[0, :, pl.ds(pl.multiple_of(2 * e * ffn, 2 * ffn), 2 * ffn)] = d_pre
            acc[...] += dot_t(d_pre, w13_ref[e]).astype(BF16).astype(F32)
            return carry

        lax.fori_loop(0, n_local, expert, 0)

    pair_sum(compute, half, steps, tile, inbox_ref, dx_ref, *refs[n_carried + 4:])


def expert_bwd(x, dy, gates, w13, w2, start, rows, carried, collective_id):
    n_src, n_tok, model = x.shape
    n_local, ffn = w2.shape[:2]
    tile = min(TILE_A, rows)
    steps = rows // tile
    n_own = n_src // CORES
    half = n_own * steps
    flops = 2 * n_src * rows * n_local * model * ffn * 5

    def at(i):
        src, t = pair_source(i, half, steps)
        return src, start // tile + t, 0

    hbm = pl.BlockSpec(memory_space=pl.ANY)
    part = jax.ShapeDtypeStruct((n_own, rows, model), F32)
    outs = pl.pallas_call(
        functools.partial(bwd_body, ffn, n_local, half, steps, len(carried)),
        grid=(2 * half,),
        in_specs=[
            pl.BlockSpec((1, tile, model), at),
            pl.BlockSpec((1, tile, model), at),
            pl.BlockSpec((1, tile, n_local), at),
            whole(w13),
            whole(w2),
        ] + [hbm] * len(carried),
        out_specs=[
            hbm,
            hbm,
            pl.BlockSpec((1, tile, 2 * ffn * n_local), at),
            pl.BlockSpec((1, tile, ffn * n_local), at),
        ],
        out_shape=[
            part,
            part,
            jax.ShapeDtypeStruct((n_src, n_tok, 2 * ffn * n_local), BF16),
            jax.ShapeDtypeStruct((n_src, n_tok, ffn * n_local), BF16),
        ],
        scratch_shapes=pair_scratch(tile, model, half),
        input_output_aliases={5 + i: 2 + i for i in range(len(carried))},
        compiler_params=pltpu.CompilerParams(
            dimension_semantics=('arbitrary',), vmem_limit_bytes=VMEM_LIMIT, collective_id=collective_id, has_side_effects=True),
        cost_estimate=pl.CostEstimate(flops=flops, bytes_accessed=n_src * rows * model * 14, transcendentals=0),
        name='expert_bwd',
    )(x, dy, gates, w13, w2, *carried)
    return outs[0], outs[2:]


def grad_body(ffn, x_ref, dy_ref, g_ref, da_ref, h_ref, dw1_ref, dw3_ref, dw2_ref, acc13_ref, acc2_ref):
    e, k = pl.program_id(0), pl.program_id(1)

    @pl.when(k == 0)
    def _():
        acc13_ref[...] = jnp.zeros_like(acc13_ref)
        acc2_ref[...] = jnp.zeros_like(acc2_ref)

    acc13_ref[...] += dot_a(x_ref[0], da_ref[0])
    d_out = (gate_column(g_ref[0], e) * dy_ref[0].astype(F32)).astype(BF16)
    acc2_ref[...] += dot_a(h_ref[0], d_out)

    @pl.when(k == pl.num_programs(1) - 1)
    def _():
        dw1_ref[0] = acc13_ref[:, :ffn].astype(BF16)
        dw3_ref[0] = acc13_ref[:, ffn:].astype(BF16)
        dw2_ref[0] = acc2_ref[...].astype(BF16)


def weight_grads(x, dy, gates, d_pre, hidden):
    n_src, n_tok, model = x.shape
    n_local = gates.shape[2]
    ffn = hidden.shape[2] // n_local
    flops = 2 * n_src * n_tok * n_local * model * ffn * 3
    at = lambda e, k: (k, 0, 0)
    at_e = lambda e, k: (k, 0, e)
    out = lambda e, k: (e, 0, 0)
    return pl.pallas_call(
        functools.partial(grad_body, ffn),
        grid=(n_local, n_src),
        in_specs=[
            pl.BlockSpec((1, n_tok, model), at),
            pl.BlockSpec((1, n_tok, model), at),
            pl.BlockSpec((1, n_tok, n_local), at),
            pl.BlockSpec((1, n_tok, 2 * ffn), at_e),
            pl.BlockSpec((1, n_tok, ffn), at_e),
        ],
        out_specs=[
            pl.BlockSpec((1, model, ffn), out),
            pl.BlockSpec((1, model, ffn), out),
            pl.BlockSpec((1, ffn, model), out),
        ],
        out_shape=[
            jax.ShapeDtypeStruct((n_local, model, ffn), BF16),
            jax.ShapeDtypeStruct((n_local, model, ffn), BF16),
            jax.ShapeDtypeStruct((n_local, ffn, model), BF16),
        ],
        scratch_shapes=[pltpu.VMEM((model, 2 * ffn), F32), pltpu.VMEM((ffn, model), F32)],
        compiler_params=pltpu.CompilerParams(dimension_semantics=('arbitrary', 'arbitrary'), vmem_limit_bytes=VMEM_LIMIT),
        cost_estimate=pl.CostEstimate(flops=flops, bytes_accessed=n_src * n_tok * model * 4 * n_local, transcendentals=0),
        name='weight_grads',
    )(x, dy, gates, d_pre, hidden)


def solution(mesh):
    n_stage = mesh.shape['stage']
    n_dev = mesh.shape['expert']
    to_next = [(stage_idx, (stage_idx + 1) % n_stage) for stage_idx in range(n_stage)]
    to_prev = [((stage_idx + 1) % n_stage, stage_idx) for stage_idx in range(n_stage)]
    tok_spec = P('stage', 'expert', None)
    w_spec = P('stage', 'expert', None, None)
    same_core = [list(range(core, n_dev, CORES)) for core in range(CORES)]
    n_fwd = len(FWD_CHUNKS)

    def moe_body(x_act, route_idx, route_wts, w_one, w_three, w_two, dy_act):
        x_src = x_act[0]
        n_tok, _ = x_src.shape
        n_local = w_one.shape[1]
        n_exp = n_local * n_dev

        def gather(rows):
            return lax.all_gather(rows, 'expert', axis=0, tiled=False)

        def reduce_rows(part):
            return lax.psum_scatter(part, 'expert', scatter_dimension=0, axis_index_groups=same_core, tiled=False).astype(BF16)

        dy_all = gather(dy_act[0])

        hits = route_idx[0][:, :, None] == jnp.arange(n_exp, dtype=jnp.int32)
        gate_src = jnp.sum(jnp.where(hits, route_wts[0][:, :, None], 0.0), axis=1)
        gate_src = jnp.transpose(gate_src.reshape(n_tok, n_dev, n_local), (1, 2, 0))
        gate_dst = lax.ppermute(gate_src, 'stage', to_next)
        gates = jnp.transpose(lax.all_to_all(gate_dst, 'expert', 0, 0), (0, 2, 1))

        w13 = jnp.concatenate([w_one[0], w_three[0]], axis=2)
        w2 = w_two[0]

        y_parts = []
        start = 0
        y_part = None
        for k, rows in enumerate(FWD_CHUNKS):
            x_dst = lax.ppermute(x_src[start:start + rows], 'stage', to_next)
            x_all = gather(x_dst)
            if y_part is None:
                x_first = x_all
            else:
                x_all, _ = lax.optimization_barrier((x_all, y_part))
            y_part = expert_fwd(x_all, gates, w13, w2, start, k)
            y_parts.append(reduce_rows(y_part))
            start += rows
        y_out = jnp.concatenate(y_parts, axis=0)

        x_again, _ = lax.optimization_barrier((x_src, x_first))
        x_dst = lax.ppermute(x_again, 'stage', to_next)
        x_all = gather(x_dst)
        x_all, _ = lax.optimization_barrier((x_all, y_part))

        dx_parts = []
        carried = ()
        start = 0
        for k, rows in enumerate(BWD_CHUNKS):
            dx_part, carried = expert_bwd(x_all, dy_all, gates, w13, w2, start, rows, carried, n_fwd + k)
            dx_dst = reduce_rows(dx_part)
            dx_parts.append(lax.ppermute(dx_dst, 'stage', to_prev))
            start += rows
        dx_out = jnp.concatenate(dx_parts, axis=0)

        g_one, g_three, g_two = weight_grads(x_all, dy_all, gates, *carried)
        return y_out[None], dx_out[None], g_one[None], g_three[None], g_two[None]

    return jax.shard_map(moe_body, mesh=mesh, in_specs=(tok_spec, tok_spec, tok_spec, w_spec, w_spec, w_spec, tok_spec), out_specs=(tok_spec, tok_spec, w_spec, w_spec, w_spec), check_vma=False)
```

```python
import functools

import jax
import jax.numpy as jnp
from jax import lax
from jax.experimental import pallas as pl
from jax.experimental.pallas import tpu as pltpu
from jax.sharding import PartitionSpec as P


F32 = jnp.float32
BF16 = jnp.bfloat16
FWD_CHUNKS = ((384, 384), (640, 320))
BWD_TILE = 512
DX_SPLIT = 768
VMEM_LIMIT = 65400 * 1024
N_ACC = 3
CORES = 2
MESH = pl.DeviceIdType.MESH


def dot(lhs, rhs):
    return jnp.dot(lhs, rhs, preferred_element_type=F32)


def dot_t(lhs, rhs):
    return lax.dot_general(lhs, rhs, (((1,), (1,)), ((), ())), preferred_element_type=F32)


def dot_a(lhs, rhs):
    return lax.dot_general(lhs, rhs, (((0,), (0,)), ((), ())), preferred_element_type=F32)


def gate_column(gates, expert):
    lanes = lax.broadcasted_iota(jnp.int32, gates.shape, 1)
    return jnp.sum(jnp.where(lanes == expert, gates, 0.0), axis=1, keepdims=True)


def pair_source(step, half, steps):
    core = lax.rem(lax.axis_index('expert'), CORES)
    mine = step // half
    tile = lax.rem(step, half)
    lane = lax.rem(core + 1 + mine, CORES)
    return CORES * (tile // steps) + lane, lax.rem(tile, steps)


def pair_sum(compute, half, steps, tile, inbox_ref, pieces, acc_ref, send_sem, recv_sem, in_sem, out_sem):
    step = pl.program_id(0)
    last = 2 * half - 1
    me = lax.axis_index('expert')
    other = me + 1 - 2 * lax.rem(me, CORES)

    def at(ref, job):
        return ref.at[job // steps, pl.ds(lax.rem(job, steps) * tile, tile)]

    class Store:
        def __init__(self, job):
            slot = lax.rem(job + half, N_ACC)
            self.copies = [
                pltpu.make_async_copy(
                    acc_ref.at[slot, pl.ds(row, rows)],
                    out_ref.at[job // steps, pl.ds(first + lax.rem(job, steps) * tile, rows)],
                    out_sem.at[slot, k])
                for k, (out_ref, first, row, rows) in enumerate(pieces)]

        def start(self):
            for copy in self.copies:
                copy.start()

        def wait(self):
            for copy in self.copies:
                copy.wait()

    def send(job):
        slot = lax.rem(job, N_ACC)
        return pltpu.make_async_remote_copy(
            src_ref=acc_ref.at[slot], dst_ref=at(inbox_ref, job), send_sem=send_sem.at[slot], recv_sem=recv_sem.at[job],
            device_id={'expert': other}, device_id_type=MESH)

    def fetch(job):
        slot = lax.rem(job + half, N_ACC)
        return pltpu.make_async_copy(at(inbox_ref, job), acc_ref.at[slot], in_sem.at[slot])

    @pl.when(step == 0)
    def _():
        barrier = pltpu.get_barrier_semaphore()
        pl.semaphore_signal(barrier, inc=1, device_id={'expert': other}, device_id_type=MESH)
        pl.semaphore_wait(barrier, 1)

    back = step - (N_ACC - 1)

    @pl.when((back >= 0) & (back < half))
    def _():
        send(back).wait_send()

    @pl.when(back >= half)
    def _():
        Store(back - half).wait()

    ahead = step + 1 - half

    @pl.when((ahead >= 0) & (ahead < half))
    def _():
        send(ahead).wait_recv()
        fetch(ahead).start()

    acc = acc_ref.at[lax.rem(step, N_ACC)]

    @pl.when(step < half)
    def _():
        acc[...] = jnp.zeros_like(acc)

    @pl.when(step >= half)
    def _():
        fetch(step - half).wait()

    compute(acc)

    @pl.when(step < half)
    def _():
        send(step).start()

    @pl.when(step >= half)
    def _():
        Store(step - half).start()

    @pl.when(step == last)
    def _():
        for job in range(half - N_ACC + 1, half):
            Store(job).wait()


def fwd_body(ffn, n_local, half, steps, start, n_carried, x_ref, g_ref, w13_ref, w2_ref, *refs):
    y_ref, inbox_ref = refs[n_carried:n_carried + 2]
    tile = x_ref.shape[1]

    def compute(acc):
        for e in range(n_local):
            gate = gate_column(g_ref[0], e)
            pre = dot(x_ref[0], w13_ref[e])
            one, three = pre[:, :ffn], pre[:, ffn:]
            hidden = jnp.where(gate > 0.0, one * jax.nn.sigmoid(one) * three, 0.0).astype(BF16)
            acc[...] += gate * dot(hidden, w2_ref[e]).astype(BF16).astype(F32)

    pair_sum(compute, half, steps, tile, inbox_ref, [(y_ref, start, 0, tile)], *refs[n_carried + 2:])


def pair_scratch(tile, model, half, n_pieces):
    return [
        pltpu.VMEM((N_ACC, tile, model), F32),
        pltpu.SemaphoreType.DMA((N_ACC,)),
        pltpu.SemaphoreType.DMA((half,)),
        pltpu.SemaphoreType.DMA((N_ACC,)),
        pltpu.SemaphoreType.DMA((N_ACC, n_pieces)),
    ]


def pair_params(collective_id):
    return pltpu.CompilerParams(
        dimension_semantics=('arbitrary',), vmem_limit_bytes=VMEM_LIMIT, collective_id=collective_id, has_side_effects=True)


def whole(array):
    return pl.BlockSpec(array.shape, lambda i: (0,) * array.ndim, pipeline_mode=pl.Buffered(1))


HBM = pl.BlockSpec(memory_space=pl.ANY)


def expert_fwd(x, gates, w13, w2, tile, start, n_tok, carried, collective_id):
    n_src, rows, model = x.shape
    n_local, ffn = w2.shape[:2]
    steps = rows // tile
    n_own = n_src // CORES
    half = n_own * steps
    flops = 2 * n_src * rows * n_local * model * ffn * 3

    def at(i):
        src, t = pair_source(i, half, steps)
        return src, t, 0

    return pl.pallas_call(
        functools.partial(fwd_body, ffn, n_local, half, steps, start, len(carried)),
        grid=(2 * half,),
        in_specs=[
            pl.BlockSpec((1, tile, model), at),
            pl.BlockSpec((1, tile, n_local), at),
            whole(w13),
            whole(w2),
        ] + [HBM] * len(carried),
        out_specs=[HBM, HBM],
        out_shape=[jax.ShapeDtypeStruct((n_own, n_tok, model), F32), jax.ShapeDtypeStruct((n_own, rows, model), F32)],
        scratch_shapes=pair_scratch(tile, model, half, 1),
        input_output_aliases={4 + i: i for i in range(len(carried))},
        compiler_params=pair_params(collective_id),
        cost_estimate=pl.CostEstimate(flops=flops, bytes_accessed=n_src * rows * model * 6, transcendentals=0),
        name='expert_fwd',
    )(x, gates, w13, w2, *carried)[0]


def bwd_body(ffn, n_local, half, steps, pieces, n_carried, x_ref, dy_ref, g_ref, w13_ref, w2_ref, *refs):
    lo_ref, hi_ref, da_ref, h_ref, inbox_ref = refs[n_carried:n_carried + 5]
    tile = x_ref.shape[2]

    def compute(acc):
        def expert(e, carry):
            gate = gate_column(g_ref[0], e)
            live = gate > 0.0
            pre = dot(x_ref[0, 0], w13_ref[e])
            one, three = pre[:, :ffn], pre[:, ffn:]
            sig = jax.nn.sigmoid(one)
            act = one * sig
            h_ref[0, :, pl.ds(pl.multiple_of(e * ffn, ffn), ffn)] = jnp.where(live, act * three, 0.0).astype(BF16)
            d_out = (gate * dy_ref[0, 0].astype(F32)).astype(BF16)
            d_hid = dot_t(d_out, w2_ref[e]).astype(BF16).astype(F32)
            d_one = jnp.where(live, d_hid * three * sig * (1.0 + one * (1.0 - sig)), 0.0).astype(BF16)
            d_three = jnp.where(live, d_hid * act, 0.0).astype(BF16)
            d_pre = jnp.concatenate([d_one, d_three], axis=1)
            da_ref[0, :, pl.ds(pl.multiple_of(2 * e * ffn, 2 * ffn), 2 * ffn)] = d_pre
            acc[...] += dot_t(d_pre, w13_ref[e]).astype(BF16).astype(F32)
            return carry

        lax.fori_loop(0, n_local, expert, 0)

    outs = [((lo_ref, hi_ref)[which], first, row, rows) for which, first, row, rows in pieces]
    pair_sum(compute, half, steps, tile, inbox_ref, outs, *refs[n_carried + 5:])


def expert_bwd(rows_in, gates, w13, w2, start, n_tok, pieces, carried, collective_id):
    n_src, _, rows, model = rows_in.shape
    n_local, ffn = w2.shape[:2]
    tile = min(BWD_TILE, rows)
    steps = rows // tile
    n_own = n_src // CORES
    half = n_own * steps
    flops = 2 * n_src * rows * n_local * model * ffn * 5

    def rows_of(which):
        def index(i):
            src, t = pair_source(i, half, steps)
            return src, which, t, 0

        return index

    def at(i):
        src, t = pair_source(i, half, steps)
        return src, start // tile + t, 0

    outs = pl.pallas_call(
        functools.partial(bwd_body, ffn, n_local, half, steps, pieces, len(carried)),
        grid=(2 * half,),
        in_specs=[
            pl.BlockSpec((1, 1, tile, model), rows_of(1)),
            pl.BlockSpec((1, 1, tile, model), rows_of(0)),
            pl.BlockSpec((1, tile, n_local), at),
            whole(w13),
            whole(w2),
        ] + [HBM] * len(carried),
        out_specs=[
            HBM,
            HBM,
            pl.BlockSpec((1, tile, 2 * ffn * n_local), at),
            pl.BlockSpec((1, tile, ffn * n_local), at),
            HBM,
        ],
        out_shape=[
            jax.ShapeDtypeStruct((n_own, DX_SPLIT, model), F32),
            jax.ShapeDtypeStruct((n_own, n_tok - DX_SPLIT, model), F32),
            jax.ShapeDtypeStruct((n_src, n_tok, 2 * ffn * n_local), BF16),
            jax.ShapeDtypeStruct((n_src, n_tok, ffn * n_local), BF16),
            jax.ShapeDtypeStruct((n_own, rows, model), F32),
        ],
        scratch_shapes=pair_scratch(tile, model, half, len(pieces)),
        input_output_aliases={5 + i: i for i in range(len(carried))},
        compiler_params=pair_params(collective_id),
        cost_estimate=pl.CostEstimate(flops=flops, bytes_accessed=n_src * rows * model * 14, transcendentals=0),
        name='expert_bwd',
    )(rows_in, rows_in, gates, w13, w2, *carried)
    return outs[:4]


def grad_body(ffn, lo_ref, hi_ref, g_ref, da_ref, h_ref, dw1_ref, dw3_ref, dw2_ref, acc13_ref, acc2_ref):
    e, k = pl.program_id(0), pl.program_id(1)

    @pl.when(k == 0)
    def _():
        acc13_ref[...] = jnp.zeros_like(acc13_ref)
        acc2_ref[...] = jnp.zeros_like(acc2_ref)

    acc13_ref[...] += dot_a(jnp.concatenate([lo_ref[0, 1], hi_ref[0, 1]], axis=0), da_ref[0])
    d_out = jnp.concatenate([lo_ref[0, 0], hi_ref[0, 0]], axis=0).astype(F32)
    d_out = (gate_column(g_ref[0], e) * d_out).astype(BF16)
    acc2_ref[...] += dot_a(h_ref[0], d_out)

    @pl.when(k == pl.num_programs(1) - 1)
    def _():
        dw1_ref[0] = acc13_ref[:, :ffn].astype(BF16)
        dw3_ref[0] = acc13_ref[:, ffn:].astype(BF16)
        dw2_ref[0] = acc2_ref[...].astype(BF16)


def weight_grads(lo, hi, gates, d_pre, hidden):
    n_src, n_tok, n_local = gates.shape
    model = lo.shape[3]
    ffn = hidden.shape[2] // n_local
    flops = 2 * n_src * n_tok * n_local * model * ffn * 3
    at = lambda e, k: (k, 0, 0)
    at_e = lambda e, k: (k, 0, e)
    out = lambda e, k: (e, 0, 0)
    return pl.pallas_call(
        functools.partial(grad_body, ffn),
        grid=(n_local, n_src),
        in_specs=[
            pl.BlockSpec((1,) + lo.shape[1:], lambda e, k: (k, 0, 0, 0)),
            pl.BlockSpec((1,) + hi.shape[1:], lambda e, k: (k, 0, 0, 0)),
            pl.BlockSpec((1, n_tok, n_local), at),
            pl.BlockSpec((1, n_tok, 2 * ffn), at_e),
            pl.BlockSpec((1, n_tok, ffn), at_e),
        ],
        out_specs=[
            pl.BlockSpec((1, model, ffn), out),
            pl.BlockSpec((1, model, ffn), out),
            pl.BlockSpec((1, ffn, model), out),
        ],
        out_shape=[
            jax.ShapeDtypeStruct((n_local, model, ffn), BF16),
            jax.ShapeDtypeStruct((n_local, model, ffn), BF16),
            jax.ShapeDtypeStruct((n_local, ffn, model), BF16),
        ],
        scratch_shapes=[pltpu.VMEM((model, 2 * ffn), F32), pltpu.VMEM((ffn, model), F32)],
        compiler_params=pltpu.CompilerParams(dimension_semantics=('arbitrary', 'arbitrary'), vmem_limit_bytes=VMEM_LIMIT),
        cost_estimate=pl.CostEstimate(flops=flops, bytes_accessed=n_src * n_tok * model * 4 * n_local, transcendentals=0),
        name='weight_grads',
    )(lo, hi, gates, d_pre, hidden)


def solution(mesh):
    n_stage = mesh.shape['stage']
    n_dev = mesh.shape['expert']
    to_next = [(stage_idx, (stage_idx + 1) % n_stage) for stage_idx in range(n_stage)]
    to_prev = [((stage_idx + 1) % n_stage, stage_idx) for stage_idx in range(n_stage)]
    tok_spec = P('stage', 'expert', None)
    w_spec = P('stage', 'expert', None, None)
    same_core = [list(range(core, n_dev, CORES)) for core in range(CORES)]
    n_fwd = len(FWD_CHUNKS)

    def moe_body(x_act, route_idx, route_wts, w_one, w_three, w_two, dy_act):
        x_src = x_act[0]
        n_tok, _ = x_src.shape
        n_local = w_one.shape[1]
        n_exp = n_local * n_dev

        def gather(rows):
            return lax.all_gather(rows, 'expert', axis=0, tiled=False)

        def reduce_rows(part):
            return lax.psum_scatter(part, 'expert', scatter_dimension=0, axis_index_groups=same_core, tiled=False).astype(BF16)

        hits = route_idx[0][:, :, None] == jnp.arange(n_exp, dtype=jnp.int32)
        gate_src = jnp.sum(jnp.where(hits, route_wts[0][:, :, None], 0.0), axis=1)
        gate_src = jnp.transpose(gate_src.reshape(n_tok, n_dev, n_local), (1, 2, 0))
        gate_dst = lax.ppermute(gate_src, 'stage', to_next)
        gates = jnp.transpose(lax.all_to_all(gate_dst, 'expert', 0, 0), (0, 2, 1))

        w13 = jnp.concatenate([w_one[0], w_three[0]], axis=2)
        w2 = w_two[0]

        half = n_tok // 2
        carried = ()
        start = 0
        for k, (rows, tile) in enumerate(FWD_CHUNKS):
            x_dst = lax.ppermute(x_src[start:start + rows], 'stage', to_next)
            x_all = gather(x_dst)
            if k == 0:
                x_first = x_all
            y_part = expert_fwd(x_all, gates[:, start:start + rows], w13, w2, tile, start, n_tok, carried, k)
            carried = (y_part,)
            start += rows
        y_out = reduce_rows(y_part)

        x_again, _ = lax.optimization_barrier((x_src, x_first))
        both = []
        for rows in (slice(0, half), slice(half, n_tok)):
            x_dst = lax.ppermute(x_again[rows], 'stage', to_next)
            both.append(gather(jnp.stack([dy_act[0, rows], x_dst])))
        lo, hi = both

        lo_now, _ = lax.optimization_barrier((lo, y_part))
        carried = expert_bwd(lo_now, gates, w13, w2, 0, n_tok, [(0, 0, 0, half)], (), n_fwd)
        cut = DX_SPLIT - half
        carried = expert_bwd(hi, gates, w13, w2, half, n_tok, [(0, half, 0, cut), (1, 0, cut, half - cut)], carried, n_fwd + 1)
        dx_parts = []
        for k in range(2):
            dx_dst = reduce_rows(carried[k])
            dx_parts.append(lax.ppermute(dx_dst, 'stage', to_prev))
        dx_out = jnp.concatenate(dx_parts, axis=0)

        g_one, g_three, g_two = weight_grads(lo, hi, gates, *carried[2:])
        return y_out[None], dx_out[None], g_one[None], g_three[None], g_two[None]

    return jax.shard_map(moe_body, mesh=mesh, in_specs=(tok_spec, tok_spec, tok_spec, w_spec, w_spec, w_spec, tok_spec), out_specs=(tok_spec, tok_spec, w_spec, w_spec, w_spec), check_vma=False)
```

```python
import functools

import jax
import jax.numpy as jnp
from jax import lax
from jax.experimental import pallas as pl
from jax.experimental.pallas import tpu as pltpu
from jax.sharding import PartitionSpec as P


F32 = jnp.float32
BF16 = jnp.bfloat16
FWD_CHUNKS = ((256, 256), (768, 256))
FWD_STAGES = (0, 7, 13, 19)
BWD_STAGES = (0, 2, 4, 6)
VMEM_LIMIT = 65400 * 1024
N_ACC = 3
CORES = 2
MESH = pl.DeviceIdType.MESH


def dot(lhs, rhs):
    return jnp.dot(lhs, rhs, preferred_element_type=F32)


def dot_t(lhs, rhs):
    return lax.dot_general(lhs, rhs, (((1,), (1,)), ((), ())), preferred_element_type=F32)


def dot_a(lhs, rhs):
    return lax.dot_general(lhs, rhs, (((0,), (0,)), ((), ())), preferred_element_type=F32)


def gate_column(gates, expert):
    lanes = lax.broadcasted_iota(jnp.int32, gates.shape, 1)
    return jnp.sum(jnp.where(lanes == expert, gates, 0.0), axis=1, keepdims=True)


def pair_source(step, half, steps):
    core = lax.rem(lax.axis_index('expert'), CORES)
    mine = step // half
    tile = lax.rem(step, half)
    lane = lax.rem(core + 1 + mine, CORES)
    return CORES * (tile // steps) + lane, lax.rem(tile, steps)


def pair_sum(compute, half, steps, tile, inbox_ref, pieces, exchange, acc_ref, send_sem, recv_sem, in_sem, out_sem):
    step = pl.program_id(0)
    last = 2 * half - 1
    me = lax.axis_index('expert')
    other = me + 1 - 2 * lax.rem(me, CORES)

    def at(ref, job):
        return ref.at[job // steps, pl.ds(lax.rem(job, steps) * tile, tile)]

    class Store:
        def __init__(self, job):
            slot = lax.rem(job + half, N_ACC)
            self.copies = [
                pltpu.make_async_copy(
                    acc_ref.at[slot, pl.ds(row, rows)],
                    out_ref.at[job // steps, pl.ds(first + lax.rem(job, steps) * tile, rows)],
                    out_sem.at[slot, k])
                for k, (out_ref, first, row, rows) in enumerate(pieces)]

        def start(self):
            for copy in self.copies:
                copy.start()

        def wait(self):
            for copy in self.copies:
                copy.wait()

    def send(job):
        slot = lax.rem(job, N_ACC)
        return pltpu.make_async_remote_copy(
            src_ref=acc_ref.at[slot], dst_ref=at(inbox_ref, job), send_sem=send_sem.at[slot], recv_sem=recv_sem.at[job],
            device_id={'expert': other}, device_id_type=MESH)

    def fetch(job):
        slot = lax.rem(job + half, N_ACC)
        return pltpu.make_async_copy(at(inbox_ref, job), acc_ref.at[slot], in_sem.at[slot])

    @pl.when(step == 0)
    def _():
        peers = [other] + (exchange.peers if exchange else [])
        barrier = pltpu.get_barrier_semaphore()
        for peer in peers:
            pl.semaphore_signal(barrier, inc=1, device_id={'expert': peer}, device_id_type=MESH)
        pl.semaphore_wait(barrier, len(peers))

    if exchange:
        exchange.advance(step)

    back = step - (N_ACC - 1)

    @pl.when((back >= 0) & (back < half))
    def _():
        send(back).wait_send()

    @pl.when(back >= half)
    def _():
        Store(back - half).wait()

    ahead = step + 1 - half

    @pl.when((ahead >= 0) & (ahead < half))
    def _():
        send(ahead).wait_recv()
        fetch(ahead).start()

    acc = acc_ref.at[lax.rem(step, N_ACC)]

    @pl.when(step < half)
    def _():
        acc[...] = jnp.zeros_like(acc)

    @pl.when(step >= half)
    def _():
        fetch(step - half).wait()

    compute(acc)

    @pl.when(step < half)
    def _():
        send(step).start()

    @pl.when(step >= half)
    def _():
        Store(step - half).start()

    @pl.when(step == last)
    def _():
        for job in range(half - N_ACC + 1, half):
            Store(job).wait()
        if exchange:
            exchange.finish()


class Exchange:
    def __init__(self, ref, send_sem, recv_sem, stages):
        me = lax.axis_index('expert')
        flip = lambda dev, bit: dev + bit - 2 * bit * lax.rem(dev // bit, 2)
        core, x, y = flip(me, 1), flip(me, 2), flip(me, 4)
        diag = flip(x, 4)
        self.peers = [x, y]
        self.stages = stages
        rows = ref.shape[1] // 2
        first, second, both = pl.ds(0, rows), pl.ds(rows, rows), pl.ds(0, 2 * rows)
        plan = [
            (first, me, x, x),
            (second, me, y, y),
            (second, me, x, x),
            (first, me, y, y),
            (both, me, core, core),
            (first, x, diag, y),
            (second, y, diag, x),
            (first, x, flip(x, 1), core),
            (second, y, flip(y, 1), core),
            (second, x, flip(x, 1), core),
            (first, y, flip(y, 1), core),
            (first, diag, flip(diag, 1), core),
            (second, diag, flip(diag, 1), core),
        ]

        def copy(k, block):
            part, _, _, to = plan[k]
            return pltpu.make_async_remote_copy(
                src_ref=ref.at[block, part], dst_ref=ref.at[block, part], send_sem=send_sem.at[k], recv_sem=recv_sem.at[k],
                device_id={'expert': to}, device_id_type=MESH)

        self.out = [copy(k, plan[k][1]) for k in range(len(plan))]
        self.into = [copy(k, plan[k][2]) for k in range(len(plan))]

    def advance(self, step):
        for at, arrived, started in zip(self.stages, ((), (0, 1), (2, 3), (5, 6)), ((0, 1, 2, 3, 4), (5, 6, 7, 8), (9, 10), (11, 12))):
            @pl.when(step == at)
            def _(arrived=arrived, started=started):
                for k in arrived:
                    self.into[k].wait_recv()
                for k in started:
                    self.out[k].start()

    def finish(self):
        for k in (4,) + tuple(range(7, 13)):
            self.into[k].wait_recv()
        for copy in self.out:
            copy.wait_send()


N_COPIES = 13
EXCHANGE_SEMS = [pltpu.SemaphoreType.DMA((N_COPIES,)), pltpu.SemaphoreType.DMA((N_COPIES,))]


def place_body(x_ref, out_ref):
    out_ref[0] = x_ref[...]


def place(x, first, rows, n_dev):
    model = x.shape[1]
    return pl.pallas_call(
        place_body,
        grid=(1,),
        in_specs=[pl.BlockSpec((rows, model), lambda i: (first // rows, 0))],
        out_specs=pl.BlockSpec((1, rows, model), lambda i: (lax.axis_index('expert'), 0, 0)),
        out_shape=jax.ShapeDtypeStruct((n_dev, rows, model), x.dtype),
        name='place',
    )(x)


class Weights:
    def __init__(self, n_local, hbm, vmem, sem):
        self.copies = [[pltpu.make_async_copy(src.at[e], dst.at[e], sem.at[e, k]) for k, (src, dst) in enumerate(zip(hbm, vmem))]
                       for e in range(n_local)]
        self.at = lambda e: [pltpu.make_async_copy(src.at[e], dst.at[e], sem.at[e, k]) for k, (src, dst) in enumerate(zip(hbm, vmem))]

    def start(self):
        for pair in self.copies:
            for copy in pair:
                copy.start()

    def wait(self, e):
        for copy in self.at(e):
            copy.wait()


def weight_scratch(w13, w2):
    return [pltpu.VMEM(w13.shape, BF16), pltpu.VMEM(w2.shape, BF16), pltpu.SemaphoreType.DMA((w13.shape[0], 2))]


def fwd_body(ffn, n_local, half, steps, start, stages, n_carried, x_ref, g_ref, w13_hbm, w2_hbm, *refs):
    y_ref, inbox_ref = refs[n_carried:n_carried + 2]
    rest = list(refs[n_carried + 2:])
    buf_ref = rest.pop(0) if stages else None
    w13_ref, w2_ref, w_sem = rest[:3]
    scratch = rest[3:8]
    exchange = Exchange(buf_ref, *rest[8:], stages) if stages else None
    tile = x_ref.shape[1]
    weights = Weights(n_local, (w13_hbm, w2_hbm), (w13_ref, w2_ref), w_sem)
    step = pl.program_id(0)

    def expert(acc, e):
        gate = gate_column(g_ref[0], e)
        pre = dot(x_ref[0], w13_ref[e])
        one, three = pre[:, :ffn], pre[:, ffn:]
        hidden = jnp.where(gate > 0.0, one * jax.nn.sigmoid(one) * three, 0.0).astype(BF16)
        acc[...] += gate * dot(hidden, w2_ref[e]).astype(BF16).astype(F32)

    def compute(acc):
        @pl.when(step == 0)
        def _():
            def one_by_one(e, carry):
                weights.wait(e)
                expert(acc, e)
                return carry

            lax.fori_loop(0, n_local, one_by_one, 0)

        @pl.when(step > 0)
        def _():
            for e in range(n_local):
                expert(acc, e)

    @pl.when(step == 0)
    def _():
        weights.start()

    pair_sum(compute, half, steps, tile, inbox_ref, [(y_ref, start, 0, tile)], exchange, *scratch)


def pair_scratch(tile, model, half, n_pieces):
    return [
        pltpu.VMEM((N_ACC, tile, model), F32),
        pltpu.SemaphoreType.DMA((N_ACC,)),
        pltpu.SemaphoreType.DMA((half,)),
        pltpu.SemaphoreType.DMA((N_ACC,)),
        pltpu.SemaphoreType.DMA((N_ACC, n_pieces)),
    ]


def pair_params(collective_id):
    return pltpu.CompilerParams(
        dimension_semantics=('arbitrary',), vmem_limit_bytes=VMEM_LIMIT, collective_id=collective_id, has_side_effects=True)


HBM = pl.BlockSpec(memory_space=pl.ANY)


def expert_fwd(x, gates, w13, w2, tile, start, n_tok, carried, hosted, stages, collective_id):
    n_src, rows, model = x.shape
    n_local, ffn = w2.shape[:2]
    steps = rows // tile
    n_own = n_src // CORES
    half = n_own * steps
    flops = 2 * n_src * rows * n_local * model * ffn * 3
    extra = list(carried) + list(hosted)

    def at(i):
        src, t = pair_source(i, half, steps)
        return src, t, 0

    aliases = {4 + i: i for i in range(len(carried))}
    aliases.update({4 + len(carried) + i: 2 + i for i in range(len(hosted))})
    outs = pl.pallas_call(
        functools.partial(fwd_body, ffn, n_local, half, steps, start, stages, len(extra)),
        grid=(2 * half,),
        in_specs=[
            pl.BlockSpec((1, tile, model), at),
            pl.BlockSpec((1, tile, n_local), at),
            HBM,
            HBM,
        ] + [HBM] * len(extra),
        out_specs=[HBM] * (2 + len(hosted)),
        out_shape=[jax.ShapeDtypeStruct((n_own, n_tok, model), F32), jax.ShapeDtypeStruct((n_own, rows, model), F32)]
        + [jax.ShapeDtypeStruct(h.shape, h.dtype) for h in hosted],
        scratch_shapes=weight_scratch(w13, w2) + pair_scratch(tile, model, half, 1) + EXCHANGE_SEMS * len(hosted),
        input_output_aliases=aliases,
        compiler_params=pair_params(collective_id),
        cost_estimate=pl.CostEstimate(flops=flops, bytes_accessed=n_src * rows * model * 6, transcendentals=0),
        name='expert_fwd',
    )(x, gates, w13, w2, *extra)
    return outs[0], outs[2:]


def bwd_body(ffn, n_local, half, steps, pieces, stages, n_carried, x_ref, dy_ref, g_ref, w13_hbm, w2_hbm, *refs):
    refs = list(refs[n_carried:])
    n_out = len(pieces)
    outs, (da_ref, h_ref, inbox_ref), rest = refs[:n_out], refs[n_out:n_out + 3], refs[n_out + 3:]
    buf_ref = rest.pop(0) if stages else None
    w13_ref, w2_ref, w_sem = rest[:3]
    scratch = rest[3:8]
    exchange = Exchange(buf_ref, *rest[8:], stages) if stages else None
    tile = g_ref.shape[1]
    weights = Weights(n_local, (w13_hbm, w2_hbm), (w13_ref, w2_ref), w_sem)
    step = pl.program_id(0)

    def compute(acc):
        def expert(e, carry):
            @pl.when(step == 0)
            def _():
                weights.wait(e)

            gate = gate_column(g_ref[0], e)
            live = gate > 0.0
            pre = dot(x_ref[...].reshape(tile, x_ref.shape[-1]), w13_ref[e])
            one, three = pre[:, :ffn], pre[:, ffn:]
            sig = jax.nn.sigmoid(one)
            act = one * sig
            h_ref[0, :, pl.ds(pl.multiple_of(e * ffn, ffn), ffn)] = jnp.where(live, act * three, 0.0).astype(BF16)
            d_out = (gate * dy_ref[...].reshape(tile, dy_ref.shape[-1]).astype(F32)).astype(BF16)
            d_hid = dot_t(d_out, w2_ref[e]).astype(BF16).astype(F32)
            d_one = jnp.where(live, d_hid * three * sig * (1.0 + one * (1.0 - sig)), 0.0).astype(BF16)
            d_three = jnp.where(live, d_hid * act, 0.0).astype(BF16)
            d_pre = jnp.concatenate([d_one, d_three], axis=1)
            da_ref[0, :, pl.ds(pl.multiple_of(2 * e * ffn, 2 * ffn), 2 * ffn)] = d_pre
            acc[...] += dot_t(d_pre, w13_ref[e]).astype(BF16).astype(F32)
            return carry

        lax.fori_loop(0, n_local, expert, 0)

    @pl.when(step == 0)
    def _():
        weights.start()

    places = [(ref, 0, row, rows) for ref, (row, rows) in zip(outs, pieces)]
    pair_sum(compute, half, steps, tile, inbox_ref, places, exchange, *scratch)


def expert_bwd(x, dy, which, gates, w13, w2, start, pieces, carried, hosted, stages, collective_id):
    n_src, model = x.shape[0], x.shape[-1]
    n_tok = gates.shape[1]
    n_local, ffn = w2.shape[:2]
    tile = x.shape[-2]
    steps = 1
    half = n_src // CORES
    flops = 2 * n_src * tile * n_local * model * ffn * 5
    extra = list(carried) + list(hosted)
    n_out = len(pieces)

    def rows_of(array, k):
        def index(i):
            src, t = pair_source(i, half, steps)
            return (src, t, 0) if array.ndim == 3 else (src, k, t, 0)

        return pl.BlockSpec((1,) * (array.ndim - 2) + (tile, model), index)

    def at(i):
        src, t = pair_source(i, half, steps)
        return src, start // tile + t, 0

    aliases = {5 + i: n_out + i for i in range(len(carried))}
    aliases.update({5 + len(carried) + i: n_out + 3 + i for i in range(len(hosted))})
    outs = pl.pallas_call(
        functools.partial(bwd_body, ffn, n_local, half, steps, pieces, stages, len(extra)),
        grid=(2 * half,),
        in_specs=[
            rows_of(x, which[0]),
            rows_of(dy, which[1]),
            pl.BlockSpec((1, tile, n_local), at),
            HBM,
            HBM,
        ] + [HBM] * len(extra),
        out_specs=[HBM] * n_out + [
            pl.BlockSpec((1, tile, 2 * ffn * n_local), at),
            pl.BlockSpec((1, tile, ffn * n_local), at),
        ] + [HBM] * (1 + len(hosted)),
        out_shape=[jax.ShapeDtypeStruct((half, rows, model), F32) for _, rows in pieces] + [
            jax.ShapeDtypeStruct((n_src, n_tok, 2 * ffn * n_local), BF16),
            jax.ShapeDtypeStruct((n_src, n_tok, ffn * n_local), BF16),
            jax.ShapeDtypeStruct((half, tile, model), F32),
        ] + [jax.ShapeDtypeStruct(h.shape, h.dtype) for h in hosted],
        scratch_shapes=weight_scratch(w13, w2) + pair_scratch(tile, model, half, n_out) + EXCHANGE_SEMS * len(hosted),
        input_output_aliases=aliases,
        compiler_params=pair_params(collective_id),
        cost_estimate=pl.CostEstimate(flops=flops, bytes_accessed=n_src * tile * model * 14, transcendentals=0),
        name='expert_bwd',
    )(x, dy, gates, w13, w2, *extra)
    return outs[:n_out], outs[n_out:n_out + 2], outs[n_out + 3:]


def grad_body(ffn, lo_ref, x_ref, dy_ref, g_ref, da_ref, h_ref, dw1_ref, dw3_ref, dw2_ref, acc13_ref, acc2_ref):
    e, k = pl.program_id(0), pl.program_id(1)

    @pl.when(k == 0)
    def _():
        acc13_ref[...] = jnp.zeros_like(acc13_ref)
        acc2_ref[...] = jnp.zeros_like(acc2_ref)

    acc13_ref[...] += dot_a(jnp.concatenate([lo_ref[0, 1], x_ref[0]], axis=0), da_ref[0])
    d_out = jnp.concatenate([lo_ref[0, 0], dy_ref[0]], axis=0).astype(F32)
    d_out = (gate_column(g_ref[0], e) * d_out).astype(BF16)
    acc2_ref[...] += dot_a(h_ref[0], d_out)

    @pl.when(k == pl.num_programs(1) - 1)
    def _():
        dw1_ref[0] = acc13_ref[:, :ffn].astype(BF16)
        dw3_ref[0] = acc13_ref[:, ffn:].astype(BF16)
        dw2_ref[0] = acc2_ref[...].astype(BF16)


def weight_grads(lo, x_hi, dy_hi, gates, d_pre, hidden):
    n_src, n_tok, n_local = gates.shape
    model = lo.shape[3]
    ffn = hidden.shape[2] // n_local
    flops = 2 * n_src * n_tok * n_local * model * ffn * 3
    at = lambda e, k: (k, 0, 0)
    at_e = lambda e, k: (k, 0, e)
    out = lambda e, k: (e, 0, 0)
    return pl.pallas_call(
        functools.partial(grad_body, ffn),
        grid=(n_local, n_src),
        in_specs=[
            pl.BlockSpec((1,) + lo.shape[1:], lambda e, k: (k, 0, 0, 0)),
            pl.BlockSpec((1,) + x_hi.shape[1:], at),
            pl.BlockSpec((1,) + dy_hi.shape[1:], at),
            pl.BlockSpec((1, n_tok, n_local), at),
            pl.BlockSpec((1, n_tok, 2 * ffn), at_e),
            pl.BlockSpec((1, n_tok, ffn), at_e),
        ],
        out_specs=[
            pl.BlockSpec((1, model, ffn), out),
            pl.BlockSpec((1, model, ffn), out),
            pl.BlockSpec((1, ffn, model), out),
        ],
        out_shape=[
            jax.ShapeDtypeStruct((n_local, model, ffn), BF16),
            jax.ShapeDtypeStruct((n_local, model, ffn), BF16),
            jax.ShapeDtypeStruct((n_local, ffn, model), BF16),
        ],
        scratch_shapes=[pltpu.VMEM((model, 2 * ffn), F32), pltpu.VMEM((ffn, model), F32)],
        compiler_params=pltpu.CompilerParams(dimension_semantics=('arbitrary', 'arbitrary'), vmem_limit_bytes=VMEM_LIMIT),
        cost_estimate=pl.CostEstimate(flops=flops, bytes_accessed=n_src * n_tok * model * 4 * n_local, transcendentals=0),
        name='weight_grads',
    )(lo, x_hi, dy_hi, gates, d_pre, hidden)


def solution(mesh):
    n_stage = mesh.shape['stage']
    n_dev = mesh.shape['expert']
    to_next = [(stage_idx, (stage_idx + 1) % n_stage) for stage_idx in range(n_stage)]
    to_prev = [((stage_idx + 1) % n_stage, stage_idx) for stage_idx in range(n_stage)]
    tok_spec = P('stage', 'expert', None)
    w_spec = P('stage', 'expert', None, None)
    same_core = [list(range(core, n_dev, CORES)) for core in range(CORES)]
    n_fwd = len(FWD_CHUNKS)

    def moe_body(x_act, route_idx, route_wts, w_one, w_three, w_two, dy_act):
        x_src = x_act[0]
        n_tok, _ = x_src.shape
        n_local = w_one.shape[1]
        n_exp = n_local * n_dev

        def gather(rows):
            return lax.all_gather(rows, 'expert', axis=0, tiled=False)

        def reduce_rows(part):
            return lax.psum_scatter(part, 'expert', scatter_dimension=0, axis_index_groups=same_core, tiled=False).astype(BF16)

        hits = route_idx[0][:, :, None] == jnp.arange(n_exp, dtype=jnp.int32)
        gate_src = jnp.sum(jnp.where(hits, route_wts[0][:, :, None], 0.0), axis=1)
        gate_src = jnp.transpose(gate_src.reshape(n_tok, n_dev, n_local), (1, 2, 0))
        gate_dst = lax.ppermute(gate_src, 'stage', to_next)
        gates = jnp.transpose(lax.all_to_all(gate_dst, 'expert', 0, 0), (0, 2, 1))

        w13 = jnp.concatenate([w_one[0], w_three[0]], axis=2)
        w2 = w_two[0]

        half = n_tok // 2
        dy_hi = place(dy_act[0], half, half, n_dev)
        carried = ()
        start = 0
        for k, (rows, tile) in enumerate(FWD_CHUNKS):
            x_dst = lax.ppermute(x_src[start:start + rows], 'stage', to_next)
            x_all = gather(x_dst)
            if k == 0:
                x_first = x_all
            hosted, stages = ((dy_hi,), FWD_STAGES) if k == n_fwd - 1 else ((), ())
            y_part, arrived = expert_fwd(x_all, gates[:, start:start + rows], w13, w2, tile, start, n_tok, carried, hosted, stages, k)
            carried = (y_part,)
            start += rows
        dy_hi, = arrived
        y_out = reduce_rows(y_part)

        x_again, _ = lax.optimization_barrier((x_src, x_first))
        x_dst = lax.ppermute(x_again[:half], 'stage', to_next)
        lo = gather(jnp.stack([dy_act[0, :half], x_dst]))
        x_dst = lax.ppermute(x_again[half:], 'stage', to_next)
        x_hi = place(x_dst, 0, half, n_dev)

        lo_now, _ = lax.optimization_barrier((lo, y_part))
        dx_lo, carried, (x_hi,) = expert_bwd(lo_now, lo_now, (1, 0), gates, w13, w2, 0, ((0, half),), (), (x_hi,), BWD_STAGES, n_fwd)
        cut = half // 2
        dx_hi, carried, _ = expert_bwd(x_hi, dy_hi, (0, 0), gates, w13, w2, half, ((0, cut), (cut, cut)), carried, (), (), n_fwd + 1)
        dx_parts = []
        for part in list(dx_lo) + list(dx_hi):
            dx_dst = reduce_rows(part)
            dx_parts.append(lax.ppermute(dx_dst, 'stage', to_prev))
        dx_out = jnp.concatenate(dx_parts, axis=0)

        g_one, g_three, g_two = weight_grads(lo, x_hi, dy_hi, gates, *carried)
        return y_out[None], dx_out[None], g_one[None], g_three[None], g_two[None]

    return jax.shard_map(moe_body, mesh=mesh, in_specs=(tok_spec, tok_spec, tok_spec, w_spec, w_spec, w_spec, tok_spec), out_specs=(tok_spec, tok_spec, w_spec, w_spec, w_spec), check_vma=False)
```

```python
import functools

import jax
import jax.numpy as jnp
from jax import lax
from jax.experimental import pallas as pl
from jax.experimental.pallas import tpu as pltpu
from jax.sharding import PartitionSpec as P


F32 = jnp.float32
BF16 = jnp.bfloat16
BWD_ROWS = (256, 384, 384)
FWD_ROWS = (512, 512)
FWD_TILE = 256
STAGES = (0, 3, 5, 7)
VMEM_LIMIT = 65400 * 1024
N_ACC = 3
CORES = 2
MESH = pl.DeviceIdType.MESH


def dot(lhs, rhs):
    return jnp.dot(lhs, rhs, preferred_element_type=F32)


def dot_t(lhs, rhs):
    return lax.dot_general(lhs, rhs, (((1,), (1,)), ((), ())), preferred_element_type=F32)


def dot_a(lhs, rhs):
    return lax.dot_general(lhs, rhs, (((0,), (0,)), ((), ())), preferred_element_type=F32)


def gate_column(gates, expert):
    lanes = lax.broadcasted_iota(jnp.int32, gates.shape, 1)
    return jnp.sum(jnp.where(lanes == expert, gates, 0.0), axis=1, keepdims=True)


def pair_source(step, half, steps):
    core = lax.rem(lax.axis_index('expert'), CORES)
    mine = step // half
    tile = lax.rem(step, half)
    lane = lax.rem(core + 1 + mine, CORES)
    return CORES * (tile // steps) + lane, lax.rem(tile, steps)


def pair_sum(compute, half, steps, tile, inbox_ref, out, exchange, acc_ref, send_sem, recv_sem, in_sem, out_sem):
    step = pl.program_id(0)
    last = 2 * half - 1
    me = lax.axis_index('expert')
    other = me + 1 - 2 * lax.rem(me, CORES)

    def at(ref, job):
        return ref.at[job // steps, pl.ds(lax.rem(job, steps) * tile, tile)]

    def store(job):
        slot = lax.rem(job + half, N_ACC)
        out_ref, first = out
        rows = pl.ds(first + lax.rem(job, steps) * tile, tile)
        return pltpu.make_async_copy(acc_ref.at[slot], out_ref.at[job // steps, rows], out_sem.at[slot])

    def send(job):
        slot = lax.rem(job, N_ACC)
        return pltpu.make_async_remote_copy(
            src_ref=acc_ref.at[slot], dst_ref=at(inbox_ref, job), send_sem=send_sem.at[slot], recv_sem=recv_sem.at[job],
            device_id={'expert': other}, device_id_type=MESH)

    def fetch(job):
        slot = lax.rem(job + half, N_ACC)
        return pltpu.make_async_copy(at(inbox_ref, job), acc_ref.at[slot], in_sem.at[slot])

    @pl.when(step == 0)
    def _():
        peers = [other] + (exchange.peers if exchange else [])
        barrier = pltpu.get_barrier_semaphore()
        for peer in peers:
            pl.semaphore_signal(barrier, inc=1, device_id={'expert': peer}, device_id_type=MESH)
        pl.semaphore_wait(barrier, len(peers))

    if exchange:
        exchange.advance(step)

    back = step - (N_ACC - 1)

    @pl.when((back >= 0) & (back < half))
    def _():
        send(back).wait_send()

    @pl.when(back >= half)
    def _():
        store(back - half).wait()

    ahead = step + 1 - half

    @pl.when((ahead >= 0) & (ahead < half))
    def _():
        send(ahead).wait_recv()
        fetch(ahead).start()

    acc = acc_ref.at[lax.rem(step, N_ACC)]

    @pl.when(step < half)
    def _():
        acc[...] = jnp.zeros_like(acc)

    @pl.when(step >= half)
    def _():
        fetch(step - half).wait()

    compute(acc)

    @pl.when(step < half)
    def _():
        send(step).start()

    @pl.when(step >= half)
    def _():
        store(step - half).start()

    @pl.when(step == last)
    def _():
        for job in range(half - N_ACC + 1, half):
            store(job).wait()
        if exchange:
            exchange.finish()


class Exchange:
    def __init__(self, ref, send_sem, recv_sem, stages):
        me = lax.axis_index('expert')
        flip = lambda dev, bit: dev + bit - 2 * bit * lax.rem(dev // bit, 2)
        core, x, y = flip(me, 1), flip(me, 2), flip(me, 4)
        diag = flip(x, 4)
        self.peers = [x, y]
        self.stages = stages
        rows = ref.shape[1] // 2
        first, second, both = pl.ds(0, rows), pl.ds(rows, rows), pl.ds(0, 2 * rows)
        plan = [
            (first, me, x, x),
            (second, me, y, y),
            (second, me, x, x),
            (first, me, y, y),
            (both, me, core, core),
            (first, x, diag, y),
            (second, y, diag, x),
            (first, x, flip(x, 1), core),
            (second, y, flip(y, 1), core),
            (second, x, flip(x, 1), core),
            (first, y, flip(y, 1), core),
            (first, diag, flip(diag, 1), core),
            (second, diag, flip(diag, 1), core),
        ]

        def copy(k, block):
            part, _, _, to = plan[k]
            return pltpu.make_async_remote_copy(
                src_ref=ref.at[block, part], dst_ref=ref.at[block, part], send_sem=send_sem.at[k], recv_sem=recv_sem.at[k],
                device_id={'expert': to}, device_id_type=MESH)

        self.out = [copy(k, plan[k][1]) for k in range(len(plan))]
        self.into = [copy(k, plan[k][2]) for k in range(len(plan))]

    def advance(self, step):
        for at, arrived, started in zip(self.stages, ((), (0, 1), (2, 3), (5, 6)), ((0, 1, 2, 3, 4), (5, 6, 7, 8), (9, 10), (11, 12))):
            @pl.when(step == at)
            def _(arrived=arrived, started=started):
                for k in arrived:
                    self.into[k].wait_recv()
                for k in started:
                    self.out[k].start()

    def finish(self):
        for k in (4,) + tuple(range(7, 13)):
            self.into[k].wait_recv()
        for copy in self.out:
            copy.wait_send()


N_COPIES = 13
EXCHANGE_SEMS = [pltpu.SemaphoreType.DMA((N_COPIES,)), pltpu.SemaphoreType.DMA((N_COPIES,))]


def place_body(x_ref, out_ref):
    out_ref[0] = x_ref[...]


def place(x, first, rows, n_dev):
    model = x.shape[1]
    return pl.pallas_call(
        place_body,
        grid=(1,),
        in_specs=[pl.BlockSpec((rows, model), lambda i: (first // rows, 0))],
        out_specs=pl.BlockSpec((1, rows, model), lambda i: (lax.axis_index('expert'), 0, 0)),
        out_shape=jax.ShapeDtypeStruct((n_dev, rows, model), x.dtype),
        name='place',
    )(x)


class Weights:
    def __init__(self, n_local, hbm, vmem, sem):
        self.copies = [[pltpu.make_async_copy(src.at[e], dst.at[e], sem.at[e, k]) for k, (src, dst) in enumerate(zip(hbm, vmem))]
                       for e in range(n_local)]
        self.at = lambda e: [pltpu.make_async_copy(src.at[e], dst.at[e], sem.at[e, k]) for k, (src, dst) in enumerate(zip(hbm, vmem))]

    def start(self):
        for pair in self.copies:
            for copy in pair:
                copy.start()

    def wait(self, e):
        for copy in self.at(e):
            copy.wait()


def weight_scratch(w13, w2):
    return [pltpu.VMEM(w13.shape, BF16), pltpu.VMEM(w2.shape, BF16), pltpu.SemaphoreType.DMA((w13.shape[0], 2))]


def fwd_body(ffn, n_local, half, steps, x_ref, g_ref, w13_hbm, w2_hbm, y_ref, inbox_ref, w13_ref, w2_ref, w_sem, *scratch):
    tile = x_ref.shape[1]
    weights = Weights(n_local, (w13_hbm, w2_hbm), (w13_ref, w2_ref), w_sem)
    step = pl.program_id(0)

    def expert(acc, e):
        gate = gate_column(g_ref[0], e)
        pre = dot(x_ref[0], w13_ref[e])
        one, three = pre[:, :ffn], pre[:, ffn:]
        hidden = jnp.where(gate > 0.0, one * jax.nn.sigmoid(one) * three, 0.0).astype(BF16)
        acc[...] += gate * dot(hidden, w2_ref[e]).astype(BF16).astype(F32)

    def compute(acc):
        @pl.when(step == 0)
        def _():
            def one_by_one(e, carry):
                weights.wait(e)
                expert(acc, e)
                return carry

            lax.fori_loop(0, n_local, one_by_one, 0)

        @pl.when(step > 0)
        def _():
            for e in range(n_local):
                expert(acc, e)

    @pl.when(step == 0)
    def _():
        weights.start()

    pair_sum(compute, half, steps, tile, inbox_ref, (y_ref, 0), None, *scratch)


def pair_scratch(tile, model, half):
    return [
        pltpu.VMEM((N_ACC, tile, model), F32),
        pltpu.SemaphoreType.DMA((N_ACC,)),
        pltpu.SemaphoreType.DMA((half,)),
        pltpu.SemaphoreType.DMA((N_ACC,)),
        pltpu.SemaphoreType.DMA((N_ACC,)),
    ]


def pair_params(collective_id):
    return pltpu.CompilerParams(
        dimension_semantics=('arbitrary',), vmem_limit_bytes=VMEM_LIMIT, collective_id=collective_id, has_side_effects=True)


HBM = pl.BlockSpec(memory_space=pl.ANY)


def expert_fwd(x, gates, w13, w2, collective_id):
    n_src, rows, model = x.shape
    n_local, ffn = w2.shape[:2]
    tile = FWD_TILE
    steps = rows // tile
    n_own = n_src // CORES
    half = n_own * steps
    flops = 2 * n_src * rows * n_local * model * ffn * 3

    def at(i):
        src, t = pair_source(i, half, steps)
        return src, t, 0

    part = jax.ShapeDtypeStruct((n_own, rows, model), F32)
    return pl.pallas_call(
        functools.partial(fwd_body, ffn, n_local, half, steps),
        grid=(2 * half,),
        in_specs=[pl.BlockSpec((1, tile, model), at), pl.BlockSpec((1, tile, n_local), at), HBM, HBM],
        out_specs=[HBM, HBM],
        out_shape=[part, part],
        scratch_shapes=weight_scratch(w13, w2) + pair_scratch(tile, model, half),
        compiler_params=pair_params(collective_id),
        cost_estimate=pl.CostEstimate(flops=flops, bytes_accessed=n_src * rows * model * 6, transcendentals=0),
        name='expert_fwd',
    )(x, gates, w13, w2)[0]


def bwd_body(ffn, n_local, half, first, n_carried, n_hosted, x_ref, dy_ref, g_ref, w13_hbm, w2_hbm, *refs):
    refs = list(refs[n_carried + n_hosted:])
    (dx_ref, da_ref, h_ref, inbox_ref), rest = refs[:4], refs[4:]
    buf_ref = rest.pop(0) if n_hosted else None
    w13_ref, w2_ref, w_sem = rest[:3]
    scratch = rest[3:8]
    exchange = Exchange(buf_ref, *rest[8:], STAGES) if n_hosted else None
    tile = g_ref.shape[1]
    weights = Weights(n_local, (w13_hbm, w2_hbm), (w13_ref, w2_ref), w_sem)
    step = pl.program_id(0)

    def compute(acc):
        def expert(e, carry):
            @pl.when(step == 0)
            def _():
                weights.wait(e)

            gate = gate_column(g_ref[0], e)
            live = gate > 0.0
            pre = dot(x_ref[...].reshape(tile, x_ref.shape[-1]), w13_ref[e])
            one, three = pre[:, :ffn], pre[:, ffn:]
            sig = jax.nn.sigmoid(one)
            act = one * sig
            h_ref[0, :, pl.ds(pl.multiple_of(e * ffn, ffn), ffn)] = jnp.where(live, act * three, 0.0).astype(BF16)
            d_out = (gate * dy_ref[...].reshape(tile, dy_ref.shape[-1]).astype(F32)).astype(BF16)
            d_hid = dot_t(d_out, w2_ref[e]).astype(BF16).astype(F32)
            d_one = jnp.where(live, d_hid * three * sig * (1.0 + one * (1.0 - sig)), 0.0).astype(BF16)
            d_three = jnp.where(live, d_hid * act, 0.0).astype(BF16)
            d_pre = jnp.concatenate([d_one, d_three], axis=1)
            da_ref[0, :, pl.ds(pl.multiple_of(2 * e * ffn, 2 * ffn), 2 * ffn)] = d_pre
            acc[...] += dot_t(d_pre, w13_ref[e]).astype(BF16).astype(F32)
            return carry

        lax.fori_loop(0, n_local, expert, 0)

    @pl.when(step == 0)
    def _():
        weights.start()

    pair_sum(compute, half, 1, tile, inbox_ref, (dx_ref, first), exchange, *scratch)


def expert_bwd(x, dy, which, gates, w13, w2, dx_rows, first, carried, hosted, collective_id):
    n_src, model = x.shape[0], x.shape[-1]
    n_local, ffn = w2.shape[:2]
    tile = x.shape[-2]
    half = n_src // CORES
    flops = 2 * n_src * tile * n_local * model * ffn * 5

    def at(i):
        src, _ = pair_source(i, half, 1)
        return src, 0, 0

    def rows_of(array, k):
        def stacked(i):
            src, _ = pair_source(i, half, 1)
            return src, k, 0, 0

        return pl.BlockSpec((1,) * (array.ndim - 2) + (tile, model), at if array.ndim == 3 else stacked)

    aliases = {5 + i: 0 for i in range(len(carried))}
    aliases.update({5 + len(carried) + i: 4 + i for i in range(len(hosted))})
    outs = pl.pallas_call(
        functools.partial(bwd_body, ffn, n_local, half, first, len(carried), len(hosted)),
        grid=(2 * half,),
        in_specs=[rows_of(x, which[0]), rows_of(dy, which[1]), pl.BlockSpec((1, tile, n_local), at)]
        + [HBM] * (2 + len(carried) + len(hosted)),
        out_specs=[
            HBM,
            pl.BlockSpec((1, tile, 2 * ffn * n_local), at),
            pl.BlockSpec((1, tile, ffn * n_local), at),
        ] + [HBM] * (1 + len(hosted)),
        out_shape=[
            jax.ShapeDtypeStruct((half, dx_rows, model), F32),
            jax.ShapeDtypeStruct((n_src, tile, 2 * ffn * n_local), BF16),
            jax.ShapeDtypeStruct((n_src, tile, ffn * n_local), BF16),
            jax.ShapeDtypeStruct((half, tile, model), F32),
        ] + [jax.ShapeDtypeStruct(h.shape, h.dtype) for h in hosted],
        scratch_shapes=weight_scratch(w13, w2) + pair_scratch(tile, model, half) + EXCHANGE_SEMS * len(hosted),
        input_output_aliases=aliases,
        compiler_params=pair_params(collective_id),
        cost_estimate=pl.CostEstimate(flops=flops, bytes_accessed=n_src * tile * model * 14, transcendentals=0),
        name='expert_bwd',
    )(x, dy, gates, w13, w2, *carried, *hosted)
    return outs[0], outs[1], outs[2], outs[4:]


def rows_joined(refs):
    parts = [ref[...].reshape(ref.shape[-2:]) for ref in refs]
    return parts[0] if len(parts) == 1 else jnp.concatenate(parts, axis=0)


def grad_body(ffn, n_parts, g_ref, *refs):
    x_refs, dy_refs, da_refs, h_refs = (refs[k * n_parts:(k + 1) * n_parts] for k in range(4))
    dw1_ref, dw3_ref, dw2_ref, acc13_ref, acc2_ref = refs[4 * n_parts:]
    e, k = pl.program_id(0), pl.program_id(1)

    @pl.when(k == 0)
    def _():
        acc13_ref[...] = jnp.zeros_like(acc13_ref)
        acc2_ref[...] = jnp.zeros_like(acc2_ref)

    acc13_ref[...] += dot_a(rows_joined(x_refs), rows_joined(da_refs))
    d_out = (gate_column(g_ref[0], e) * rows_joined(dy_refs).astype(F32)).astype(BF16)
    acc2_ref[...] += dot_a(rows_joined(h_refs), d_out)

    @pl.when(k == pl.num_programs(1) - 1)
    def _():
        dw1_ref[0] = acc13_ref[:, :ffn].astype(BF16)
        dw3_ref[0] = acc13_ref[:, ffn:].astype(BF16)
        dw2_ref[0] = acc2_ref[...].astype(BF16)


def weight_grads(gates, xs, dys, d_pres, hiddens):
    n_src, n_tok, n_local = gates.shape
    model = xs[0][0].shape[-1]
    ffn = hiddens[0].shape[2] // n_local
    flops = 2 * n_src * n_tok * n_local * model * ffn * 3
    at = lambda e, k: (k, 0, 0)
    at_e = lambda e, k: (k, 0, e)
    out = lambda e, k: (e, 0, 0)

    def rows_of(array, which):
        block = (1,) * (array.ndim - 2) + array.shape[-2:]
        return pl.BlockSpec(block, at if array.ndim == 3 else (lambda e, k: (k, which, 0, 0)))

    return pl.pallas_call(
        functools.partial(grad_body, ffn, len(xs)),
        grid=(n_local, n_src),
        in_specs=[pl.BlockSpec((1, n_tok, n_local), at)]
        + [rows_of(*x) for x in xs]
        + [rows_of(*dy) for dy in dys]
        + [pl.BlockSpec((1, d.shape[1], 2 * ffn), at_e) for d in d_pres]
        + [pl.BlockSpec((1, h.shape[1], ffn), at_e) for h in hiddens],
        out_specs=[
            pl.BlockSpec((1, model, ffn), out),
            pl.BlockSpec((1, model, ffn), out),
            pl.BlockSpec((1, ffn, model), out),
        ],
        out_shape=[
            jax.ShapeDtypeStruct((n_local, model, ffn), BF16),
            jax.ShapeDtypeStruct((n_local, model, ffn), BF16),
            jax.ShapeDtypeStruct((n_local, ffn, model), BF16),
        ],
        scratch_shapes=[pltpu.VMEM((model, 2 * ffn), F32), pltpu.VMEM((ffn, model), F32)],
        compiler_params=pltpu.CompilerParams(dimension_semantics=('arbitrary', 'arbitrary'), vmem_limit_bytes=VMEM_LIMIT),
        cost_estimate=pl.CostEstimate(flops=flops, bytes_accessed=n_src * n_tok * model * 4 * n_local, transcendentals=0),
        name='weight_grads',
    )(gates, *[x for x, _ in xs], *[dy for dy, _ in dys], *d_pres, *hiddens)


def solution(mesh):
    n_stage = mesh.shape['stage']
    n_dev = mesh.shape['expert']
    to_next = [(stage_idx, (stage_idx + 1) % n_stage) for stage_idx in range(n_stage)]
    to_prev = [((stage_idx + 1) % n_stage, stage_idx) for stage_idx in range(n_stage)]
    tok_spec = P('stage', 'expert', None)
    w_spec = P('stage', 'expert', None, None)
    same_core = [list(range(core, n_dev, CORES)) for core in range(CORES)]

    def moe_body(x_act, route_idx, route_wts, w_one, w_three, w_two, dy_act):
        x_src = x_act[0]
        n_tok, _ = x_src.shape
        n_local = w_one.shape[1]
        n_exp = n_local * n_dev

        def gather(rows):
            return lax.all_gather(rows, 'expert', axis=0, tiled=False)

        def reduce_rows(part):
            return lax.psum_scatter(part, 'expert', scatter_dimension=0, axis_index_groups=same_core, tiled=False).astype(BF16)

        hits = route_idx[0][:, :, None] == jnp.arange(n_exp, dtype=jnp.int32)
        gate_src = jnp.sum(jnp.where(hits, route_wts[0][:, :, None], 0.0), axis=1)
        gate_src = jnp.transpose(gate_src.reshape(n_tok, n_dev, n_local), (1, 2, 0))
        gate_dst = lax.ppermute(gate_src, 'stage', to_next)
        gates = jnp.transpose(lax.all_to_all(gate_dst, 'expert', 0, 0), (0, 2, 1))

        w13 = jnp.concatenate([w_one[0], w_three[0]], axis=2)
        w2 = w_two[0]

        def spans(sizes):
            ends = [sum(sizes[:k + 1]) for k in range(len(sizes))]
            return [slice(end - size, end) for end, size in zip(ends, sizes)]

        bwd, fwd = spans(BWD_ROWS), spans(FWD_ROWS)
        dx_rows = sum(BWD_ROWS[:2]), BWD_ROWS[2]

        def hop(rows):
            return lax.ppermute(x_src[rows], 'stage', to_next)

        dys = [(gather(dy_act[0, bwd[0]]), 0)]
        xs = [(gather(hop(bwd[0])), 0)]
        for k in (1, 2):
            x_dst = hop(bwd[k])
            both = gather(jnp.stack([dy_act[0, bwd[k]], x_dst]))
            dys.append((both, 0))
            xs.append((both, 1))

        d_pres, hiddens, x_fwd = [], [], []
        dx_parts = []
        for k in range(3):
            carried, hosted = (), ()
            if k == 1:
                carried = (dx_part,)
            if k > 0:
                x_dst = hop(fwd[k - 1])
                hosted = (place(x_dst, 0, FWD_ROWS[k - 1], n_dev),)
            dx_part, d_pre, hidden, arrived = expert_bwd(
                xs[k][0], dys[k][0], (xs[k][1], dys[k][1]), gates[:, bwd[k]], w13, w2,
                dx_rows[k // 2], BWD_ROWS[0] if k == 1 else 0, carried, hosted, k)
            x_fwd += arrived
            d_pres.append(d_pre)
            hiddens.append(hidden)
            if k > 0:
                dx_dst = reduce_rows(dx_part)
                dx_parts.append(lax.ppermute(dx_dst, 'stage', to_prev))
        dx_out = jnp.concatenate(dx_parts, axis=0)

        y_parts = []
        for k in range(2):
            y_part = expert_fwd(x_fwd[k], gates[:, fwd[k]], w13, w2, 3 + k)
            y_parts.append(reduce_rows(y_part))
        y_out = jnp.concatenate(y_parts, axis=0)

        g_one, g_three, g_two = weight_grads(gates, xs, dys, d_pres, hiddens)
        return y_out[None], dx_out[None], g_one[None], g_three[None], g_two[None]

    return jax.shard_map(moe_body, mesh=mesh, in_specs=(tok_spec, tok_spec, tok_spec, w_spec, w_spec, w_spec, tok_spec), out_specs=(tok_spec, tok_spec, w_spec, w_spec, w_spec), check_vma=False)
```

```python
import functools

import jax
import jax.numpy as jnp
from jax import lax
from jax.experimental import pallas as pl
from jax.experimental.pallas import tpu as pltpu
from jax.sharding import PartitionSpec as P


F32 = jnp.float32
BF16 = jnp.bfloat16
BWD_ROWS = (256, 384, 384)
FWD_ROWS = (512, 512)
STAGES = (((0, 2, 3, 7), (0, 4, 6, 7)), ((0, 2, 3, 5), (0, 4, 5, 7)), ((0, 3, 5, 7),))
VMEM_LIMIT = 65400 * 1024
N_ACC = 3
CORES = 2
UNROLL = 2
MESH = pl.DeviceIdType.MESH


def dot(lhs, rhs):
    return jnp.dot(lhs, rhs, preferred_element_type=F32)


def dot_t(lhs, rhs):
    return lax.dot_general(lhs, rhs, (((1,), (1,)), ((), ())), preferred_element_type=F32)


def dot_a(lhs, rhs):
    return lax.dot_general(lhs, rhs, (((0,), (0,)), ((), ())), preferred_element_type=F32)


def gate_column(gates, expert):
    lanes = lax.broadcasted_iota(jnp.int32, gates.shape, 1)
    return jnp.sum(jnp.where(lanes == expert, gates, 0.0), axis=1, keepdims=True)


def pair_source(step, half, steps):
    core = lax.rem(lax.axis_index('expert'), CORES)
    mine = step // half
    tile = lax.rem(step, half)
    lane = lax.rem(core + 1 + mine, CORES)
    return CORES * (tile // steps) + lane, lax.rem(tile, steps)


def pair_sum(compute, half, steps, tile, inbox_ref, out, exchanges, acc_ref, send_sem, recv_sem, in_sem, out_sem):
    step = pl.program_id(0)
    last = 2 * half - 1
    me = lax.axis_index('expert')
    other = me + 1 - 2 * lax.rem(me, CORES)

    def at(ref, job):
        return ref.at[job // steps, pl.ds(lax.rem(job, steps) * tile, tile)]

    def store(job):
        slot = lax.rem(job + half, N_ACC)
        out_ref, first = out
        rows = pl.ds(first + lax.rem(job, steps) * tile, tile)
        return pltpu.make_async_copy(acc_ref.at[slot], out_ref.at[job // steps, rows], out_sem.at[slot])

    def send(job):
        slot = lax.rem(job, N_ACC)
        return pltpu.make_async_remote_copy(
            src_ref=acc_ref.at[slot], dst_ref=at(inbox_ref, job), send_sem=send_sem.at[slot], recv_sem=recv_sem.at[job],
            device_id={'expert': other}, device_id_type=MESH)

    def fetch(job):
        slot = lax.rem(job + half, N_ACC)
        return pltpu.make_async_copy(at(inbox_ref, job), acc_ref.at[slot], in_sem.at[slot])

    @pl.when(step == 0)
    def _():
        peers = [other] + (exchanges[0].peers if exchanges else [])
        barrier = pltpu.get_barrier_semaphore()
        for peer in peers:
            pl.semaphore_signal(barrier, inc=1, device_id={'expert': peer}, device_id_type=MESH)
        pl.semaphore_wait(barrier, len(peers))

    for exchange in exchanges:
        exchange.advance(step)

    back = step - (N_ACC - 1)

    @pl.when((back >= 0) & (back < half))
    def _():
        send(back).wait_send()

    @pl.when(back >= half)
    def _():
        store(back - half).wait()

    ahead = step + 1 - half

    @pl.when((ahead >= 0) & (ahead < half))
    def _():
        send(ahead).wait_recv()
        fetch(ahead).start()

    acc = acc_ref.at[lax.rem(step, N_ACC)]

    @pl.when(step < half)
    def _():
        acc[...] = jnp.zeros_like(acc)

    @pl.when(step >= half)
    def _():
        fetch(step - half).wait()

    compute(acc)

    @pl.when(step < half)
    def _():
        send(step).start()

    @pl.when(step >= half)
    def _():
        store(step - half).start()

    @pl.when(step == last)
    def _():
        for job in range(half - N_ACC + 1, half):
            store(job).wait()
        for exchange in exchanges:
            exchange.finish()


class Exchange:
    def __init__(self, own_ref, first, ref, stage_ref, send_sem, recv_sem, local_sem, stages):
        me = lax.axis_index('expert')
        flip = lambda dev, bit: dev + bit - 2 * bit * lax.rem(dev // bit, 2)
        core, x, y = flip(me, 1), flip(me, 2), flip(me, 4)
        diag = flip(x, 4)
        self.peers = [x, y]
        self.stages = stages
        rows = ref.shape[1] // 2
        plan = [
            (0, rows, None, x, x),
            (rows, rows, None, y, y),
            (rows, rows, None, x, x),
            (0, rows, None, y, y),
            (0, 2 * rows, None, core, core),
            (0, rows, x, diag, y),
            (rows, rows, y, diag, x),
            (0, rows, x, flip(x, 1), core),
            (rows, rows, y, flip(y, 1), core),
            (rows, rows, x, flip(x, 1), core),
            (0, rows, y, flip(y, 1), core),
            (0, rows, diag, flip(diag, 1), core),
            (rows, rows, diag, flip(diag, 1), core),
        ]

        def copy(k, source, block):
            return pltpu.make_async_remote_copy(
                src_ref=source, dst_ref=ref.at[block, pl.ds(plan[k][0], plan[k][1])], send_sem=send_sem.at[k],
                recv_sem=recv_sem.at[k], device_id={'expert': plan[k][4]}, device_id_type=MESH)

        self.out, self.into = [], []
        for k, (row, n_rows, here, arrives, _) in enumerate(plan):
            own = own_ref.at[pl.ds(first + row, n_rows)]
            self.out.append(copy(k, own if here is None else ref.at[here, pl.ds(row, n_rows)], me if here is None else here))
            self.into.append(copy(k, own, arrives))
        self.take = pltpu.make_async_copy(own_ref.at[pl.ds(first, 2 * rows)], stage_ref, local_sem.at[0])
        self.put = pltpu.make_async_copy(stage_ref, ref.at[me], local_sem.at[1])

    def advance(self, step):
        for at, arrived, started in zip(self.stages, ((), (0, 1), (2, 3), (5, 6)), ((0, 1, 2, 3, 4), (5, 6, 7, 8), (9, 10), (11, 12))):
            @pl.when(step == at)
            def _(arrived=arrived, started=started):
                for k in arrived:
                    self.into[k].wait_recv()
                for k in started:
                    self.out[k].start()
                if not arrived:
                    self.take.start()

        @pl.when(step == 1)
        def _():
            self.take.wait()
            self.put.start()

    def finish(self):
        for k in (4,) + tuple(range(7, 13)):
            self.into[k].wait_recv()
        for copy in self.out:
            copy.wait_send()
        self.put.wait()


N_COPIES = 13


def exchange_scratch(rows, model):
    return [
        pltpu.VMEM((rows, model), BF16),
        pltpu.SemaphoreType.DMA((N_COPIES,)),
        pltpu.SemaphoreType.DMA((N_COPIES,)),
        pltpu.SemaphoreType.DMA((2,)),
    ]


class Weights:
    def __init__(self, hbm, vmem, sem):
        self.n_local = vmem[0].shape[0]
        self.copies = lambda e: [
            pltpu.make_async_copy(src.at[e], dst.at[e], sem.at[e, k]) for k, (src, dst) in enumerate(zip(hbm, vmem))]

        @pl.when(pl.program_id(0) == 0)
        def _():
            for e in range(self.n_local):
                for copy in self.copies(e):
                    copy.start()

    def for_each(self, expert):
        def group(k, carry):
            @pl.when(pl.program_id(0) == 0)
            def _():
                for u in range(UNROLL):
                    for copy in self.copies(k * UNROLL + u):
                        copy.wait()

            for u in range(UNROLL):
                expert(k * UNROLL + u)
            return carry

        lax.fori_loop(0, self.n_local // UNROLL, group, 0)


def weight_scratch(w13, w2):
    return [pltpu.VMEM(w13.shape, BF16), pltpu.VMEM(w2.shape, BF16), pltpu.SemaphoreType.DMA((w13.shape[0], 2))]


def fwd_body(ffn, half, start, n_carried, x_ref, g_ref, w13_hbm, w2_hbm, *refs):
    y_ref, inbox_ref, w13_ref, w2_ref, w_sem, *scratch = refs[n_carried:]
    tile = x_ref.shape[1]
    weights = Weights((w13_hbm, w2_hbm), (w13_ref, w2_ref), w_sem)

    def compute(acc):
        def expert(e):
            gate = gate_column(g_ref[0, start:start + tile], e)
            pre = dot(x_ref[0], w13_ref[e])
            one, three = pre[:, :ffn], pre[:, ffn:]
            hidden = jnp.where(gate > 0.0, one * jax.nn.sigmoid(one) * three, 0.0).astype(BF16)
            acc[...] += gate * dot(hidden, w2_ref[e]).astype(BF16).astype(F32)

        weights.for_each(expert)

    pair_sum(compute, half, 1, tile, inbox_ref, (y_ref, start), [], *scratch)


def pair_scratch(tile, model, half):
    return [
        pltpu.VMEM((N_ACC, tile, model), F32),
        pltpu.SemaphoreType.DMA((N_ACC,)),
        pltpu.SemaphoreType.DMA((half,)),
        pltpu.SemaphoreType.DMA((N_ACC,)),
        pltpu.SemaphoreType.DMA((N_ACC,)),
    ]


def pair_params(collective_id):
    return pltpu.CompilerParams(
        dimension_semantics=('arbitrary',), vmem_limit_bytes=VMEM_LIMIT, collective_id=collective_id, has_side_effects=True)


HBM = pl.BlockSpec(memory_space=pl.ANY)


def at_source(half):
    def index(i):
        return pair_source(i, half, 1)[0], 0, 0

    return index


def expert_fwd(x, gates, w13, w2, start, carried, collective_id):
    n_src, tile, model = x.shape
    n_tok = gates.shape[1]
    n_local, ffn = w2.shape[:2]
    half = n_src // CORES
    at = at_source(half)
    flops = 2 * n_src * tile * n_local * model * ffn * 3
    return pl.pallas_call(
        functools.partial(fwd_body, ffn, half, start, len(carried)),
        grid=(2 * half,),
        in_specs=[pl.BlockSpec((1, tile, model), at), pl.BlockSpec((1, n_tok, n_local), at), HBM, HBM] + [HBM] * len(carried),
        out_specs=[HBM, HBM],
        out_shape=[jax.ShapeDtypeStruct((half, n_tok, model), F32), jax.ShapeDtypeStruct((half, tile, model), F32)],
        scratch_shapes=weight_scratch(w13, w2) + pair_scratch(tile, model, half),
        input_output_aliases={4 + i: i for i in range(len(carried))},
        compiler_params=pair_params(collective_id),
        cost_estimate=pl.CostEstimate(flops=flops, bytes_accessed=n_src * tile * model * 6, transcendentals=0),
        name='expert_fwd',
    )(x, gates, w13, w2, *carried)[0]


def bwd_body(ffn, half, start, first, n_carried, hosted, stages, x_ref, dy_ref, g_ref, w13_hbm, w2_hbm, *refs):
    refs = list(refs[n_carried:])
    own_refs, refs = refs[:len(hosted)], refs[len(hosted):]
    (dx_ref, da_ref, h_ref, inbox_ref), refs = refs[:4], refs[4:]
    buf_refs, refs = refs[:len(hosted)], refs[len(hosted):]
    w13_ref, w2_ref, w_sem, *refs = refs
    scratch, refs = refs[:5], refs[5:]
    exchanges = [Exchange(own_refs[k], row, buf_refs[k], *refs[4 * k:4 * k + 4], stages[k]) for k, (row, _) in enumerate(hosted)]
    tile = x_ref.shape[1]
    weights = Weights((w13_hbm, w2_hbm), (w13_ref, w2_ref), w_sem)

    def compute(acc):
        def expert(e):
            gate = gate_column(g_ref[0, start:start + tile], e)
            live = gate > 0.0
            pre = dot(x_ref[0], w13_ref[e])
            one, three = pre[:, :ffn], pre[:, ffn:]
            sig = jax.nn.sigmoid(one)
            act = one * sig
            h_ref[0, :, pl.ds(pl.multiple_of(e * ffn, ffn), ffn)] = jnp.where(live, act * three, 0.0).astype(BF16)
            d_out = (gate * dy_ref[0].astype(F32)).astype(BF16)
            d_hid = dot_t(d_out, w2_ref[e]).astype(BF16).astype(F32)
            d_one = jnp.where(live, d_hid * three * sig * (1.0 + one * (1.0 - sig)), 0.0).astype(BF16)
            d_three = jnp.where(live, d_hid * act, 0.0).astype(BF16)
            d_pre = jnp.concatenate([d_one, d_three], axis=1)
            da_ref[0, :, pl.ds(pl.multiple_of(2 * e * ffn, 2 * ffn), 2 * ffn)] = d_pre
            acc[...] += dot_t(d_pre, w13_ref[e]).astype(BF16).astype(F32)

        weights.for_each(expert)

    pair_sum(compute, half, 1, tile, inbox_ref, (dx_ref, first), exchanges, *scratch)


def expert_bwd(x, dy, gates, w13, w2, start, dx_rows, first, carried, hosted, stages, collective_id):
    n_src, tile, model = x.shape
    n_tok = gates.shape[1]
    n_local, ffn = w2.shape[:2]
    half = n_src // CORES
    at = at_source(half)
    flops = 2 * n_src * tile * n_local * model * ffn * 5
    outs = pl.pallas_call(
        functools.partial(bwd_body, ffn, half, start, first, len(carried), [h[1:] for h in hosted], stages),
        grid=(2 * half,),
        in_specs=[pl.BlockSpec((1, tile, model), at)] * 2 + [pl.BlockSpec((1, n_tok, n_local), at)]
        + [HBM] * (2 + len(carried) + len(hosted)),
        out_specs=[
            HBM,
            pl.BlockSpec((1, tile, 2 * ffn * n_local), at),
            pl.BlockSpec((1, tile, ffn * n_local), at),
        ] + [HBM] * (1 + len(hosted)),
        out_shape=[
            jax.ShapeDtypeStruct((half, dx_rows, model), F32),
            jax.ShapeDtypeStruct((n_src, tile, 2 * ffn * n_local), BF16),
            jax.ShapeDtypeStruct((n_src, tile, ffn * n_local), BF16),
            jax.ShapeDtypeStruct((half, tile, model), F32),
        ] + [jax.ShapeDtypeStruct((n_src, rows, model), BF16) for _, _, rows in hosted],
        scratch_shapes=weight_scratch(w13, w2) + pair_scratch(tile, model, half)
        + [ref for _, _, rows in hosted for ref in exchange_scratch(rows, model)],
        input_output_aliases={5 + i: 0 for i in range(len(carried))},
        compiler_params=pair_params(collective_id),
        cost_estimate=pl.CostEstimate(flops=flops, bytes_accessed=n_src * tile * model * 14, transcendentals=0),
        name='expert_bwd',
    )(x, dy, gates, w13, w2, *carried, *[h[0] for h in hosted])
    return outs[0], outs[1], outs[2], outs[4:]


def rows_joined(refs, column=0, columns=None):
    parts = [ref[0, :, column:column + (columns or ref.shape[2])] for ref in refs]
    return parts[0] if len(parts) == 1 else jnp.concatenate(parts, axis=0)


def grad_body(ffn, n_parts, g_ref, *refs):
    x_refs, dy_refs, da_refs, h_refs = (refs[k * n_parts:(k + 1) * n_parts] for k in range(4))
    dw1_ref, dw3_ref, dw2_ref, acc13_ref, acc2_ref = refs[4 * n_parts:]
    e, k = pl.program_id(0), pl.program_id(1)

    @pl.when(k == 0)
    def _():
        acc13_ref[...] = jnp.zeros_like(acc13_ref)
        acc2_ref[...] = jnp.zeros_like(acc2_ref)

    for m in range(0, acc13_ref.shape[0], ffn):
        acc13_ref[m:m + ffn] += dot_a(rows_joined(x_refs, m, ffn), rows_joined(da_refs))
    d_out = (gate_column(g_ref[0], e) * rows_joined(dy_refs).astype(F32)).astype(BF16)
    acc2_ref[...] += dot_a(rows_joined(h_refs), d_out)

    @pl.when(k == pl.num_programs(1) - 1)
    def _():
        dw1_ref[0] = acc13_ref[:, :ffn].astype(BF16)
        dw3_ref[0] = acc13_ref[:, ffn:].astype(BF16)
        dw2_ref[0] = acc2_ref[...].astype(BF16)


def weight_grads(gates, xs, dys, d_pres, hiddens):
    n_src, n_tok, n_local = gates.shape
    model = xs[0].shape[2]
    ffn = hiddens[0].shape[2] // n_local
    flops = 2 * n_src * n_tok * n_local * model * ffn * 3
    at = lambda e, k: (k, 0, 0)
    at_e = lambda e, k: (k, 0, e)
    out = lambda e, k: (e, 0, 0)

    return pl.pallas_call(
        functools.partial(grad_body, ffn, len(xs)),
        grid=(n_local, n_src),
        in_specs=[pl.BlockSpec((1, n_tok, n_local), at)]
        + [pl.BlockSpec((1, x.shape[1], model), at) for x in list(xs) + list(dys)]
        + [pl.BlockSpec((1, d.shape[1], 2 * ffn), at_e) for d in d_pres]
        + [pl.BlockSpec((1, h.shape[1], ffn), at_e) for h in hiddens],
        out_specs=[
            pl.BlockSpec((1, model, ffn), out),
            pl.BlockSpec((1, model, ffn), out),
            pl.BlockSpec((1, ffn, model), out),
        ],
        out_shape=[
            jax.ShapeDtypeStruct((n_local, model, ffn), BF16),
            jax.ShapeDtypeStruct((n_local, model, ffn), BF16),
            jax.ShapeDtypeStruct((n_local, ffn, model), BF16),
        ],
        scratch_shapes=[pltpu.VMEM((model, 2 * ffn), F32), pltpu.VMEM((ffn, model), F32)],
        compiler_params=pltpu.CompilerParams(dimension_semantics=('arbitrary', 'arbitrary'), vmem_limit_bytes=VMEM_LIMIT),
        cost_estimate=pl.CostEstimate(flops=flops, bytes_accessed=n_src * n_tok * model * 4 * n_local, transcendentals=0),
        name='weight_grads',
    )(gates, *xs, *dys, *d_pres, *hiddens)


def solution(mesh):
    n_stage = mesh.shape['stage']
    n_dev = mesh.shape['expert']
    to_next = [(stage_idx, (stage_idx + 1) % n_stage) for stage_idx in range(n_stage)]
    to_prev = [((stage_idx + 1) % n_stage, stage_idx) for stage_idx in range(n_stage)]
    tok_spec = P('stage', 'expert', None)
    w_spec = P('stage', 'expert', None, None)
    same_core = [list(range(core, n_dev, CORES)) for core in range(CORES)]

    def moe_body(x_act, route_idx, route_wts, w_one, w_three, w_two, dy_act):
        x_src = x_act[0]
        n_tok, _ = x_src.shape
        n_local = w_one.shape[1]
        n_exp = n_local * n_dev

        def gather(rows):
            return lax.all_gather(rows, 'expert', axis=0, tiled=False)

        def reduce_rows(part):
            return lax.psum_scatter(part, 'expert', scatter_dimension=0, axis_index_groups=same_core, tiled=False).astype(BF16)

        hits = route_idx[0][:, :, None] == jnp.arange(n_exp, dtype=jnp.int32)
        gate_src = jnp.sum(jnp.where(hits, route_wts[0][:, :, None], 0.0), axis=1)
        gate_src = jnp.transpose(gate_src.reshape(n_tok, n_dev, n_local), (1, 2, 0))
        gate_dst = lax.ppermute(gate_src, 'stage', to_next)
        gates = jnp.transpose(lax.all_to_all(gate_dst, 'expert', 0, 0), (0, 2, 1))

        w13 = jnp.concatenate([w_one[0], w_three[0]], axis=2)
        w2 = w_two[0]

        def spans(sizes):
            ends = [sum(sizes[:k + 1]) for k in range(len(sizes))]
            return [slice(end - size, end) for end, size in zip(ends, sizes)]

        bwd, fwd = spans(BWD_ROWS), spans(FWD_ROWS)
        dx_rows = sum(BWD_ROWS[:2]), BWD_ROWS[2]

        def hop(rows):
            return lax.ppermute(x_src[rows], 'stage', to_next)

        dys = [gather(dy_act[0, bwd[0]])]
        xs = [gather(hop(bwd[0]))]

        d_pres, hiddens = [], []
        dx_parts = []
        for k in range(3):
            if k < 2:
                rows = BWD_ROWS[k + 1]
                hosted = ((dy_act[0], bwd[k + 1].start, rows), (hop(bwd[k + 1]), 0, rows))
            else:
                hosted = ((hop(fwd[1]), 0, FWD_ROWS[1]),)
            dx_part, d_pre, hidden, arrived = expert_bwd(
                xs[k], dys[k], gates, w13, w2, bwd[k].start, dx_rows[k // 2], BWD_ROWS[0] if k == 1 else 0,
                (dx_part,) if k == 1 else (), hosted, STAGES[k], k)
            if k < 2:
                dys.append(arrived[0])
                xs.append(arrived[1])
            d_pres.append(d_pre)
            hiddens.append(hidden)
            if k > 0:
                dx_dst = reduce_rows(dx_part)
                dx_parts.append(lax.ppermute(dx_dst, 'stage', to_prev))
        dx_out = jnp.concatenate(dx_parts, axis=0)

        x_dst = hop(fwd[0])
        x_fwd = gather(x_dst), arrived[0]
        y_part = ()
        for k in range(2):
            y_part = (expert_fwd(x_fwd[k], gates, w13, w2, fwd[k].start, y_part, 3 + k),)
        y_out = reduce_rows(y_part[0])

        g_one, g_three, g_two = weight_grads(gates, xs, dys, d_pres, hiddens)
        return y_out[None], dx_out[None], g_one[None], g_three[None], g_two[None]

    return jax.shard_map(moe_body, mesh=mesh, in_specs=(tok_spec, tok_spec, tok_spec, w_spec, w_spec, w_spec, tok_spec), out_specs=(tok_spec, tok_spec, w_spec, w_spec, w_spec), check_vma=False)
```

```python
import functools

import jax
import jax.numpy as jnp
from jax import lax
from jax.experimental import pallas as pl
from jax.experimental.pallas import tpu as pltpu
from jax.sharding import PartitionSpec as P


F32 = jnp.float32
BF16 = jnp.bfloat16
BWD_ROWS = (256, 384, 384)
FWD_ROWS = (512, 512)
X_ROWS = 256
STAGES = {'bwd_1': ((0, 2, 4, 6),), 'bwd_2': ((0, 2, 4, 6), (0, 3, 5, 7)), 'fwd_0': ((0, 2, 4, 6),)}
VMEM_LIMIT = 65400 * 1024
N_ACC = 3
CORES = 2
UNROLL = 2
MESH = pl.DeviceIdType.MESH


def dot(lhs, rhs):
    return jnp.dot(lhs, rhs, preferred_element_type=F32)


def dot_t(lhs, rhs):
    return lax.dot_general(lhs, rhs, (((1,), (1,)), ((), ())), preferred_element_type=F32)


def dot_a(lhs, rhs):
    return lax.dot_general(lhs, rhs, (((0,), (0,)), ((), ())), preferred_element_type=F32)


def gate_column(gates, expert):
    lanes = lax.broadcasted_iota(jnp.int32, gates.shape, 1)
    return jnp.sum(jnp.where(lanes == expert, gates, 0.0), axis=1, keepdims=True)


def meet(peers):
    barrier = pltpu.get_barrier_semaphore()
    for peer in peers:
        pl.semaphore_signal(barrier, inc=1, device_id={'expert': peer}, device_id_type=MESH)
    pl.semaphore_wait(barrier, len(peers))


def pair_source(step, half, steps):
    core = lax.rem(lax.axis_index('expert'), CORES)
    mine = step // half
    tile = lax.rem(step, half)
    lane = lax.rem(core + 1 + mine, CORES)
    return CORES * (tile // steps) + lane, lax.rem(tile, steps)


def pair_sum(compute, half, steps, tile, inbox_ref, out, exchanges, acc_ref, send_sem, recv_sem, in_sem, out_sem):
    step = pl.program_id(0)
    last = 2 * half - 1
    me = lax.axis_index('expert')
    other = me + 1 - 2 * lax.rem(me, CORES)

    def at(ref, job):
        return ref.at[job // steps, pl.ds(lax.rem(job, steps) * tile, tile)]

    def store(job):
        slot = lax.rem(job + half, N_ACC)
        out_ref, first = out
        rows = pl.ds(first + lax.rem(job, steps) * tile, tile)
        return pltpu.make_async_copy(acc_ref.at[slot], out_ref.at[job // steps, rows], out_sem.at[slot])

    def send(job):
        slot = lax.rem(job, N_ACC)
        return pltpu.make_async_remote_copy(
            src_ref=acc_ref.at[slot], dst_ref=at(inbox_ref, job), send_sem=send_sem.at[slot], recv_sem=recv_sem.at[job],
            device_id={'expert': other}, device_id_type=MESH)

    def fetch(job):
        slot = lax.rem(job + half, N_ACC)
        return pltpu.make_async_copy(at(inbox_ref, job), acc_ref.at[slot], in_sem.at[slot])

    @pl.when(step == 0)
    def _():
        meet(exchanges[0].peers if exchanges else [other])

    for exchange in exchanges:
        exchange.advance(step)

    back = step - (N_ACC - 1)

    @pl.when((back >= 0) & (back < half))
    def _():
        send(back).wait_send()

    @pl.when(back >= half)
    def _():
        store(back - half).wait()

    ahead = step + 1 - half

    @pl.when((ahead >= 0) & (ahead < half))
    def _():
        send(ahead).wait_recv()
        fetch(ahead).start()

    acc = acc_ref.at[lax.rem(step, N_ACC)]

    @pl.when(step < half)
    def _():
        acc[...] = jnp.zeros_like(acc)

    @pl.when(step >= half)
    def _():
        fetch(step - half).wait()

    compute(acc)

    @pl.when(step < half)
    def _():
        send(step).start()

    @pl.when(step >= half)
    def _():
        store(step - half).start()

    @pl.when(step == last)
    def _():
        for job in range(half - N_ACC + 1, half):
            store(job).wait()
        for exchange in exchanges:
            exchange.finish()


class Exchange:
    def __init__(self, own_ref, first, ref, stage_ref, send_sem, recv_sem, local_sem, stages=()):
        me = lax.axis_index('expert')
        flip = lambda dev, bit: dev + bit - 2 * bit * lax.rem(dev // bit, 2)
        core, x, y = flip(me, 1), flip(me, 2), flip(me, 4)
        diag = flip(x, 4)
        self.peers = [core, x, y]
        self.stages = stages
        rows = ref.shape[1] // 2
        plan = [
            (0, rows, None, x, x),
            (rows, rows, None, y, y),
            (rows, rows, None, x, x),
            (0, rows, None, y, y),
            (0, 2 * rows, None, core, core),
            (0, rows, x, diag, y),
            (rows, rows, y, diag, x),
            (0, rows, x, flip(x, 1), core),
            (rows, rows, y, flip(y, 1), core),
            (rows, rows, x, flip(x, 1), core),
            (0, rows, y, flip(y, 1), core),
            (0, rows, diag, flip(diag, 1), core),
            (rows, rows, diag, flip(diag, 1), core),
        ]

        def copy(k, source, block):
            return pltpu.make_async_remote_copy(
                src_ref=source, dst_ref=ref.at[block, pl.ds(plan[k][0], plan[k][1])], send_sem=send_sem.at[k],
                recv_sem=recv_sem.at[k], device_id={'expert': plan[k][4]}, device_id_type=MESH)

        self.out, self.into = [], []
        for k, (row, n_rows, here, arrives, _) in enumerate(plan):
            own = own_ref.at[pl.ds(first + row, n_rows)]
            self.out.append(copy(k, own if here is None else ref.at[here, pl.ds(row, n_rows)], me if here is None else here))
            self.into.append(copy(k, own, arrives))
        self.take = pltpu.make_async_copy(own_ref.at[pl.ds(first, 2 * rows)], stage_ref, local_sem.at[0])
        self.put = pltpu.make_async_copy(stage_ref, ref.at[me], local_sem.at[1])

    def stage(self, k):
        arrived, started = (((), (0, 1, 2, 3, 4)), ((0, 1), (5, 6, 7, 8)), ((2, 3), (9, 10)), ((5, 6), (11, 12)))[k]
        for n in arrived:
            self.into[n].wait_recv()
        for n in started:
            self.out[n].start()
        if k == 0:
            self.take.start()

    def settle(self):
        self.take.wait()
        self.put.start()

    def advance(self, step):
        for k, at in enumerate(self.stages):
            pl.when(step == at)(functools.partial(self.stage, k))
        pl.when(step == 1)(self.settle)

    def run(self):
        for k in range(4):
            self.stage(k)
            if k == 0:
                self.settle()
        self.finish()

    def finish(self):
        for k in (4,) + tuple(range(7, 13)):
            self.into[k].wait_recv()
        for copy in self.out:
            copy.wait_send()
        self.put.wait()


N_COPIES = 13


def exchange_scratch(rows, model):
    return [
        pltpu.VMEM((rows, model), BF16),
        pltpu.SemaphoreType.DMA((N_COPIES,)),
        pltpu.SemaphoreType.DMA((N_COPIES,)),
        pltpu.SemaphoreType.DMA((2,)),
    ]


def gather_body(first, own_ref, buf_ref, *scratch):
    exchange = Exchange(own_ref, first, buf_ref, *scratch)
    meet(exchange.peers)
    exchange.run()


def gather_now(array, first, rows, n_dev, collective_id):
    model = array.shape[1]
    return pl.pallas_call(
        functools.partial(gather_body, first),
        in_specs=[pl.BlockSpec(memory_space=pl.ANY)],
        out_specs=pl.BlockSpec(memory_space=pl.ANY),
        out_shape=jax.ShapeDtypeStruct((n_dev, rows, model), array.dtype),
        scratch_shapes=exchange_scratch(rows, model),
        compiler_params=pltpu.CompilerParams(collective_id=collective_id, has_side_effects=True),
        name='gather_now',
    )(array)


def hosted_parts(hosted, stages, own_refs, buf_refs, scratch):
    return [Exchange(own_refs[k], row, buf_refs[k], *scratch[4 * k:4 * k + 4], stages[k]) for k, (row, _) in enumerate(hosted)]


class Weights:
    def __init__(self, hbm, vmem, sem):
        self.n_local = vmem[0].shape[0]
        self.copies = lambda e: [
            pltpu.make_async_copy(src.at[e], dst.at[e], sem.at[e, k]) for k, (src, dst) in enumerate(zip(hbm, vmem))]

        @pl.when(pl.program_id(0) == 0)
        def _():
            for e in range(self.n_local):
                for copy in self.copies(e):
                    copy.start()

    def for_each(self, experts):
        def group(k, carry):
            @pl.when(pl.program_id(0) == 0)
            def _():
                for u in range(UNROLL):
                    for copy in self.copies(k * UNROLL + u):
                        copy.wait()

            experts([k * UNROLL + u for u in range(UNROLL)])
            return carry

        lax.fori_loop(0, self.n_local // UNROLL, group, 0)


def weight_scratch(w13, w2):
    return [pltpu.VMEM(w13.shape, BF16), pltpu.VMEM(w2.shape, BF16), pltpu.SemaphoreType.DMA((w13.shape[0], 2))]


def fwd_body(ffn, half, tile, start, n_x, n_carried, hosted, stages, *refs):
    refs = list(refs)
    x_refs, (g_ref, w13_hbm, w2_hbm), refs = refs[:n_x], refs[n_x:n_x + 3], refs[n_x + 3 + n_carried:]
    own_refs, refs = refs[:len(hosted)], refs[len(hosted):]
    (y_ref, inbox_ref), refs = refs[:2], refs[2:]
    buf_refs, refs = refs[:len(hosted)], refs[len(hosted):]
    w13_ref, w2_ref, w_sem, *refs = refs
    scratch, refs = refs[:5], refs[5:]
    exchanges = hosted_parts(hosted, stages, own_refs, buf_refs, refs)
    weights = Weights((w13_hbm, w2_hbm), (w13_ref, w2_ref), w_sem)

    def compute(acc):
        def experts(es):
            gates = [gate_column(g_ref[0, start:start + tile], e) for e in es]
            x = rows_joined(x_refs)
            pres = [dot(x, w13_ref[e]) for e in es]
            for gate, pre, e in zip(gates, pres, es):
                one, three = pre[:, :ffn], pre[:, ffn:]
                hidden = jnp.where(gate > 0.0, one * jax.nn.sigmoid(one) * three, 0.0).astype(BF16)
                acc[...] += gate * dot(hidden, w2_ref[e]).astype(BF16).astype(F32)

        weights.for_each(experts)

    pair_sum(compute, half, 1, tile, inbox_ref, (y_ref, start), exchanges, *scratch)


def pair_scratch(tile, model, half):
    return [
        pltpu.VMEM((N_ACC, tile, model), F32),
        pltpu.SemaphoreType.DMA((N_ACC,)),
        pltpu.SemaphoreType.DMA((half,)),
        pltpu.SemaphoreType.DMA((N_ACC,)),
        pltpu.SemaphoreType.DMA((N_ACC,)),
    ]


def pair_params(collective_id):
    return pltpu.CompilerParams(
        dimension_semantics=('arbitrary',), vmem_limit_bytes=VMEM_LIMIT, collective_id=collective_id, has_side_effects=True)


HBM = pl.BlockSpec(memory_space=pl.ANY)


def at_source(half):
    def index(i):
        return pair_source(i, half, 1)[0], 0, 0

    return index


def expert_fwd(xs, gates, w13, w2, start, carried, hosted, stages, collective_id):
    n_src, _, model = xs[0].shape
    tile = sum(x.shape[1] for x in xs)
    n_tok = gates.shape[1]
    n_local, ffn = w2.shape[:2]
    half = n_src // CORES
    at = at_source(half)
    flops = 2 * n_src * tile * n_local * model * ffn * 3
    outs = pl.pallas_call(
        functools.partial(fwd_body, ffn, half, tile, start, len(xs), len(carried), [h[1:] for h in hosted], stages),
        grid=(2 * half,),
        in_specs=[pl.BlockSpec((1, x.shape[1], model), at) for x in xs] + [pl.BlockSpec((1, n_tok, n_local), at)]
        + [HBM] * (2 + len(carried) + len(hosted)),
        out_specs=[HBM] * (2 + len(hosted)),
        out_shape=[jax.ShapeDtypeStruct((half, n_tok, model), F32), jax.ShapeDtypeStruct((half, tile, model), F32)]
        + [jax.ShapeDtypeStruct((n_src, rows, model), BF16) for _, _, rows in hosted],
        scratch_shapes=weight_scratch(w13, w2) + pair_scratch(tile, model, half)
        + [ref for _, _, rows in hosted for ref in exchange_scratch(rows, model)],
        input_output_aliases={len(xs) + 3 + i: i for i in range(len(carried))},
        compiler_params=pair_params(collective_id),
        cost_estimate=pl.CostEstimate(flops=flops, bytes_accessed=n_src * tile * model * 6, transcendentals=0),
        name='expert_fwd',
    )(*xs, gates, w13, w2, *carried, *[h[0] for h in hosted])
    return outs[0], outs[2:]


def bwd_body(ffn, half, start, first, n_carried, hosted, stages, x_ref, dy_ref, g_ref, w13_hbm, w2_hbm, *refs):
    refs = list(refs[n_carried:])
    own_refs, refs = refs[:len(hosted)], refs[len(hosted):]
    (dx_ref, da_ref, h_ref, inbox_ref), refs = refs[:4], refs[4:]
    buf_refs, refs = refs[:len(hosted)], refs[len(hosted):]
    w13_ref, w2_ref, w_sem, *refs = refs
    scratch, refs = refs[:5], refs[5:]
    exchanges = hosted_parts(hosted, stages, own_refs, buf_refs, refs)
    tile = x_ref.shape[-2]
    weights = Weights((w13_hbm, w2_hbm), (w13_ref, w2_ref), w_sem)

    def compute(acc):
        def experts(es):
            gates = [gate_column(g_ref[0, start:start + tile], e) for e in es]
            x = rows_joined([x_ref])
            pres = [dot(x, w13_ref[e]) for e in es]
            d_hids = []
            for gate, e in zip(gates, es):
                d_out = (gate * rows_joined([dy_ref]).astype(F32)).astype(BF16)
                d_hids.append(dot_t(d_out, w2_ref[e]).astype(BF16).astype(F32))
            for gate, pre, d_hid, e in zip(gates, pres, d_hids, es):
                live = gate > 0.0
                one, three = pre[:, :ffn], pre[:, ffn:]
                sig = jax.nn.sigmoid(one)
                act = one * sig
                h_ref[0, :, pl.ds(pl.multiple_of(e * ffn, ffn), ffn)] = jnp.where(live, act * three, 0.0).astype(BF16)
                d_one = jnp.where(live, d_hid * three * sig * (1.0 + one * (1.0 - sig)), 0.0).astype(BF16)
                d_three = jnp.where(live, d_hid * act, 0.0).astype(BF16)
                d_pre = jnp.concatenate([d_one, d_three], axis=1)
                da_ref[0, :, pl.ds(pl.multiple_of(2 * e * ffn, 2 * ffn), 2 * ffn)] = d_pre
                acc[...] += dot_t(d_pre, w13_ref[e]).astype(BF16).astype(F32)

        weights.for_each(experts)

    pair_sum(compute, half, 1, tile, inbox_ref, (dx_ref, first), exchanges, *scratch)


def expert_bwd(x, dy, gates, w13, w2, start, dx_rows, first, carried, hosted, stages, collective_id):
    n_src, tile, model = x[0].shape[0], x[0].shape[-2], x[0].shape[-1]
    n_tok = gates.shape[1]
    n_local, ffn = w2.shape[:2]
    half = n_src // CORES
    at = at_source(half)
    flops = 2 * n_src * tile * n_local * model * ffn * 5

    def rows_of(array, which):
        if array.ndim == 3:
            return pl.BlockSpec((1, tile, model), at)
        return pl.BlockSpec((1, 1, tile, model), lambda i: (pair_source(i, half, 1)[0], which, 0, 0))

    outs = pl.pallas_call(
        functools.partial(bwd_body, ffn, half, start, first, len(carried), [h[1:] for h in hosted], stages),
        grid=(2 * half,),
        in_specs=[rows_of(*x), rows_of(*dy), pl.BlockSpec((1, n_tok, n_local), at)]
        + [HBM] * (2 + len(carried) + len(hosted)),
        out_specs=[
            HBM,
            pl.BlockSpec((1, tile, 2 * ffn * n_local), at),
            pl.BlockSpec((1, tile, ffn * n_local), at),
        ] + [HBM] * (1 + len(hosted)),
        out_shape=[
            jax.ShapeDtypeStruct((half, dx_rows, model), F32),
            jax.ShapeDtypeStruct((n_src, tile, 2 * ffn * n_local), BF16),
            jax.ShapeDtypeStruct((n_src, tile, ffn * n_local), BF16),
            jax.ShapeDtypeStruct((half, tile, model), F32),
        ] + [jax.ShapeDtypeStruct((n_src, rows, model), BF16) for _, _, rows in hosted],
        scratch_shapes=weight_scratch(w13, w2) + pair_scratch(tile, model, half)
        + [ref for _, _, rows in hosted for ref in exchange_scratch(rows, model)],
        input_output_aliases={5 + i: 0 for i in range(len(carried))},
        compiler_params=pair_params(collective_id),
        cost_estimate=pl.CostEstimate(flops=flops, bytes_accessed=n_src * tile * model * 14, transcendentals=0),
        name='expert_bwd',
    )(x[0], dy[0], gates, w13, w2, *carried, *[h[0] for h in hosted])
    return outs[0], outs[1], outs[2], outs[4:]


def rows_joined(refs, column=0, columns=None):
    parts = [ref[(0,) * (len(ref.shape) - 2) + (slice(None), slice(column, column + (columns or ref.shape[-1])))] for ref in refs]
    return parts[0] if len(parts) == 1 else jnp.concatenate(parts, axis=0)


def grad_body(ffn, n_parts, g_ref, *refs):
    x_refs, dy_refs, da_refs, h_refs = (refs[k * n_parts:(k + 1) * n_parts] for k in range(4))
    dw1_ref, dw3_ref, dw2_ref, acc13_ref, acc2_ref = refs[4 * n_parts:]
    e, k = pl.program_id(0), pl.program_id(1)

    @pl.when(k == 0)
    def _():
        acc13_ref[...] = jnp.zeros_like(acc13_ref)
        acc2_ref[...] = jnp.zeros_like(acc2_ref)

    for m in range(0, acc13_ref.shape[0], ffn):
        acc13_ref[m:m + ffn] += dot_a(rows_joined(x_refs, m, ffn), rows_joined(da_refs))
    d_out = (gate_column(g_ref[0], e) * rows_joined(dy_refs).astype(F32)).astype(BF16)
    acc2_ref[...] += dot_a(rows_joined(h_refs), d_out)

    @pl.when(k == pl.num_programs(1) - 1)
    def _():
        dw1_ref[0] = acc13_ref[:, :ffn].astype(BF16)
        dw3_ref[0] = acc13_ref[:, ffn:].astype(BF16)
        dw2_ref[0] = acc2_ref[...].astype(BF16)


def weight_grads(gates, xs, dys, d_pres, hiddens):
    n_src, n_tok, n_local = gates.shape
    model = xs[0][0].shape[-1]
    ffn = hiddens[0].shape[2] // n_local
    flops = 2 * n_src * n_tok * n_local * model * ffn * 3
    at = lambda e, k: (k, 0, 0)
    at_e = lambda e, k: (k, 0, e)
    out = lambda e, k: (e, 0, 0)

    def rows_of(array, which):
        block = (1,) * (array.ndim - 2) + array.shape[-2:]
        return pl.BlockSpec(block, at if array.ndim == 3 else (lambda e, k: (k, which, 0, 0)))


    return pl.pallas_call(
        functools.partial(grad_body, ffn, len(xs)),
        grid=(n_local, n_src),
        in_specs=[pl.BlockSpec((1, n_tok, n_local), at)]
        + [rows_of(*x) for x in list(xs) + list(dys)]
        + [pl.BlockSpec((1, d.shape[1], 2 * ffn), at_e) for d in d_pres]
        + [pl.BlockSpec((1, h.shape[1], ffn), at_e) for h in hiddens],
        out_specs=[
            pl.BlockSpec((1, model, ffn), out),
            pl.BlockSpec((1, model, ffn), out),
            pl.BlockSpec((1, ffn, model), out),
        ],
        out_shape=[
            jax.ShapeDtypeStruct((n_local, model, ffn), BF16),
            jax.ShapeDtypeStruct((n_local, model, ffn), BF16),
            jax.ShapeDtypeStruct((n_local, ffn, model), BF16),
        ],
        scratch_shapes=[pltpu.VMEM((model, 2 * ffn), F32), pltpu.VMEM((ffn, model), F32)],
        compiler_params=pltpu.CompilerParams(dimension_semantics=('arbitrary', 'arbitrary'), vmem_limit_bytes=VMEM_LIMIT),
        cost_estimate=pl.CostEstimate(flops=flops, bytes_accessed=n_src * n_tok * model * 4 * n_local, transcendentals=0),
        name='weight_grads',
    )(gates, *[x for x, _ in xs], *[dy for dy, _ in dys], *d_pres, *hiddens)


def solution(mesh):
    n_stage = mesh.shape['stage']
    n_dev = mesh.shape['expert']
    to_next = [(stage_idx, (stage_idx + 1) % n_stage) for stage_idx in range(n_stage)]
    to_prev = [((stage_idx + 1) % n_stage, stage_idx) for stage_idx in range(n_stage)]
    tok_spec = P('stage', 'expert', None)
    w_spec = P('stage', 'expert', None, None)
    same_core = [list(range(core, n_dev, CORES)) for core in range(CORES)]

    def moe_body(x_act, route_idx, route_wts, w_one, w_three, w_two, dy_act):
        x_src = x_act[0]
        n_tok, _ = x_src.shape
        n_local = w_one.shape[1]
        n_exp = n_local * n_dev

        def gather(rows):
            return lax.all_gather(rows, 'expert', axis=0, tiled=False)

        def reduce_rows(part):
            return lax.psum_scatter(part, 'expert', scatter_dimension=0, axis_index_groups=same_core, tiled=False).astype(BF16)

        hits = route_idx[0][:, :, None] == jnp.arange(n_exp, dtype=jnp.int32)
        gate_src = jnp.sum(jnp.where(hits, route_wts[0][:, :, None], 0.0), axis=1)
        gate_src = jnp.transpose(gate_src.reshape(n_tok, n_dev, n_local), (1, 2, 0))
        gate_dst = lax.ppermute(gate_src, 'stage', to_next)
        gates = jnp.transpose(lax.all_to_all(gate_dst, 'expert', 0, 0), (0, 2, 1))

        w13 = jnp.concatenate([w_one[0], w_three[0]], axis=2)
        w2 = w_two[0]

        def spans(sizes):
            ends = [sum(sizes[:k + 1]) for k in range(len(sizes))]
            return [slice(end - size, end) for end, size in zip(ends, sizes)]

        bwd, fwd = spans(BWD_ROWS), spans(FWD_ROWS)
        dx_rows = sum(BWD_ROWS[:2]), BWD_ROWS[2]

        def hop(rows):
            return lax.ppermute(x_src[rows], 'stage', to_next)

        dys = [(gather_now(dy_act[0], 0, BWD_ROWS[0], n_dev, 5), 0)]
        xs = [(gather(hop(bwd[0])), 0)]
        for k in (1, 2):
            x_dst = hop(bwd[k])
            both = gather(jnp.stack([dy_act[0, bwd[k]], x_dst]))
            dys.append((both, 0))
            xs.append((both, 1))
        x_half = [hop(fwd[k]) for k in range(2)]
        pieces = [(x_half[k], first, X_ROWS) for k in range(2) for first in range(0, FWD_ROWS[k], X_ROWS)]
        hosts = {'bwd_1': pieces[:1], 'bwd_2': pieces[1:3], 'fwd_0': pieces[3:]}

        x_fwd, d_pres, hiddens = [], [], []
        dx_parts = []
        for k in range(3):
            dx_part, d_pre, hidden, arrived = expert_bwd(
                xs[k], dys[k], gates, w13, w2, bwd[k].start, dx_rows[k // 2], BWD_ROWS[0] if k == 1 else 0,
                (dx_part,) if k == 1 else (), hosts.get(f'bwd_{k}', ()), STAGES.get(f'bwd_{k}'), k)
            x_fwd += arrived
            d_pres.append(d_pre)
            hiddens.append(hidden)
            if k > 0:
                dx_dst = reduce_rows(dx_part)
                dx_parts.append(lax.ppermute(dx_dst, 'stage', to_prev))
        dx_out = jnp.concatenate(dx_parts, axis=0)

        y_part = ()
        for k in range(2):
            out, arrived = expert_fwd(
                x_fwd[2 * k:2 * k + 2], gates, w13, w2, fwd[k].start, y_part, hosts.get(f'fwd_{k}', ()), STAGES.get(f'fwd_{k}'), 3 + k)
            y_part = (out,)
            x_fwd += arrived
        y_out = reduce_rows(y_part[0])

        g_one, g_three, g_two = weight_grads(gates, xs, dys, d_pres, hiddens)
        return y_out[None], dx_out[None], g_one[None], g_three[None], g_two[None]

    return jax.shard_map(moe_body, mesh=mesh, in_specs=(tok_spec, tok_spec, tok_spec, w_spec, w_spec, w_spec, tok_spec), out_specs=(tok_spec, tok_spec, w_spec, w_spec, w_spec), check_vma=False)
```

```python
import functools

import jax
import jax.numpy as jnp
from jax import lax
from jax.experimental import pallas as pl
from jax.experimental.pallas import tpu as pltpu
from jax.sharding import PartitionSpec as P


F32 = jnp.float32
BF16 = jnp.bfloat16
BWD_ROWS = (256, 384, 384)
FWD_ROWS = (512, 512)
X_ROWS = (256, 512, 256)
STAGES = (0, 2, 4, 6), (0, 3, 5, 7), (0, 2, 4, 6)
VMEM_LIMIT = 65400 * 1024
N_ACC = 3
CORES = 2
UNROLL = 2
BLOCK = 256
MESH = pl.DeviceIdType.MESH


def dot(lhs, rhs):
    return jnp.dot(lhs, rhs, preferred_element_type=F32)


def dot_t(lhs, rhs):
    return lax.dot_general(lhs, rhs, (((1,), (1,)), ((), ())), preferred_element_type=F32)


def dot_a(lhs, rhs):
    return lax.dot_general(lhs, rhs, (((0,), (0,)), ((), ())), preferred_element_type=F32)


def gate_column(gates, expert):
    lanes = lax.broadcasted_iota(jnp.int32, gates.shape, 1)
    return jnp.sum(jnp.where(lanes == expert, gates, 0.0), axis=1, keepdims=True)


def meet(peers):
    barrier = pltpu.get_barrier_semaphore()
    for peer in peers:
        pl.semaphore_signal(barrier, inc=1, device_id={'expert': peer}, device_id_type=MESH)
    pl.semaphore_wait(barrier, len(peers))


def pair_source(step, half, steps):
    core = lax.rem(lax.axis_index('expert'), CORES)
    mine = step // half
    tile = lax.rem(step, half)
    lane = lax.rem(core + 1 + mine, CORES)
    return CORES * (tile // steps) + lane, lax.rem(tile, steps)


def pair_sum(compute, half, steps, tile, inbox_ref, out, exchanges, acc_ref, send_sem, recv_sem, in_sem, out_sem):
    step = pl.program_id(0)
    last = 2 * half - 1
    me = lax.axis_index('expert')
    other = me + 1 - 2 * lax.rem(me, CORES)

    def at(ref, job):
        return ref.at[job // steps, pl.ds(lax.rem(job, steps) * tile, tile)]

    def store(job):
        slot = lax.rem(job + half, N_ACC)
        out_ref, first = out
        rows = pl.ds(first + lax.rem(job, steps) * tile, tile)
        return pltpu.make_async_copy(acc_ref.at[slot], out_ref.at[job // steps, rows], out_sem.at[slot])

    def send(job):
        slot = lax.rem(job, N_ACC)
        return pltpu.make_async_remote_copy(
            src_ref=acc_ref.at[slot], dst_ref=at(inbox_ref, job), send_sem=send_sem.at[slot], recv_sem=recv_sem.at[job],
            device_id={'expert': other}, device_id_type=MESH)

    def fetch(job):
        slot = lax.rem(job + half, N_ACC)
        return pltpu.make_async_copy(at(inbox_ref, job), acc_ref.at[slot], in_sem.at[slot])

    @pl.when(step == 0)
    def _():
        meet(exchanges[0].peers if exchanges else [other])

    for exchange in exchanges:
        exchange.advance(step)

    back = step - (N_ACC - 1)

    @pl.when((back >= 0) & (back < half))
    def _():
        send(back).wait_send()

    @pl.when(back >= half)
    def _():
        store(back - half).wait()

    ahead = step + 1 - half

    @pl.when((ahead >= 0) & (ahead < half))
    def _():
        send(ahead).wait_recv()
        fetch(ahead).start()

    acc = acc_ref.at[lax.rem(step, N_ACC)]

    @pl.when(step >= half)
    def _():
        fetch(step - half).wait()

    def add(expert, rows):
        fresh = (expert == 0) & (step < half)
        acc[...] = jnp.where(fresh, 0.0, acc[...]) + rows

    compute(add)

    @pl.when(step < half)
    def _():
        send(step).start()

    @pl.when(step >= half)
    def _():
        store(step - half).start()

    @pl.when(step == last)
    def _():
        for job in range(half - N_ACC + 1, half):
            store(job).wait()
        for exchange in exchanges:
            exchange.finish()


class Exchange:
    def __init__(self, own_ref, first, ref, stage_ref, send_sem, recv_sem, local_sem, stages=()):
        me = lax.axis_index('expert')
        flip = lambda dev, bit: dev + bit - 2 * bit * lax.rem(dev // bit, 2)
        core, x, y = flip(me, 1), flip(me, 2), flip(me, 4)
        diag = flip(x, 4)
        self.peers = [core, x, y]
        self.stages = stages
        rows = ref.shape[1] // 2
        plan = [
            (0, rows, None, x, x),
            (rows, rows, None, y, y),
            (rows, rows, None, x, x),
            (0, rows, None, y, y),
            (0, 2 * rows, None, core, core),
            (0, rows, x, diag, y),
            (rows, rows, y, diag, x),
            (0, rows, x, flip(x, 1), core),
            (rows, rows, y, flip(y, 1), core),
            (rows, rows, x, flip(x, 1), core),
            (0, rows, y, flip(y, 1), core),
            (0, rows, diag, flip(diag, 1), core),
            (rows, rows, diag, flip(diag, 1), core),
        ]

        def copy(k, source, block):
            return pltpu.make_async_remote_copy(
                src_ref=source, dst_ref=ref.at[block, pl.ds(plan[k][0], plan[k][1])], send_sem=send_sem.at[k],
                recv_sem=recv_sem.at[k], device_id={'expert': plan[k][4]}, device_id_type=MESH)

        self.out, self.into = [], []
        for k, (row, n_rows, here, arrives, _) in enumerate(plan):
            own = own_ref.at[pl.ds(first + row, n_rows)]
            self.out.append(copy(k, own if here is None else ref.at[here, pl.ds(row, n_rows)], me if here is None else here))
            self.into.append(copy(k, own, arrives))
        self.take = pltpu.make_async_copy(own_ref.at[pl.ds(first, 2 * rows)], stage_ref, local_sem.at[0])
        self.put = pltpu.make_async_copy(stage_ref, ref.at[me], local_sem.at[1])

    def stage(self, k):
        arrived, started = (((), (0, 1, 2, 3, 4)), ((0, 1), (5, 6, 7, 8)), ((2, 3), (9, 10)), ((5, 6), (11, 12)))[k]
        for n in arrived:
            self.into[n].wait_recv()
        for n in started:
            self.out[n].start()
        if k == 0:
            self.take.start()

    def settle(self):
        self.take.wait()
        self.put.start()

    def advance(self, step):
        for k, at in enumerate(self.stages):
            pl.when(step == at)(functools.partial(self.stage, k))
        pl.when(step == 1)(self.settle)

    def run(self):
        for k in range(4):
            self.stage(k)
            if k == 0:
                self.settle()
        self.finish()

    def finish(self):
        for k in (4,) + tuple(range(7, 13)):
            self.into[k].wait_recv()
        for copy in self.out:
            copy.wait_send()
        self.put.wait()


N_COPIES = 13


def exchange_scratch(rows, model):
    return [
        pltpu.VMEM((rows, model), BF16),
        pltpu.SemaphoreType.DMA((N_COPIES,)),
        pltpu.SemaphoreType.DMA((N_COPIES,)),
        pltpu.SemaphoreType.DMA((2,)),
    ]


def gather_body(first, own_ref, buf_ref, *scratch):
    exchange = Exchange(own_ref, first, buf_ref, *scratch)
    meet(exchange.peers)
    exchange.run()


def gather_now(array, first, rows, n_dev, collective_id):
    model = array.shape[1]
    return pl.pallas_call(
        functools.partial(gather_body, first),
        in_specs=[pl.BlockSpec(memory_space=pl.ANY)],
        out_specs=pl.BlockSpec(memory_space=pl.ANY),
        out_shape=jax.ShapeDtypeStruct((n_dev, rows, model), array.dtype),
        scratch_shapes=exchange_scratch(rows, model),
        compiler_params=pltpu.CompilerParams(collective_id=collective_id, has_side_effects=True),
        name='gather_now',
    )(array)


def hosted_parts(hosted, stages, own_refs, buf_refs, scratch):
    return [Exchange(own_refs[k], row, buf_refs[k], *scratch[4 * k:4 * k + 4], stages[k]) for k, (row, _) in enumerate(hosted)]


class Weights:
    def __init__(self, hbm, vmem, sem):
        self.n_local = vmem[0].shape[0]
        self.copies = lambda e: [
            pltpu.make_async_copy(src.at[e], dst.at[e], sem.at[e, k]) for k, (src, dst) in enumerate(zip(hbm, vmem))]

        @pl.when(pl.program_id(0) == 0)
        def _():
            for e in range(self.n_local):
                for copy in self.copies(e):
                    copy.start()

    def for_each(self, experts):
        def group(k, carry):
            @pl.when(pl.program_id(0) == 0)
            def _():
                for u in range(UNROLL):
                    for copy in self.copies(k * UNROLL + u):
                        copy.wait()

            experts([k * UNROLL + u for u in range(UNROLL)])
            return carry

        lax.fori_loop(0, self.n_local // UNROLL, group, 0)


def weight_scratch(w13, w2):
    return [pltpu.VMEM(w13.shape, BF16), pltpu.VMEM(w2.shape, BF16), pltpu.SemaphoreType.DMA((w13.shape[0], 2))]


def fwd_body(ffn, half, tile, start, n_x, n_carried, hosted, stages, *refs):
    refs = list(refs)
    x_refs, (g_ref, w13_hbm, w2_hbm), refs = refs[:n_x], refs[n_x:n_x + 3], refs[n_x + 3 + n_carried:]
    own_refs, refs = refs[:len(hosted)], refs[len(hosted):]
    (y_ref, inbox_ref), refs = refs[:2], refs[2:]
    buf_refs, refs = refs[:len(hosted)], refs[len(hosted):]
    w13_ref, w2_ref, w_sem, *refs = refs
    scratch, refs = refs[:5], refs[5:]
    exchanges = hosted_parts(hosted, stages, own_refs, buf_refs, refs)
    weights = Weights((w13_hbm, w2_hbm), (w13_ref, w2_ref), w_sem)

    def compute(add):
        def experts(es):
            gates = [gate_column(g_ref[0, start:start + tile], e) for e in es]
            x = rows_joined(x_refs)
            pres = [dot(x, w13_ref[e]) for e in es]
            for gate, pre, e in zip(gates, pres, es):
                one, three = pre[:, :ffn], pre[:, ffn:]
                hidden = jnp.where(gate > 0.0, one * jax.nn.sigmoid(one) * three, 0.0).astype(BF16)
                add(e, gate * dot(hidden, w2_ref[e]).astype(BF16).astype(F32))

        weights.for_each(experts)

    pair_sum(compute, half, 1, tile, inbox_ref, (y_ref, start), exchanges, *scratch)


def pair_scratch(tile, model, half):
    return [
        pltpu.VMEM((N_ACC, tile, model), F32),
        pltpu.SemaphoreType.DMA((N_ACC,)),
        pltpu.SemaphoreType.DMA((half,)),
        pltpu.SemaphoreType.DMA((N_ACC,)),
        pltpu.SemaphoreType.DMA((N_ACC,)),
    ]


def pair_params(collective_id):
    return pltpu.CompilerParams(
        dimension_semantics=('arbitrary',), vmem_limit_bytes=VMEM_LIMIT, collective_id=collective_id, has_side_effects=True)


HBM = pl.BlockSpec(memory_space=pl.ANY)


def at_source(half):
    def index(i):
        return pair_source(i, half, 1)[0], 0, 0

    return index


def expert_fwd(xs, gates, w13, w2, start, carried, hosted, stages, collective_id):
    n_src, _, model = xs[0][0].shape
    tile = BLOCK * len(xs)
    n_tok = gates.shape[1]
    n_local, ffn = w2.shape[:2]
    half = n_src // CORES
    at = at_source(half)
    flops = 2 * n_src * tile * n_local * model * ffn * 3

    def rows_of(block):
        return pl.BlockSpec((1, BLOCK, model), lambda i: (pair_source(i, half, 1)[0], block, 0))

    outs = pl.pallas_call(
        functools.partial(fwd_body, ffn, half, tile, start, len(xs), len(carried), [h[1:] for h in hosted], stages),
        grid=(2 * half,),
        in_specs=[rows_of(block) for _, block in xs] + [pl.BlockSpec((1, n_tok, n_local), at)]
        + [HBM] * (2 + len(carried) + len(hosted)),
        out_specs=[HBM] * (2 + len(hosted)),
        out_shape=[jax.ShapeDtypeStruct((half, n_tok, model), F32), jax.ShapeDtypeStruct((half, tile, model), F32)]
        + [jax.ShapeDtypeStruct((n_src, rows, model), BF16) for _, _, rows in hosted],
        scratch_shapes=weight_scratch(w13, w2) + pair_scratch(tile, model, half)
        + [ref for _, _, rows in hosted for ref in exchange_scratch(rows, model)],
        input_output_aliases={len(xs) + 3 + i: i for i in range(len(carried))},
        compiler_params=pair_params(collective_id),
        cost_estimate=pl.CostEstimate(flops=flops, bytes_accessed=n_src * tile * model * 6, transcendentals=0),
        name='expert_fwd',
    )(*[x for x, _ in xs], gates, w13, w2, *carried, *[h[0] for h in hosted])
    return outs[0], outs[2:]


def bwd_body(ffn, half, start, first, n_carried, hosted, stages, x_ref, dy_ref, g_ref, w13_hbm, w2_hbm, *refs):
    refs = list(refs[n_carried:])
    own_refs, refs = refs[:len(hosted)], refs[len(hosted):]
    (dx_ref, da_ref, h_ref, inbox_ref), refs = refs[:4], refs[4:]
    buf_refs, refs = refs[:len(hosted)], refs[len(hosted):]
    w13_ref, w2_ref, w_sem, *refs = refs
    scratch, refs = refs[:5], refs[5:]
    exchanges = hosted_parts(hosted, stages, own_refs, buf_refs, refs)
    tile = x_ref.shape[-2]
    weights = Weights((w13_hbm, w2_hbm), (w13_ref, w2_ref), w_sem)

    def compute(add):
        def experts(es):
            gates = [gate_column(g_ref[0, start:start + tile], e) for e in es]
            x = rows_joined([x_ref])
            pres = [dot(x, w13_ref[e]) for e in es]
            d_hids = []
            for gate, e in zip(gates, es):
                d_out = (gate * rows_joined([dy_ref]).astype(F32)).astype(BF16)
                d_hids.append(dot_t(d_out, w2_ref[e]).astype(BF16).astype(F32))
            for gate, pre, d_hid, e in zip(gates, pres, d_hids, es):
                live = gate > 0.0
                one, three = pre[:, :ffn], pre[:, ffn:]
                sig = jax.nn.sigmoid(one)
                act = one * sig
                h_ref[0, :, pl.ds(pl.multiple_of(e * ffn, ffn), ffn)] = jnp.where(live, act * three, 0.0).astype(BF16)
                d_one = jnp.where(live, d_hid * three * sig * (1.0 + one * (1.0 - sig)), 0.0).astype(BF16)
                d_three = jnp.where(live, d_hid * act, 0.0).astype(BF16)
                d_pre = jnp.concatenate([d_one, d_three], axis=1)
                da_ref[0, :, pl.ds(pl.multiple_of(2 * e * ffn, 2 * ffn), 2 * ffn)] = d_pre
                add(e, dot_t(d_pre, w13_ref[e]).astype(BF16).astype(F32))

        weights.for_each(experts)

    pair_sum(compute, half, 1, tile, inbox_ref, (dx_ref, first), exchanges, *scratch)


def expert_bwd(x, dy, gates, w13, w2, start, dx_rows, first, carried, hosted, stages, collective_id):
    n_src, tile, model = x[0].shape[0], x[0].shape[-2], x[0].shape[-1]
    n_tok = gates.shape[1]
    n_local, ffn = w2.shape[:2]
    half = n_src // CORES
    at = at_source(half)
    flops = 2 * n_src * tile * n_local * model * ffn * 5

    def rows_of(array, which):
        if array.ndim == 3:
            return pl.BlockSpec((1, tile, model), at)
        return pl.BlockSpec((1, 1, tile, model), lambda i: (pair_source(i, half, 1)[0], which, 0, 0))

    outs = pl.pallas_call(
        functools.partial(bwd_body, ffn, half, start, first, len(carried), [h[1:] for h in hosted], stages),
        grid=(2 * half,),
        in_specs=[rows_of(*x), rows_of(*dy), pl.BlockSpec((1, n_tok, n_local), at)]
        + [HBM] * (2 + len(carried) + len(hosted)),
        out_specs=[
            HBM,
            pl.BlockSpec((1, tile, 2 * ffn * n_local), at),
            pl.BlockSpec((1, tile, ffn * n_local), at),
        ] + [HBM] * (1 + len(hosted)),
        out_shape=[
            jax.ShapeDtypeStruct((half, dx_rows, model), F32),
            jax.ShapeDtypeStruct((n_src, tile, 2 * ffn * n_local), BF16),
            jax.ShapeDtypeStruct((n_src, tile, ffn * n_local), BF16),
            jax.ShapeDtypeStruct((half, tile, model), F32),
        ] + [jax.ShapeDtypeStruct((n_src, rows, model), BF16) for _, _, rows in hosted],
        scratch_shapes=weight_scratch(w13, w2) + pair_scratch(tile, model, half)
        + [ref for _, _, rows in hosted for ref in exchange_scratch(rows, model)],
        input_output_aliases={5 + i: 0 for i in range(len(carried))},
        compiler_params=pair_params(collective_id),
        cost_estimate=pl.CostEstimate(flops=flops, bytes_accessed=n_src * tile * model * 14, transcendentals=0),
        name='expert_bwd',
    )(x[0], dy[0], gates, w13, w2, *carried, *[h[0] for h in hosted])
    return outs[0], outs[1], outs[2], outs[4:]


def rows_joined(refs, column=0, columns=None):
    parts = [ref[(0,) * (len(ref.shape) - 2) + (slice(None), slice(column, column + (columns or ref.shape[-1])))] for ref in refs]
    return parts[0] if len(parts) == 1 else jnp.concatenate(parts, axis=0)


def grad_body(ffn, n_parts, g_ref, *refs):
    x_refs, dy_refs, da_refs, h_refs = (refs[k * n_parts:(k + 1) * n_parts] for k in range(4))
    dw1_ref, dw3_ref, dw2_ref, acc13_ref, acc2_ref = refs[4 * n_parts:]
    e, k = pl.program_id(0), pl.program_id(1)

    @pl.when(k == 0)
    def _():
        acc13_ref[...] = jnp.zeros_like(acc13_ref)
        acc2_ref[...] = jnp.zeros_like(acc2_ref)

    for m in range(0, acc13_ref.shape[0], ffn):
        acc13_ref[m:m + ffn] += dot_a(rows_joined(x_refs, m, ffn), rows_joined(da_refs))
    d_out = (gate_column(g_ref[0], e) * rows_joined(dy_refs).astype(F32)).astype(BF16)
    acc2_ref[...] += dot_a(rows_joined(h_refs), d_out)

    @pl.when(k == pl.num_programs(1) - 1)
    def _():
        dw1_ref[0] = acc13_ref[:, :ffn].astype(BF16)
        dw3_ref[0] = acc13_ref[:, ffn:].astype(BF16)
        dw2_ref[0] = acc2_ref[...].astype(BF16)


def weight_grads(gates, xs, dys, d_pres, hiddens):
    n_src, n_tok, n_local = gates.shape
    model = xs[0][0].shape[-1]
    ffn = hiddens[0].shape[2] // n_local
    flops = 2 * n_src * n_tok * n_local * model * ffn * 3
    at = lambda e, k: (k, 0, 0)
    at_e = lambda e, k: (k, 0, e)
    out = lambda e, k: (e, 0, 0)

    def rows_of(array, which):
        block = (1,) * (array.ndim - 2) + array.shape[-2:]
        return pl.BlockSpec(block, at if array.ndim == 3 else (lambda e, k: (k, which, 0, 0)))


    return pl.pallas_call(
        functools.partial(grad_body, ffn, len(xs)),
        grid=(n_local, n_src),
        in_specs=[pl.BlockSpec((1, n_tok, n_local), at)]
        + [rows_of(*x) for x in list(xs) + list(dys)]
        + [pl.BlockSpec((1, d.shape[1], 2 * ffn), at_e) for d in d_pres]
        + [pl.BlockSpec((1, h.shape[1], ffn), at_e) for h in hiddens],
        out_specs=[
            pl.BlockSpec((1, model, ffn), out),
            pl.BlockSpec((1, model, ffn), out),
            pl.BlockSpec((1, ffn, model), out),
        ],
        out_shape=[
            jax.ShapeDtypeStruct((n_local, model, ffn), BF16),
            jax.ShapeDtypeStruct((n_local, model, ffn), BF16),
            jax.ShapeDtypeStruct((n_local, ffn, model), BF16),
        ],
        scratch_shapes=[pltpu.VMEM((model, 2 * ffn), F32), pltpu.VMEM((ffn, model), F32)],
        compiler_params=pltpu.CompilerParams(dimension_semantics=('arbitrary', 'arbitrary'), vmem_limit_bytes=VMEM_LIMIT),
        cost_estimate=pl.CostEstimate(flops=flops, bytes_accessed=n_src * n_tok * model * 4 * n_local, transcendentals=0),
        name='weight_grads',
    )(gates, *[x for x, _ in xs], *[dy for dy, _ in dys], *d_pres, *hiddens)


def solution(mesh):
    n_stage = mesh.shape['stage']
    n_dev = mesh.shape['expert']
    to_next = [(stage_idx, (stage_idx + 1) % n_stage) for stage_idx in range(n_stage)]
    to_prev = [((stage_idx + 1) % n_stage, stage_idx) for stage_idx in range(n_stage)]
    tok_spec = P('stage', 'expert', None)
    w_spec = P('stage', 'expert', None, None)
    same_core = [list(range(core, n_dev, CORES)) for core in range(CORES)]

    def moe_body(x_act, route_idx, route_wts, w_one, w_three, w_two, dy_act):
        x_src = x_act[0]
        n_tok, _ = x_src.shape
        n_local = w_one.shape[1]
        n_exp = n_local * n_dev

        def gather(rows):
            return lax.all_gather(rows, 'expert', axis=0, tiled=False)

        def reduce_rows(part):
            return lax.psum_scatter(part, 'expert', scatter_dimension=0, axis_index_groups=same_core, tiled=False).astype(BF16)

        hits = route_idx[0][:, :, None] == jnp.arange(n_exp, dtype=jnp.int32)
        gate_src = jnp.sum(jnp.where(hits, route_wts[0][:, :, None], 0.0), axis=1)
        gate_src = jnp.transpose(gate_src.reshape(n_tok, n_dev, n_local), (1, 2, 0))
        gate_dst = lax.ppermute(gate_src, 'stage', to_next)
        gates = jnp.transpose(lax.all_to_all(gate_dst, 'expert', 0, 0), (0, 2, 1))

        w13 = jnp.concatenate([w_one[0], w_three[0]], axis=2)
        w2 = w_two[0]

        def spans(sizes):
            ends = [sum(sizes[:k + 1]) for k in range(len(sizes))]
            return [slice(end - size, end) for end, size in zip(ends, sizes)]

        bwd, fwd = spans(BWD_ROWS), spans(FWD_ROWS)
        dx_rows = sum(BWD_ROWS[:2]), BWD_ROWS[2]

        def hop(rows):
            return lax.ppermute(x_src[rows], 'stage', to_next)

        dys = [(gather_now(dy_act[0], 0, BWD_ROWS[0], n_dev, 5), 0)]
        xs = [(gather(hop(bwd[0])), 0)]
        for k in (1, 2):
            x_dst = hop(bwd[k])
            both = gather(jnp.stack([dy_act[0, bwd[k]], x_dst]))
            dys.append((both, 0))
            xs.append((both, 1))
        cut = sum(X_ROWS[:2])
        x_lo, x_hi = hop(slice(0, cut)), hop(slice(cut, n_tok))
        pieces = (x_lo, 0, X_ROWS[0]), (x_lo, X_ROWS[0], X_ROWS[1]), (x_hi, 0, X_ROWS[2])

        def blocks(arrived):
            return [(x, block) for x in arrived for block in range(x.shape[1] // BLOCK)]

        x_fwd, d_pres, hiddens = [], [], []
        dx_parts = []
        for k in range(3):
            dx_part, d_pre, hidden, arrived = expert_bwd(
                xs[k], dys[k], gates, w13, w2, bwd[k].start, dx_rows[k // 2], BWD_ROWS[0] if k == 1 else 0,
                (dx_part,) if k == 1 else (), pieces[k - 1:k] if k else (), STAGES[k - 1:k], k)
            x_fwd += blocks(arrived)
            d_pres.append(d_pre)
            hiddens.append(hidden)
            if k > 0:
                dx_dst = reduce_rows(dx_part)
                dx_parts.append(lax.ppermute(dx_dst, 'stage', to_prev))
        dx_out = jnp.concatenate(dx_parts, axis=0)[None]

        y_part = ()
        for k in range(2):
            out, arrived = expert_fwd(
                x_fwd[2 * k:2 * k + 2], gates, w13, w2, fwd[k].start, y_part, () if k else pieces[2:], STAGES[2:], 3 + k)
            y_part = (out,)
            x_fwd += blocks(arrived)
        y_out = reduce_rows(y_part[0])

        g_one, g_three, g_two = weight_grads(gates, xs, dys, d_pres, hiddens)
        return y_out[None], dx_out, g_one[None], g_three[None], g_two[None]

    return jax.shard_map(moe_body, mesh=mesh, in_specs=(tok_spec, tok_spec, tok_spec, w_spec, w_spec, w_spec, tok_spec), out_specs=(tok_spec, tok_spec, w_spec, w_spec, w_spec), check_vma=False)
```

```python
import functools

import jax
import jax.numpy as jnp
from jax import lax
from jax.experimental import pallas as pl
from jax.experimental.pallas import tpu as pltpu
from jax.sharding import PartitionSpec as P


F32 = jnp.float32
BF16 = jnp.bfloat16
BWD_ROWS = (256, 384, 384)
FWD_ROWS = (512, 512)
X_ROWS = (256, 512, 256)
STAGES = (0, 2, 4, 6), (0, 3, 5, 7), (0, 2, 4, 6)
VMEM_LIMIT = 65400 * 1024
N_ACC = 3
CORES = 2
UNROLL = 2
BLOCK = 256
MESH = pl.DeviceIdType.MESH


def dot(lhs, rhs):
    return jnp.dot(lhs, rhs, preferred_element_type=F32)


def dot_t(lhs, rhs):
    return lax.dot_general(lhs, rhs, (((1,), (1,)), ((), ())), preferred_element_type=F32)


def dot_a(lhs, rhs):
    return lax.dot_general(lhs, rhs, (((0,), (0,)), ((), ())), preferred_element_type=F32)


def gate_column(gates, expert):
    lanes = lax.broadcasted_iota(jnp.int32, gates.shape, 1)
    return jnp.sum(jnp.where(lanes == expert, gates, 0.0), axis=1, keepdims=True)


def meet(peers):
    barrier = pltpu.get_barrier_semaphore()
    for peer in peers:
        pl.semaphore_signal(barrier, inc=1, device_id=peer, device_id_type=MESH)
    pl.semaphore_wait(barrier, len(peers))


def pair_source(step, half, steps):
    core = lax.rem(lax.axis_index('expert'), CORES)
    mine = step // half
    tile = lax.rem(step, half)
    lane = lax.rem(core + 1 + mine, CORES)
    return CORES * (tile // steps) + lane, lax.rem(tile, steps)


def pair_sum(compute, half, steps, tile, inbox_ref, out, exchanges, acc_ref, send_sem, recv_sem, in_sem, out_sem):
    step = pl.program_id(0)
    last = 2 * half - 1
    me = lax.axis_index('expert')
    other = me + 1 - 2 * lax.rem(me, CORES)

    def at(ref, job):
        return ref.at[job // steps, pl.ds(lax.rem(job, steps) * tile, tile)]

    def store(job):
        slot = lax.rem(job + half, N_ACC)
        out_ref, first = out
        rows = pl.ds(first + lax.rem(job, steps) * tile, tile)
        return pltpu.make_async_copy(acc_ref.at[slot], out_ref.at[job // steps, rows], out_sem.at[slot])

    def send(job):
        slot = lax.rem(job, N_ACC)
        return pltpu.make_async_remote_copy(
            src_ref=acc_ref.at[slot], dst_ref=at(inbox_ref, job), send_sem=send_sem.at[slot], recv_sem=recv_sem.at[job],
            device_id={'expert': other}, device_id_type=MESH)

    def fetch(job):
        slot = lax.rem(job + half, N_ACC)
        return pltpu.make_async_copy(at(inbox_ref, job), acc_ref.at[slot], in_sem.at[slot])

    @pl.when(step == 0)
    def _():
        meet([{'expert': peer} for peer in (exchanges[0].peers if exchanges else [other])])

    for exchange in exchanges:
        exchange.advance(step)

    back = step - (N_ACC - 1)

    @pl.when((back >= 0) & (back < half))
    def _():
        send(back).wait_send()

    @pl.when(back >= half)
    def _():
        store(back - half).wait()

    ahead = step + 1 - half

    @pl.when((ahead >= 0) & (ahead < half))
    def _():
        send(ahead).wait_recv()
        fetch(ahead).start()

    acc = acc_ref.at[lax.rem(step, N_ACC)]

    @pl.when(step >= half)
    def _():
        fetch(step - half).wait()

    def add(expert, rows):
        fresh = (expert == 0) & (step < half)
        acc[...] = jnp.where(fresh, 0.0, acc[...]) + rows

    compute(add)

    @pl.when(step < half)
    def _():
        send(step).start()

    @pl.when(step >= half)
    def _():
        store(step - half).start()

    @pl.when(step == last)
    def _():
        for job in range(half - N_ACC + 1, half):
            store(job).wait()
        for exchange in exchanges:
            exchange.finish()


class Exchange:
    def __init__(self, own_ref, first, ref, stage_ref, send_sem, recv_sem, local_sem, stages=()):
        me = lax.axis_index('expert')
        flip = lambda dev, bit: dev + bit - 2 * bit * lax.rem(dev // bit, 2)
        core, x, y = flip(me, 1), flip(me, 2), flip(me, 4)
        diag = flip(x, 4)
        self.peers = [core, x, y]
        self.stages = stages
        rows = ref.shape[1] // 2
        plan = [
            (0, rows, None, x, x),
            (rows, rows, None, y, y),
            (rows, rows, None, x, x),
            (0, rows, None, y, y),
            (0, 2 * rows, None, core, core),
            (0, rows, x, diag, y),
            (rows, rows, y, diag, x),
            (0, rows, x, flip(x, 1), core),
            (rows, rows, y, flip(y, 1), core),
            (rows, rows, x, flip(x, 1), core),
            (0, rows, y, flip(y, 1), core),
            (0, rows, diag, flip(diag, 1), core),
            (rows, rows, diag, flip(diag, 1), core),
        ]

        def copy(k, source, block):
            return pltpu.make_async_remote_copy(
                src_ref=source, dst_ref=ref.at[block, pl.ds(plan[k][0], plan[k][1])], send_sem=send_sem.at[k],
                recv_sem=recv_sem.at[k], device_id={'expert': plan[k][4]}, device_id_type=MESH)

        self.out, self.into = [], []
        for k, (row, n_rows, here, arrives, _) in enumerate(plan):
            own = own_ref.at[pl.ds(first + row, n_rows)]
            self.out.append(copy(k, own if here is None else ref.at[here, pl.ds(row, n_rows)], me if here is None else here))
            self.into.append(copy(k, own, arrives))
        self.take = pltpu.make_async_copy(own_ref.at[pl.ds(first, 2 * rows)], stage_ref, local_sem.at[0])
        self.put = pltpu.make_async_copy(stage_ref, ref.at[me], local_sem.at[1])

    def stage(self, k):
        arrived, started = (((), (0, 1, 2, 3, 4)), ((0, 1), (5, 6, 7, 8)), ((2, 3), (9, 10)), ((5, 6), (11, 12)))[k]
        for n in arrived:
            self.into[n].wait_recv()
        for n in started:
            self.out[n].start()
        if k == 0:
            self.take.start()

    def settle(self):
        self.take.wait()
        self.put.start()

    def advance(self, step):
        for k, at in enumerate(self.stages):
            pl.when(step == at)(functools.partial(self.stage, k))
        pl.when(step == 1)(self.settle)

    def finish(self):
        for k in (4,) + tuple(range(7, 13)):
            self.into[k].wait_recv()
        for copy in self.out:
            copy.wait_send()
        self.put.wait()


N_COPIES = 13


def exchange_scratch(rows, model):
    return [
        pltpu.VMEM((rows, model), BF16),
        pltpu.SemaphoreType.DMA((N_COPIES,)),
        pltpu.SemaphoreType.DMA((N_COPIES,)),
        pltpu.SemaphoreType.DMA((2,)),
    ]


def opening_body(n_stage, x_ref, dy_ref, own_ref, next_ref, x_all_ref, dy_all_ref, hop_sem, *scratch):
    me = {axis: lax.axis_index(axis) for axis in ('stage', 'expert')}
    beside = dict(me, stage=lax.rem(me['stage'] + 1, n_stage))
    first = 0
    hops = []
    for k, ref in enumerate((own_ref, next_ref)):
        hops.append(pltpu.make_async_remote_copy(
            src_ref=x_ref.at[pl.ds(first, ref.shape[0])], dst_ref=ref, send_sem=hop_sem.at[k, 0], recv_sem=hop_sem.at[k, 1],
            device_id=beside, device_id_type=MESH))
        first += ref.shape[0]
    dy = Exchange(dy_ref, 0, dy_all_ref, *scratch[:4])
    x = Exchange(own_ref, 0, x_all_ref, *scratch[4:])
    meet([{'expert': peer} for peer in dy.peers] + [beside])
    for hop in hops:
        hop.start()
    dy.stage(0)
    dy.settle()
    dy.stage(1)
    dy.stage(2)
    hops[0].wait_recv()
    x.stage(0)
    x.settle()
    dy.stage(3)
    for k in (1, 2, 3):
        x.stage(k)
    dy.finish()
    x.finish()
    hops[1].wait_recv()
    for hop in hops:
        hop.wait_send()


def opening(x, dy, rows, more, n_dev, n_stage, collective_id):
    model = x.shape[1]
    full = jax.ShapeDtypeStruct((n_dev, rows, model), x.dtype)
    outs = pl.pallas_call(
        functools.partial(opening_body, n_stage),
        in_specs=[HBM] * 2,
        out_specs=[HBM] * 4,
        out_shape=[jax.ShapeDtypeStruct((n, model), x.dtype) for n in (rows, more)] + [full, full],
        scratch_shapes=[pltpu.SemaphoreType.DMA((2, 2))] + exchange_scratch(rows, model) * 2,
        compiler_params=pltpu.CompilerParams(collective_id=collective_id, has_side_effects=True),
        name='opening',
    )(x, dy)
    return outs[1:]


def hosted_parts(hosted, stages, own_refs, buf_refs, scratch):
    return [Exchange(own_refs[k], row, buf_refs[k], *scratch[4 * k:4 * k + 4], stages[k]) for k, (row, _) in enumerate(hosted)]


class Weights:
    def __init__(self, hbm, w13_ref, w2_ref, sem):
        self.n_local = w2_ref.shape[0]
        ffn = w2_ref.shape[1]
        one, three, two = hbm
        self.copies = lambda e: [
            pltpu.make_async_copy(one.at[e], w13_ref.at[e, :, pl.ds(0, ffn)], sem.at[e, 0]),
            pltpu.make_async_copy(three.at[e], w13_ref.at[e, :, pl.ds(ffn, ffn)], sem.at[e, 1]),
            pltpu.make_async_copy(two.at[e], w2_ref.at[e], sem.at[e, 2]),
        ]

        @pl.when(pl.program_id(0) == 0)
        def _():
            for e in range(self.n_local):
                for copy in self.copies(e):
                    copy.start()

    def for_each(self, experts):
        def group(k, carry):
            @pl.when(pl.program_id(0) == 0)
            def _():
                for u in range(UNROLL):
                    for copy in self.copies(k * UNROLL + u):
                        copy.wait()

            experts([k * UNROLL + u for u in range(UNROLL)])
            return carry

        lax.fori_loop(0, self.n_local // UNROLL, group, 0)


def weight_scratch(w2):
    n_local, ffn, model = w2.shape
    return [pltpu.VMEM((n_local, model, 2 * ffn), BF16), pltpu.VMEM(w2.shape, BF16), pltpu.SemaphoreType.DMA((n_local, 3))]


def fwd_body(ffn, half, tile, start, n_x, n_carried, hosted, stages, *refs):
    refs = list(refs)
    x_refs, (g_ref, *weights_hbm), refs = refs[:n_x], refs[n_x:n_x + 4], refs[n_x + 4 + n_carried:]
    own_refs, refs = refs[:len(hosted)], refs[len(hosted):]
    (y_ref, inbox_ref), refs = refs[:2], refs[2:]
    buf_refs, refs = refs[:len(hosted)], refs[len(hosted):]
    w13_ref, w2_ref, w_sem, *refs = refs
    scratch, refs = refs[:5], refs[5:]
    exchanges = hosted_parts(hosted, stages, own_refs, buf_refs, refs)
    weights = Weights(weights_hbm, w13_ref, w2_ref, w_sem)

    def compute(add):
        def experts(es):
            gates = [gate_column(g_ref[0, start:start + tile], e) for e in es]
            x = rows_joined(x_refs)
            pres = [dot(x, w13_ref[e]) for e in es]
            for gate, pre, e in zip(gates, pres, es):
                one, three = pre[:, :ffn], pre[:, ffn:]
                hidden = jnp.where(gate > 0.0, one * jax.nn.sigmoid(one) * three, 0.0).astype(BF16)
                add(e, gate * dot(hidden, w2_ref[e]).astype(BF16).astype(F32))

        weights.for_each(experts)

    pair_sum(compute, half, 1, tile, inbox_ref, (y_ref, start), exchanges, *scratch)


def pair_scratch(tile, model, half):
    return [
        pltpu.VMEM((N_ACC, tile, model), F32),
        pltpu.SemaphoreType.DMA((N_ACC,)),
        pltpu.SemaphoreType.DMA((half,)),
        pltpu.SemaphoreType.DMA((N_ACC,)),
        pltpu.SemaphoreType.DMA((N_ACC,)),
    ]


def pair_params(collective_id):
    return pltpu.CompilerParams(
        dimension_semantics=('arbitrary',), vmem_limit_bytes=VMEM_LIMIT, collective_id=collective_id, has_side_effects=True)


HBM = pl.BlockSpec(memory_space=pl.ANY)


def at_source(half):
    def index(i):
        return pair_source(i, half, 1)[0], 0, 0

    return index


def expert_fwd(xs, gates, w, start, carried, hosted, stages, collective_id):
    n_src, _, model = xs[0][0].shape
    tile = BLOCK * len(xs)
    n_tok = gates.shape[1]
    w2 = w[2]
    n_local, ffn = w2.shape[:2]
    half = n_src // CORES
    at = at_source(half)
    flops = 2 * n_src * tile * n_local * model * ffn * 3

    def rows_of(block):
        return pl.BlockSpec((1, BLOCK, model), lambda i: (pair_source(i, half, 1)[0], block, 0))

    outs = pl.pallas_call(
        functools.partial(fwd_body, ffn, half, tile, start, len(xs), len(carried), [h[1:] for h in hosted], stages),
        grid=(2 * half,),
        in_specs=[rows_of(block) for _, block in xs] + [pl.BlockSpec((1, n_tok, n_local), at)]
        + [HBM] * (3 + len(carried) + len(hosted)),
        out_specs=[HBM] * (2 + len(hosted)),
        out_shape=[jax.ShapeDtypeStruct((half, n_tok, model), F32), jax.ShapeDtypeStruct((half, tile, model), F32)]
        + [jax.ShapeDtypeStruct((n_src, rows, model), BF16) for _, _, rows in hosted],
        scratch_shapes=weight_scratch(w2) + pair_scratch(tile, model, half)
        + [ref for _, _, rows in hosted for ref in exchange_scratch(rows, model)],
        input_output_aliases={len(xs) + 4 + i: i for i in range(len(carried))},
        compiler_params=pair_params(collective_id),
        cost_estimate=pl.CostEstimate(flops=flops, bytes_accessed=n_src * tile * model * 6, transcendentals=0),
        name='expert_fwd',
    )(*[x for x, _ in xs], gates, *w, *carried, *[h[0] for h in hosted])
    return outs[0], outs[2:]


def bwd_body(ffn, half, start, first, n_carried, hosted, stages, x_ref, dy_ref, g_ref, one_hbm, three_hbm, two_hbm, *refs):
    weights_hbm = one_hbm, three_hbm, two_hbm
    refs = list(refs[n_carried:])
    own_refs, refs = refs[:len(hosted)], refs[len(hosted):]
    (dx_ref, da_ref, h_ref, inbox_ref), refs = refs[:4], refs[4:]
    buf_refs, refs = refs[:len(hosted)], refs[len(hosted):]
    w13_ref, w2_ref, w_sem, *refs = refs
    scratch, refs = refs[:5], refs[5:]
    exchanges = hosted_parts(hosted, stages, own_refs, buf_refs, refs)
    tile = x_ref.shape[-2]
    weights = Weights(weights_hbm, w13_ref, w2_ref, w_sem)

    def compute(add):
        def experts(es):
            gates = [gate_column(g_ref[0, start:start + tile], e) for e in es]
            x = rows_joined([x_ref])
            pres = [dot(x, w13_ref[e]) for e in es]
            d_hids = []
            for gate, e in zip(gates, es):
                d_out = (gate * rows_joined([dy_ref]).astype(F32)).astype(BF16)
                d_hids.append(dot_t(d_out, w2_ref[e]).astype(BF16).astype(F32))
            for gate, pre, d_hid, e in zip(gates, pres, d_hids, es):
                live = gate > 0.0
                one, three = pre[:, :ffn], pre[:, ffn:]
                sig = jax.nn.sigmoid(one)
                act = one * sig
                h_ref[0, :, pl.ds(pl.multiple_of(e * ffn, ffn), ffn)] = jnp.where(live, act * three, 0.0).astype(BF16)
                d_one = jnp.where(live, d_hid * three * sig * (1.0 + one * (1.0 - sig)), 0.0).astype(BF16)
                d_three = jnp.where(live, d_hid * act, 0.0).astype(BF16)
                d_pre = jnp.concatenate([d_one, d_three], axis=1)
                da_ref[0, :, pl.ds(pl.multiple_of(2 * e * ffn, 2 * ffn), 2 * ffn)] = d_pre
                add(e, dot_t(d_pre, w13_ref[e]).astype(BF16).astype(F32))

        weights.for_each(experts)

    pair_sum(compute, half, 1, tile, inbox_ref, (dx_ref, first), exchanges, *scratch)


def expert_bwd(x, dy, gates, w, start, dx_rows, first, carried, hosted, stages, collective_id):
    n_src, tile, model = x[0].shape[0], x[0].shape[-2], x[0].shape[-1]
    n_tok = gates.shape[1]
    w2 = w[2]
    n_local, ffn = w2.shape[:2]
    half = n_src // CORES
    at = at_source(half)
    flops = 2 * n_src * tile * n_local * model * ffn * 5

    def rows_of(array, which):
        if array.ndim == 3:
            return pl.BlockSpec((1, tile, model), at)
        return pl.BlockSpec((1, 1, tile, model), lambda i: (pair_source(i, half, 1)[0], which, 0, 0))

    outs = pl.pallas_call(
        functools.partial(bwd_body, ffn, half, start, first, len(carried), [h[1:] for h in hosted], stages),
        grid=(2 * half,),
        in_specs=[rows_of(*x), rows_of(*dy), pl.BlockSpec((1, n_tok, n_local), at)]
        + [HBM] * (3 + len(carried) + len(hosted)),
        out_specs=[
            HBM,
            pl.BlockSpec((1, tile, 2 * ffn * n_local), at),
            pl.BlockSpec((1, tile, ffn * n_local), at),
        ] + [HBM] * (1 + len(hosted)),
        out_shape=[
            jax.ShapeDtypeStruct((half, dx_rows, model), F32),
            jax.ShapeDtypeStruct((n_src, tile, 2 * ffn * n_local), BF16),
            jax.ShapeDtypeStruct((n_src, tile, ffn * n_local), BF16),
            jax.ShapeDtypeStruct((half, tile, model), F32),
        ] + [jax.ShapeDtypeStruct((n_src, rows, model), BF16) for _, _, rows in hosted],
        scratch_shapes=weight_scratch(w2) + pair_scratch(tile, model, half)
        + [ref for _, _, rows in hosted for ref in exchange_scratch(rows, model)],
        input_output_aliases={6 + i: 0 for i in range(len(carried))},
        compiler_params=pair_params(collective_id),
        cost_estimate=pl.CostEstimate(flops=flops, bytes_accessed=n_src * tile * model * 14, transcendentals=0),
        name='expert_bwd',
    )(x[0], dy[0], gates, *w, *carried, *[h[0] for h in hosted])
    return outs[0], outs[1], outs[2], outs[4:]


def rows_joined(refs, column=0, columns=None):
    parts = [ref[(0,) * (len(ref.shape) - 2) + (slice(None), slice(column, column + (columns or ref.shape[-1])))] for ref in refs]
    return parts[0] if len(parts) == 1 else jnp.concatenate(parts, axis=0)


def grad_body(ffn, n_parts, g_ref, *refs):
    x_refs, dy_refs, da_refs, h_refs = (refs[k * n_parts:(k + 1) * n_parts] for k in range(4))
    dw1_ref, dw3_ref, dw2_ref, acc13_ref, acc2_ref = refs[4 * n_parts:]
    e, k = pl.program_id(0), pl.program_id(1)

    @pl.when(k == 0)
    def _():
        acc13_ref[...] = jnp.zeros_like(acc13_ref)
        acc2_ref[...] = jnp.zeros_like(acc2_ref)

    for m in range(0, acc13_ref.shape[0], ffn):
        acc13_ref[m:m + ffn] += dot_a(rows_joined(x_refs, m, ffn), rows_joined(da_refs))
    d_out = (gate_column(g_ref[0], e) * rows_joined(dy_refs).astype(F32)).astype(BF16)
    acc2_ref[...] += dot_a(rows_joined(h_refs), d_out)

    @pl.when(k == pl.num_programs(1) - 1)
    def _():
        dw1_ref[0] = acc13_ref[:, :ffn].astype(BF16)
        dw3_ref[0] = acc13_ref[:, ffn:].astype(BF16)
        dw2_ref[0] = acc2_ref[...].astype(BF16)


def weight_grads(gates, xs, dys, d_pres, hiddens):
    n_src, n_tok, n_local = gates.shape
    model = xs[0][0].shape[-1]
    ffn = hiddens[0].shape[2] // n_local
    flops = 2 * n_src * n_tok * n_local * model * ffn * 3
    at = lambda e, k: (k, 0, 0)
    at_e = lambda e, k: (k, 0, e)
    out = lambda e, k: (e, 0, 0)

    def rows_of(array, which):
        block = (1,) * (array.ndim - 2) + array.shape[-2:]
        return pl.BlockSpec(block, at if array.ndim == 3 else (lambda e, k: (k, which, 0, 0)))


    return pl.pallas_call(
        functools.partial(grad_body, ffn, len(xs)),
        grid=(n_local, n_src),
        in_specs=[pl.BlockSpec((1, n_tok, n_local), at)]
        + [rows_of(*x) for x in list(xs) + list(dys)]
        + [pl.BlockSpec((1, d.shape[1], 2 * ffn), at_e) for d in d_pres]
        + [pl.BlockSpec((1, h.shape[1], ffn), at_e) for h in hiddens],
        out_specs=[
            pl.BlockSpec((1, model, ffn), out),
            pl.BlockSpec((1, model, ffn), out),
            pl.BlockSpec((1, ffn, model), out),
        ],
        out_shape=[
            jax.ShapeDtypeStruct((n_local, model, ffn), BF16),
            jax.ShapeDtypeStruct((n_local, model, ffn), BF16),
            jax.ShapeDtypeStruct((n_local, ffn, model), BF16),
        ],
        scratch_shapes=[pltpu.VMEM((model, 2 * ffn), F32), pltpu.VMEM((ffn, model), F32)],
        compiler_params=pltpu.CompilerParams(dimension_semantics=('arbitrary', 'arbitrary'), vmem_limit_bytes=VMEM_LIMIT),
        cost_estimate=pl.CostEstimate(flops=flops, bytes_accessed=n_src * n_tok * model * 4 * n_local, transcendentals=0),
        name='weight_grads',
    )(gates, *[x for x, _ in xs], *[dy for dy, _ in dys], *d_pres, *hiddens)


def solution(mesh):
    n_stage = mesh.shape['stage']
    n_dev = mesh.shape['expert']
    to_next = [(stage_idx, (stage_idx + 1) % n_stage) for stage_idx in range(n_stage)]
    to_prev = [((stage_idx + 1) % n_stage, stage_idx) for stage_idx in range(n_stage)]
    tok_spec = P('stage', 'expert', None)
    w_spec = P('stage', 'expert', None, None)
    same_core = [list(range(core, n_dev, CORES)) for core in range(CORES)]

    def moe_body(x_act, route_idx, route_wts, w_one, w_three, w_two, dy_act):
        x_src = x_act[0]
        n_tok, _ = x_src.shape
        n_local = w_one.shape[1]
        n_exp = n_local * n_dev

        def gather(rows):
            return lax.all_gather(rows, 'expert', axis=0, tiled=False)

        def reduce_rows(part):
            return lax.psum_scatter(part, 'expert', scatter_dimension=0, axis_index_groups=same_core, tiled=False).astype(BF16)

        hits = route_idx[0][:, :, None] == jnp.arange(n_exp, dtype=jnp.int32)
        gate_src = jnp.sum(jnp.where(hits, route_wts[0][:, :, None], 0.0), axis=1)
        gate_src = jnp.transpose(gate_src.reshape(n_tok, n_dev, n_local), (1, 2, 0))
        gate_dst = lax.ppermute(gate_src, 'stage', to_next)
        gates = jnp.transpose(lax.all_to_all(gate_dst, 'expert', 0, 0), (0, 2, 1))

        w = w_one[0], w_three[0], w_two[0]

        def spans(sizes):
            ends = [sum(sizes[:k + 1]) for k in range(len(sizes))]
            return [slice(end - size, end) for end, size in zip(ends, sizes)]

        bwd, fwd = spans(BWD_ROWS), spans(FWD_ROWS)
        dx_rows = sum(BWD_ROWS[:2]), BWD_ROWS[2]

        def hop(rows):
            return lax.ppermute(x_src[rows], 'stage', to_next)

        x_next, x_all, dy_all = opening(x_src, dy_act[0], BWD_ROWS[0], BWD_ROWS[1], n_dev, n_stage, 5)
        dys, xs = [(dy_all, 0)], [(x_all, 0)]
        for k, x_dst in ((1, x_next), (2, hop(bwd[2]))):
            both = gather(jnp.stack([dy_act[0, bwd[k]], x_dst]))
            dys.append((both, 0))
            xs.append((both, 1))
        cut = sum(X_ROWS[:2])
        x_lo, x_hi = hop(slice(0, cut)), hop(slice(cut, n_tok))
        pieces = (x_lo, 0, X_ROWS[0]), (x_lo, X_ROWS[0], X_ROWS[1]), (x_hi, 0, X_ROWS[2])

        def blocks(arrived):
            return [(x, block) for x in arrived for block in range(x.shape[1] // BLOCK)]

        x_fwd, d_pres, hiddens = [], [], []
        dx_parts = []
        for k in range(3):
            dx_part, d_pre, hidden, arrived = expert_bwd(
                xs[k], dys[k], gates, w, bwd[k].start, dx_rows[k // 2], BWD_ROWS[0] if k == 1 else 0,
                (dx_part,) if k == 1 else (), pieces[k - 1:k] if k else (), STAGES[k - 1:k], k)
            x_fwd += blocks(arrived)
            d_pres.append(d_pre)
            hiddens.append(hidden)
            if k > 0:
                dx_dst = reduce_rows(dx_part)
                dx_parts.append(lax.ppermute(dx_dst, 'stage', to_prev))
        dx_out = jnp.concatenate(dx_parts, axis=0)[None]

        y_part = ()
        for k in range(2):
            out, arrived = expert_fwd(
                x_fwd[2 * k:2 * k + 2], gates, w, fwd[k].start, y_part, () if k else pieces[2:], STAGES[2:], 3 + k)
            y_part = (out,)
            x_fwd += blocks(arrived)
        y_out = reduce_rows(y_part[0])

        g_one, g_three, g_two = weight_grads(gates, xs, dys, d_pres, hiddens)
        return y_out[None], dx_out, g_one[None], g_three[None], g_two[None]

    return jax.shard_map(moe_body, mesh=mesh, in_specs=(tok_spec, tok_spec, tok_spec, w_spec, w_spec, w_spec, tok_spec), out_specs=(tok_spec, tok_spec, w_spec, w_spec, w_spec), check_vma=False)
```

```python
import functools

import jax
import jax.numpy as jnp
from jax import lax
from jax.experimental import pallas as pl
from jax.experimental.pallas import tpu as pltpu
from jax.sharding import PartitionSpec as P


F32 = jnp.float32
BF16 = jnp.bfloat16
BWD_ROWS = (256, 384, 384)
FWD_ROWS = (512, 512)
X_ROWS = (256, 512, 256)
STAGES = (0, 2, 4, 6), (0, 3, 5, 7), (0, 2, 4, 6)
VMEM_LIMIT = 65400 * 1024
N_ACC = 3
CORES = 2
UNROLL = 2
BLOCK = 256
MESH = pl.DeviceIdType.MESH


def dot(lhs, rhs):
    return jnp.dot(lhs, rhs, preferred_element_type=F32)


def dot_t(lhs, rhs):
    return lax.dot_general(lhs, rhs, (((1,), (1,)), ((), ())), preferred_element_type=F32)


def dot_a(lhs, rhs):
    return lax.dot_general(lhs, rhs, (((0,), (0,)), ((), ())), preferred_element_type=F32)


def gate_column(gates, expert):
    lanes = lax.broadcasted_iota(jnp.int32, gates.shape, 1)
    return jnp.sum(jnp.where(lanes == expert, gates, 0.0), axis=1, keepdims=True)


def meet(peers):
    barrier = pltpu.get_barrier_semaphore()
    for peer in peers:
        pl.semaphore_signal(barrier, inc=1, device_id=peer, device_id_type=MESH)
    pl.semaphore_wait(barrier, len(peers))


def pair_source(step, half, steps):
    core = lax.rem(lax.axis_index('expert'), CORES)
    mine = step // half
    tile = lax.rem(step, half)
    lane = lax.rem(core + 1 + mine, CORES)
    return CORES * (tile // steps) + lane, lax.rem(tile, steps)


def pair_sum(compute, half, steps, tile, inbox_ref, out, exchanges, acc_ref, send_sem, recv_sem, in_sem, out_sem):
    step = pl.program_id(0)
    last = 2 * half - 1
    me = lax.axis_index('expert')
    other = me + 1 - 2 * lax.rem(me, CORES)

    def at(ref, job):
        return ref.at[job // steps, pl.ds(lax.rem(job, steps) * tile, tile)]

    def store(job):
        slot = lax.rem(job + half, N_ACC)
        out_ref, first = out
        rows = pl.ds(first + lax.rem(job, steps) * tile, tile)
        return pltpu.make_async_copy(acc_ref.at[slot], out_ref.at[job // steps, rows], out_sem.at[slot])

    def send(job):
        slot = lax.rem(job, N_ACC)
        return pltpu.make_async_remote_copy(
            src_ref=acc_ref.at[slot], dst_ref=at(inbox_ref, job), send_sem=send_sem.at[slot], recv_sem=recv_sem.at[job],
            device_id={'expert': other}, device_id_type=MESH)

    def fetch(job):
        slot = lax.rem(job + half, N_ACC)
        return pltpu.make_async_copy(at(inbox_ref, job), acc_ref.at[slot], in_sem.at[slot])

    @pl.when(step == 0)
    def _():
        meet([{'expert': peer} for peer in (exchanges[0].peers if exchanges else [other])])

    for exchange in exchanges:
        exchange.advance(step)

    back = step - (N_ACC - 1)

    @pl.when((back >= 0) & (back < half))
    def _():
        send(back).wait_send()

    @pl.when(back >= half)
    def _():
        store(back - half).wait()

    ahead = step + 1 - half

    @pl.when((ahead >= 0) & (ahead < half))
    def _():
        send(ahead).wait_recv()
        fetch(ahead).start()

    acc = acc_ref.at[lax.rem(step, N_ACC)]

    @pl.when(step >= half)
    def _():
        fetch(step - half).wait()

    def add(expert, rows):
        fresh = (expert == 0) & (step < half)
        acc[...] = jnp.where(fresh, 0.0, acc[...]) + rows

    compute(add)

    @pl.when(step < half)
    def _():
        send(step).start()

    @pl.when(step >= half)
    def _():
        store(step - half).start()

    @pl.when(step == last)
    def _():
        for job in range(half - N_ACC + 1, half):
            store(job).wait()
        for exchange in exchanges:
            exchange.finish()


class Exchange:
    def __init__(self, own_ref, first, ref, stage_ref, send_sem, recv_sem, local_sem, stages=()):
        me = lax.axis_index('expert')
        flip = lambda dev, bit: dev + bit - 2 * bit * lax.rem(dev // bit, 2)
        core, x, y = flip(me, 1), flip(me, 2), flip(me, 4)
        diag = flip(x, 4)
        self.peers = [core, x, y]
        self.stages = stages
        rows = ref.shape[1] // 2
        plan = [
            (0, rows, None, x, x),
            (rows, rows, None, y, y),
            (rows, rows, None, x, x),
            (0, rows, None, y, y),
            (0, 2 * rows, None, core, core),
            (0, rows, x, diag, y),
            (rows, rows, y, diag, x),
            (0, rows, x, flip(x, 1), core),
            (rows, rows, y, flip(y, 1), core),
            (rows, rows, x, flip(x, 1), core),
            (0, rows, y, flip(y, 1), core),
            (0, rows, diag, flip(diag, 1), core),
            (rows, rows, diag, flip(diag, 1), core),
        ]

        def copy(k, source, block):
            return pltpu.make_async_remote_copy(
                src_ref=source, dst_ref=ref.at[block, pl.ds(plan[k][0], plan[k][1])], send_sem=send_sem.at[k],
                recv_sem=recv_sem.at[k], device_id={'expert': plan[k][4]}, device_id_type=MESH)

        self.out, self.into = [], []
        for k, (row, n_rows, here, arrives, _) in enumerate(plan):
            own = own_ref.at[pl.ds(first + row, n_rows)]
            self.out.append(copy(k, own if here is None else ref.at[here, pl.ds(row, n_rows)], me if here is None else here))
            self.into.append(copy(k, own, arrives))
        self.take = pltpu.make_async_copy(own_ref.at[pl.ds(first, 2 * rows)], stage_ref, local_sem.at[0])
        self.put = pltpu.make_async_copy(stage_ref, ref.at[me], local_sem.at[1])

    def stage(self, k):
        arrived, started = (((), (0, 1, 2, 3, 4)), ((0, 1), (5, 6, 7, 8)), ((2, 3), (9, 10)), ((5, 6), (11, 12)))[k]
        for n in arrived:
            self.into[n].wait_recv()
        for n in started:
            self.out[n].start()
        if k == 0:
            self.take.start()

    def settle(self):
        self.take.wait()
        self.put.start()

    def advance(self, step):
        for k, at in enumerate(self.stages):
            pl.when(step == at)(functools.partial(self.stage, k))
        pl.when(step == 1)(self.settle)

    def finish(self):
        for k in (4,) + tuple(range(7, 13)):
            self.into[k].wait_recv()
        for copy in self.out:
            copy.wait_send()
        self.put.wait()


N_COPIES = 13


def exchange_scratch(rows, model):
    return [
        pltpu.VMEM((rows, model), BF16),
        pltpu.SemaphoreType.DMA((N_COPIES,)),
        pltpu.SemaphoreType.DMA((N_COPIES,)),
        pltpu.SemaphoreType.DMA((2,)),
    ]


def opening_body(n_stage, x_ref, dy_ref, own_ref, next_ref, x_all_ref, dy_all_ref, hop_sem, stage_ref, stage_sem, *scratch):
    me = {axis: lax.axis_index(axis) for axis in ('stage', 'expert')}
    beside = dict(me, stage=lax.rem(me['stage'] + 1, n_stage))
    rows, more = own_ref.shape[0], next_ref.shape[1]
    hops = [
        pltpu.make_async_remote_copy(
            src_ref=x_ref.at[pl.ds(first, ref.shape[0])], dst_ref=ref, send_sem=hop_sem.at[k, 0], recv_sem=hop_sem.at[k, 1],
            device_id=beside, device_id_type=MESH)
        for k, (first, ref) in enumerate(((0, own_ref), (rows, next_ref.at[1])))]
    take = pltpu.make_async_copy(dy_ref.at[pl.ds(rows, more)], stage_ref, stage_sem.at[0])
    put = pltpu.make_async_copy(stage_ref, next_ref.at[0], stage_sem.at[1])
    dy = Exchange(dy_ref, 0, dy_all_ref, *scratch[:4])
    x = Exchange(own_ref, 0, x_all_ref, *scratch[4:])
    meet([{'expert': peer} for peer in dy.peers] + [beside])
    for hop in hops:
        hop.start()
    dy.stage(0)
    take.start()
    dy.settle()
    take.wait()
    put.start()
    dy.stage(1)
    dy.stage(2)
    hops[0].wait_recv()
    x.stage(0)
    x.settle()
    dy.stage(3)
    for k in (1, 2, 3):
        x.stage(k)
    dy.finish()
    x.finish()
    put.wait()
    hops[1].wait_recv()
    for hop in hops:
        hop.wait_send()


def opening(x, dy, rows, more, n_dev, n_stage, collective_id):
    model = x.shape[1]
    shapes = (rows, model), (2, more, model), (n_dev, rows, model), (n_dev, rows, model)
    outs = pl.pallas_call(
        functools.partial(opening_body, n_stage),
        in_specs=[HBM] * 2,
        out_specs=[HBM] * 4,
        out_shape=[jax.ShapeDtypeStruct(shape, x.dtype) for shape in shapes],
        scratch_shapes=[pltpu.SemaphoreType.DMA((2, 2)), pltpu.VMEM((more, model), BF16), pltpu.SemaphoreType.DMA((2,))]
        + exchange_scratch(rows, model) * 2,
        compiler_params=pltpu.CompilerParams(collective_id=collective_id, has_side_effects=True),
        name='opening',
    )(x, dy)
    return outs[1:]


def hosted_parts(hosted, stages, own_refs, buf_refs, scratch):
    return [Exchange(own_refs[k], row, buf_refs[k], *scratch[4 * k:4 * k + 4], stages[k]) for k, (row, _) in enumerate(hosted)]


class Weights:
    def __init__(self, hbm, w13_ref, w2_ref, sem):
        self.n_local = w2_ref.shape[0]
        ffn = w2_ref.shape[1]
        one, three, two = hbm
        self.copies = lambda e: [
            pltpu.make_async_copy(one.at[e], w13_ref.at[e, :, pl.ds(0, ffn)], sem.at[e, 0]),
            pltpu.make_async_copy(three.at[e], w13_ref.at[e, :, pl.ds(ffn, ffn)], sem.at[e, 1]),
            pltpu.make_async_copy(two.at[e], w2_ref.at[e], sem.at[e, 2]),
        ]

        @pl.when(pl.program_id(0) == 0)
        def _():
            for e in range(self.n_local):
                for copy in self.copies(e):
                    copy.start()

    def for_each(self, experts):
        def group(k, carry):
            @pl.when(pl.program_id(0) == 0)
            def _():
                for u in range(UNROLL):
                    for copy in self.copies(k * UNROLL + u):
                        copy.wait()

            experts([k * UNROLL + u for u in range(UNROLL)])
            return carry

        lax.fori_loop(0, self.n_local // UNROLL, group, 0)


def weight_scratch(w2):
    n_local, ffn, model = w2.shape
    return [pltpu.VMEM((n_local, model, 2 * ffn), BF16), pltpu.VMEM(w2.shape, BF16), pltpu.SemaphoreType.DMA((n_local, 3))]


def fwd_body(ffn, half, tile, start, n_x, n_carried, hosted, stages, *refs):
    refs = list(refs)
    x_refs, (g_ref, *weights_hbm), refs = refs[:n_x], refs[n_x:n_x + 4], refs[n_x + 4 + n_carried:]
    own_refs, refs = refs[:len(hosted)], refs[len(hosted):]
    (y_ref, inbox_ref), refs = refs[:2], refs[2:]
    buf_refs, refs = refs[:len(hosted)], refs[len(hosted):]
    w13_ref, w2_ref, w_sem, *refs = refs
    scratch, refs = refs[:5], refs[5:]
    exchanges = hosted_parts(hosted, stages, own_refs, buf_refs, refs)
    weights = Weights(weights_hbm, w13_ref, w2_ref, w_sem)

    def compute(add):
        def experts(es):
            gates = [gate_column(g_ref[0, start:start + tile], e) for e in es]
            x = rows_joined(x_refs)
            pres = [dot(x, w13_ref[e]) for e in es]
            for gate, pre, e in zip(gates, pres, es):
                one, three = pre[:, :ffn], pre[:, ffn:]
                hidden = jnp.where(gate > 0.0, one * jax.nn.sigmoid(one) * three, 0.0).astype(BF16)
                add(e, gate * dot(hidden, w2_ref[e]).astype(BF16).astype(F32))

        weights.for_each(experts)

    pair_sum(compute, half, 1, tile, inbox_ref, (y_ref, start), exchanges, *scratch)


def pair_scratch(tile, model, half):
    return [
        pltpu.VMEM((N_ACC, tile, model), F32),
        pltpu.SemaphoreType.DMA((N_ACC,)),
        pltpu.SemaphoreType.DMA((half,)),
        pltpu.SemaphoreType.DMA((N_ACC,)),
        pltpu.SemaphoreType.DMA((N_ACC,)),
    ]


def pair_params(collective_id):
    return pltpu.CompilerParams(
        dimension_semantics=('arbitrary',), vmem_limit_bytes=VMEM_LIMIT, collective_id=collective_id, has_side_effects=True)


HBM = pl.BlockSpec(memory_space=pl.ANY)


def at_source(half):
    def index(i):
        return pair_source(i, half, 1)[0], 0, 0

    return index


def expert_fwd(xs, gates, w, start, carried, hosted, stages, collective_id):
    n_src, _, model = xs[0][0].shape
    tile = BLOCK * len(xs)
    n_tok = gates.shape[1]
    w2 = w[2]
    n_local, ffn = w2.shape[:2]
    half = n_src // CORES
    at = at_source(half)
    flops = 2 * n_src * tile * n_local * model * ffn * 3

    def rows_of(block):
        return pl.BlockSpec((1, BLOCK, model), lambda i: (pair_source(i, half, 1)[0], block, 0))

    outs = pl.pallas_call(
        functools.partial(fwd_body, ffn, half, tile, start, len(xs), len(carried), [h[1:] for h in hosted], stages),
        grid=(2 * half,),
        in_specs=[rows_of(block) for _, block in xs] + [pl.BlockSpec((1, n_tok, n_local), at)]
        + [HBM] * (3 + len(carried) + len(hosted)),
        out_specs=[HBM] * (2 + len(hosted)),
        out_shape=[jax.ShapeDtypeStruct((half, n_tok, model), F32), jax.ShapeDtypeStruct((half, tile, model), F32)]
        + [jax.ShapeDtypeStruct((n_src, rows, model), BF16) for _, _, rows in hosted],
        scratch_shapes=weight_scratch(w2) + pair_scratch(tile, model, half)
        + [ref for _, _, rows in hosted for ref in exchange_scratch(rows, model)],
        input_output_aliases={len(xs) + 4 + i: i for i in range(len(carried))},
        compiler_params=pair_params(collective_id),
        cost_estimate=pl.CostEstimate(flops=flops, bytes_accessed=n_src * tile * model * 6, transcendentals=0),
        name='expert_fwd',
    )(*[x for x, _ in xs], gates, *w, *carried, *[h[0] for h in hosted])
    return outs[0], outs[2:]


def bwd_body(ffn, half, start, first, n_carried, hosted, stages, x_ref, dy_ref, g_ref, one_hbm, three_hbm, two_hbm, *refs):
    weights_hbm = one_hbm, three_hbm, two_hbm
    refs = list(refs[n_carried:])
    own_refs, refs = refs[:len(hosted)], refs[len(hosted):]
    (dx_ref, da_ref, h_ref, inbox_ref), refs = refs[:4], refs[4:]
    buf_refs, refs = refs[:len(hosted)], refs[len(hosted):]
    w13_ref, w2_ref, w_sem, *refs = refs
    scratch, refs = refs[:5], refs[5:]
    exchanges = hosted_parts(hosted, stages, own_refs, buf_refs, refs)
    tile = x_ref.shape[-2]
    weights = Weights(weights_hbm, w13_ref, w2_ref, w_sem)

    def compute(add):
        def experts(es):
            gates = [gate_column(g_ref[0, start:start + tile], e) for e in es]
            x = rows_joined([x_ref])
            pres = [dot(x, w13_ref[e]) for e in es]
            d_hids = []
            for gate, e in zip(gates, es):
                d_out = (gate * rows_joined([dy_ref]).astype(F32)).astype(BF16)
                d_hids.append(dot_t(d_out, w2_ref[e]).astype(BF16).astype(F32))
            for gate, pre, d_hid, e in zip(gates, pres, d_hids, es):
                live = gate > 0.0
                one, three = pre[:, :ffn], pre[:, ffn:]
                sig = jax.nn.sigmoid(one)
                act = one * sig
                h_ref[0, :, pl.ds(pl.multiple_of(e * ffn, ffn), ffn)] = jnp.where(live, act * three, 0.0).astype(BF16)
                d_one = jnp.where(live, d_hid * three * sig * (1.0 + one * (1.0 - sig)), 0.0).astype(BF16)
                d_three = jnp.where(live, d_hid * act, 0.0).astype(BF16)
                d_pre = jnp.concatenate([d_one, d_three], axis=1)
                da_ref[0, :, pl.ds(pl.multiple_of(2 * e * ffn, 2 * ffn), 2 * ffn)] = d_pre
                add(e, dot_t(d_pre, w13_ref[e]).astype(BF16).astype(F32))

        weights.for_each(experts)

    pair_sum(compute, half, 1, tile, inbox_ref, (dx_ref, first), exchanges, *scratch)


def expert_bwd(x, dy, gates, w, start, dx_rows, first, carried, hosted, stages, collective_id):
    n_src, tile, model = x[0].shape[0], x[0].shape[-2], x[0].shape[-1]
    n_tok = gates.shape[1]
    w2 = w[2]
    n_local, ffn = w2.shape[:2]
    half = n_src // CORES
    at = at_source(half)
    flops = 2 * n_src * tile * n_local * model * ffn * 5

    def rows_of(array, which):
        if array.ndim == 3:
            return pl.BlockSpec((1, tile, model), at)
        return pl.BlockSpec((1, 1, tile, model), lambda i: (pair_source(i, half, 1)[0], which, 0, 0))

    outs = pl.pallas_call(
        functools.partial(bwd_body, ffn, half, start, first, len(carried), [h[1:] for h in hosted], stages),
        grid=(2 * half,),
        in_specs=[rows_of(*x), rows_of(*dy), pl.BlockSpec((1, n_tok, n_local), at)]
        + [HBM] * (3 + len(carried) + len(hosted)),
        out_specs=[
            HBM,
            pl.BlockSpec((1, tile, 2 * ffn * n_local), at),
            pl.BlockSpec((1, tile, ffn * n_local), at),
        ] + [HBM] * (1 + len(hosted)),
        out_shape=[
            jax.ShapeDtypeStruct((half, dx_rows, model), F32),
            jax.ShapeDtypeStruct((n_src, tile, 2 * ffn * n_local), BF16),
            jax.ShapeDtypeStruct((n_src, tile, ffn * n_local), BF16),
            jax.ShapeDtypeStruct((half, tile, model), F32),
        ] + [jax.ShapeDtypeStruct((n_src, rows, model), BF16) for _, _, rows in hosted],
        scratch_shapes=weight_scratch(w2) + pair_scratch(tile, model, half)
        + [ref for _, _, rows in hosted for ref in exchange_scratch(rows, model)],
        input_output_aliases={6 + i: 0 for i in range(len(carried))},
        compiler_params=pair_params(collective_id),
        cost_estimate=pl.CostEstimate(flops=flops, bytes_accessed=n_src * tile * model * 14, transcendentals=0),
        name='expert_bwd',
    )(x[0], dy[0], gates, *w, *carried, *[h[0] for h in hosted])
    return outs[0], outs[1], outs[2], outs[4:]


def rows_joined(refs, column=0, columns=None):
    parts = [ref[(0,) * (len(ref.shape) - 2) + (slice(None), slice(column, column + (columns or ref.shape[-1])))] for ref in refs]
    return parts[0] if len(parts) == 1 else jnp.concatenate(parts, axis=0)


def grad_body(ffn, n_parts, g_ref, *refs):
    x_refs, dy_refs, da_refs, h_refs = (refs[k * n_parts:(k + 1) * n_parts] for k in range(4))
    dw1_ref, dw3_ref, dw2_ref, acc13_ref, acc2_ref = refs[4 * n_parts:]
    e, k = pl.program_id(0), pl.program_id(1)

    @pl.when(k == 0)
    def _():
        acc13_ref[...] = jnp.zeros_like(acc13_ref)
        acc2_ref[...] = jnp.zeros_like(acc2_ref)

    for m in range(0, acc13_ref.shape[0], ffn):
        acc13_ref[m:m + ffn] += dot_a(rows_joined(x_refs, m, ffn), rows_joined(da_refs))
    d_out = (gate_column(g_ref[0], e) * rows_joined(dy_refs).astype(F32)).astype(BF16)
    acc2_ref[...] += dot_a(rows_joined(h_refs), d_out)

    @pl.when(k == pl.num_programs(1) - 1)
    def _():
        dw1_ref[0] = acc13_ref[:, :ffn].astype(BF16)
        dw3_ref[0] = acc13_ref[:, ffn:].astype(BF16)
        dw2_ref[0] = acc2_ref[...].astype(BF16)


def weight_grads(gates, xs, dys, d_pres, hiddens):
    n_src, n_tok, n_local = gates.shape
    model = xs[0][0].shape[-1]
    ffn = hiddens[0].shape[2] // n_local
    flops = 2 * n_src * n_tok * n_local * model * ffn * 3
    at = lambda e, k: (k, 0, 0)
    at_e = lambda e, k: (k, 0, e)
    out = lambda e, k: (e, 0, 0)

    def rows_of(array, which):
        block = (1,) * (array.ndim - 2) + array.shape[-2:]
        return pl.BlockSpec(block, at if array.ndim == 3 else (lambda e, k: (k, which, 0, 0)))


    return pl.pallas_call(
        functools.partial(grad_body, ffn, len(xs)),
        grid=(n_local, n_src),
        in_specs=[pl.BlockSpec((1, n_tok, n_local), at)]
        + [rows_of(*x) for x in list(xs) + list(dys)]
        + [pl.BlockSpec((1, d.shape[1], 2 * ffn), at_e) for d in d_pres]
        + [pl.BlockSpec((1, h.shape[1], ffn), at_e) for h in hiddens],
        out_specs=[
            pl.BlockSpec((1, model, ffn), out),
            pl.BlockSpec((1, model, ffn), out),
            pl.BlockSpec((1, ffn, model), out),
        ],
        out_shape=[
            jax.ShapeDtypeStruct((n_local, model, ffn), BF16),
            jax.ShapeDtypeStruct((n_local, model, ffn), BF16),
            jax.ShapeDtypeStruct((n_local, ffn, model), BF16),
        ],
        scratch_shapes=[pltpu.VMEM((model, 2 * ffn), F32), pltpu.VMEM((ffn, model), F32)],
        compiler_params=pltpu.CompilerParams(dimension_semantics=('arbitrary', 'arbitrary'), vmem_limit_bytes=VMEM_LIMIT),
        cost_estimate=pl.CostEstimate(flops=flops, bytes_accessed=n_src * n_tok * model * 4 * n_local, transcendentals=0),
        name='weight_grads',
    )(gates, *[x for x, _ in xs], *[dy for dy, _ in dys], *d_pres, *hiddens)


def solution(mesh):
    n_stage = mesh.shape['stage']
    n_dev = mesh.shape['expert']
    to_next = [(stage_idx, (stage_idx + 1) % n_stage) for stage_idx in range(n_stage)]
    to_prev = [((stage_idx + 1) % n_stage, stage_idx) for stage_idx in range(n_stage)]
    tok_spec = P('stage', 'expert', None)
    w_spec = P('stage', 'expert', None, None)
    same_core = [list(range(core, n_dev, CORES)) for core in range(CORES)]

    def moe_body(x_act, route_idx, route_wts, w_one, w_three, w_two, dy_act):
        x_src = x_act[0]
        n_tok, _ = x_src.shape
        n_local = w_one.shape[1]
        n_exp = n_local * n_dev

        def gather(rows):
            return lax.all_gather(rows, 'expert', axis=0, tiled=False)

        def reduce_rows(part):
            return lax.psum_scatter(part, 'expert', scatter_dimension=0, axis_index_groups=same_core, tiled=False).astype(BF16)

        hits = route_idx[0][:, :, None] == jnp.arange(n_exp, dtype=jnp.int32)
        gate_src = jnp.sum(jnp.where(hits, route_wts[0][:, :, None], 0.0), axis=1)
        gate_src = jnp.transpose(gate_src.reshape(n_tok, n_dev, n_local), (1, 2, 0))
        gate_dst = lax.ppermute(gate_src, 'stage', to_next)
        gates = jnp.transpose(lax.all_to_all(gate_dst, 'expert', 0, 0), (0, 2, 1))

        w = w_one[0], w_three[0], w_two[0]

        def spans(sizes):
            ends = [sum(sizes[:k + 1]) for k in range(len(sizes))]
            return [slice(end - size, end) for end, size in zip(ends, sizes)]

        bwd, fwd = spans(BWD_ROWS), spans(FWD_ROWS)
        dx_rows = sum(BWD_ROWS[:2]), BWD_ROWS[2]

        def hop(rows):
            return lax.ppermute(x_src[rows], 'stage', to_next)

        both, x_all, dy_all = opening(x_src, dy_act[0], BWD_ROWS[0], BWD_ROWS[1], n_dev, n_stage, 5)
        dys, xs = [(dy_all, 0)], [(x_all, 0)]
        for stacked in (both, jnp.stack([dy_act[0, bwd[2]], hop(bwd[2])])):
            both = gather(stacked)
            dys.append((both, 0))
            xs.append((both, 1))
        cut = sum(X_ROWS[:2])
        x_lo, x_hi = hop(slice(0, cut)), hop(slice(cut, n_tok))
        pieces = (x_lo, 0, X_ROWS[0]), (x_lo, X_ROWS[0], X_ROWS[1]), (x_hi, 0, X_ROWS[2])

        def blocks(arrived):
            return [(x, block) for x in arrived for block in range(x.shape[1] // BLOCK)]

        x_fwd, d_pres, hiddens = [], [], []
        dx_parts = []
        for k in range(3):
            dx_part, d_pre, hidden, arrived = expert_bwd(
                xs[k], dys[k], gates, w, bwd[k].start, dx_rows[k // 2], BWD_ROWS[0] if k == 1 else 0,
                (dx_part,) if k == 1 else (), pieces[k - 1:k] if k else (), STAGES[k - 1:k], k)
            x_fwd += blocks(arrived)
            d_pres.append(d_pre)
            hiddens.append(hidden)
            if k > 0:
                dx_dst = reduce_rows(dx_part)
                dx_parts.append(lax.ppermute(dx_dst, 'stage', to_prev))
        dx_out = jnp.concatenate(dx_parts, axis=0)[None]

        y_part = ()
        for k in range(2):
            out, arrived = expert_fwd(
                x_fwd[2 * k:2 * k + 2], gates, w, fwd[k].start, y_part, () if k else pieces[2:], STAGES[2:], 3 + k)
            y_part = (out,)
            x_fwd += blocks(arrived)
        y_out = reduce_rows(y_part[0])

        g_one, g_three, g_two = weight_grads(gates, xs, dys, d_pres, hiddens)
        return y_out[None], dx_out, g_one[None], g_three[None], g_two[None]

    return jax.shard_map(moe_body, mesh=mesh, in_specs=(tok_spec, tok_spec, tok_spec, w_spec, w_spec, w_spec, tok_spec), out_specs=(tok_spec, tok_spec, w_spec, w_spec, w_spec), check_vma=False)
```
